32 devices in a mesh: dp: 2 (over x), cp: 16 (over z, y, core).
Axes of the slice: x: 2, y: 2, z: 4, core: 2. Of those that a mesh axis runs over, the one named last changes fastest.
Arguments:
- x_tok: bfloat16 [256, 2048], P(('dp', 'cp')), parts along dimension 0
- prompt_lens: int32 [256], P('dp'), parts along dimension 0
- k_cache: bfloat16 [256, 1024, 2, 128], P('dp', 'cp'), parts along dimension 0
- v_cache: bfloat16 [256, 1024, 2, 128], P('dp', 'cp'), parts along dimension 0
- norm_gain: bfloat16 [2048], replicated
- w_q: bfloat16 [2048, 2048], replicated
- b_q: bfloat16 [2048], replicated
- w_k: bfloat16 [2048, 256], replicated
- b_k: bfloat16 [256], replicated
- w_v: bfloat16 [2048, 256], replicated
- b_v: bfloat16 [256], replicated
- w_o: bfloat16 [2048, 2048], replicated
Outputs:
- output 1: bfloat16 [256, 2048], P(('dp', 'cp')), parts along dimension 0
- output 2: bfloat16 [256, 1024, 2, 128], P(('dp', 'cp')), parts along dimension 0
- output 3: bfloat16 [256, 1024, 2, 128], P(('dp', 'cp')), parts along dimension 0
There are 2 independent parts. The reference program is written for one: setup_inputs(seed, part) draws one part's arguments, and reference() takes and returns one part's arrays. A program takes and returns all parts, laid end to end along the dimension named above; an argument that names none is the same for every part.
All inputs are finite; a program needn't handle non-finite values.
Results may differ from the reference program's by a relative error of at most 0.00668478.
Values are sent between devices in bfloat16 or wider.
A program may use at most 1 GiB of HBM per device.

```python
import math
import jax
import jax.numpy as jnp
from jax import lax

D = 2048
HEADS = 16
KV_HEADS = 2
HEAD = 128
BATCH = 128
SEQ = 1024

GROUP = HEADS // KV_HEADS
HALF = HEAD // 2
RMS_EPS = 1e-6
ROPE_THETA = 1000000.0
SCORE_SCALE = HEAD ** -0.5


def normal_draw(draw_key, shape, scale):
    return (jax.random.normal(draw_key, shape, jnp.float32) * scale).astype(jnp.bfloat16)


def setup_inputs(seed: int = 0, part: int = 0) -> dict:
    base_key = jax.random.key(seed)
    part_keys = jax.random.split(jax.random.fold_in(base_key, part), 5)
    weight_keys = jax.random.split(base_key, 8)
    gain = math.sqrt(SEQ) / 4.0
    low_len = SEQ // 16
    prompt_lens = jax.random.randint(part_keys[1], (BATCH,), low_len, SEQ, jnp.int32)
    order = jax.random.permutation(part_keys[2], BATCH)
    prompt_lens = prompt_lens.at[order[0]].set(SEQ - 1).at[order[1]].set(low_len)
    norm_gain = (1.0 + 0.3 * jax.random.normal(weight_keys[0], (D,), jnp.float32)).astype(jnp.bfloat16)
    return {
        'x_tok': normal_draw(part_keys[0], (BATCH, D), 1.0),
        'prompt_lens': prompt_lens,
        'k_cache': normal_draw(part_keys[3], (BATCH, SEQ, KV_HEADS, HEAD), 1.0),
        'v_cache': normal_draw(part_keys[4], (BATCH, SEQ, KV_HEADS, HEAD), 1.0),
        'norm_gain': norm_gain,
        'w_q': normal_draw(weight_keys[1], (D, HEADS * HEAD), D ** -0.5),
        'b_q': normal_draw(weight_keys[2], (HEADS * HEAD,), 0.5),
        'w_k': normal_draw(weight_keys[3], (D, KV_HEADS * HEAD), D ** -0.5),
        'b_k': normal_draw(weight_keys[4], (KV_HEADS * HEAD,), 1.0),
        'w_v': normal_draw(weight_keys[5], (D, KV_HEADS * HEAD), gain * D ** -0.5),
        'b_v': normal_draw(weight_keys[6], (KV_HEADS * HEAD,), 0.5 * gain),
        'w_o': normal_draw(weight_keys[7], (HEADS * HEAD, D), gain * (HEADS * HEAD) ** -0.5),
    }


def rotary(vectors, positions):
    inv_freq = jnp.power(ROPE_THETA, -(jnp.arange(HALF).astype(jnp.float32) * 2.0 / HEAD))
    angle = positions.astype(jnp.float32)[:, None, None] * inv_freq
    cos_t = jnp.cos(angle)
    sin_t = jnp.sin(angle)
    first = vectors[..., :HALF]
    second = vectors[..., HALF:]
    return jnp.concatenate([first * cos_t - second * sin_t, second * cos_t + first * sin_t], axis=-1)


def reference(x_tok, prompt_lens, k_cache, v_cache, norm_gain, w_q, b_q, w_k, b_k, w_v, b_v, w_o):
    x_wide = x_tok.astype(jnp.float32)
    mean_sq = jnp.mean(x_wide * x_wide, axis=-1, keepdims=True)
    normed = (x_wide * lax.rsqrt(mean_sq + RMS_EPS) * norm_gain.astype(jnp.float32)).astype(jnp.bfloat16)
    query = jnp.dot(normed, w_q, preferred_element_type=jnp.float32) + b_q.astype(jnp.float32)
    query = rotary(query.reshape(BATCH, HEADS, HEAD), prompt_lens).astype(jnp.bfloat16)
    key_new = jnp.dot(normed, w_k, preferred_element_type=jnp.float32) + b_k.astype(jnp.float32)
    key_new = rotary(key_new.reshape(BATCH, KV_HEADS, HEAD), prompt_lens).astype(jnp.bfloat16)
    value_new = jnp.dot(normed, w_v, preferred_element_type=jnp.float32) + b_v.astype(jnp.float32)
    value_new = value_new.reshape(BATCH, KV_HEADS, HEAD).astype(jnp.bfloat16)
    slot_idx = jnp.arange(SEQ)

    def one_sequence(operands):
        keys_old, vals_old, query_one, key_one, value_one, length = operands
        before = (slot_idx < length)[:, None, None]
        at_new = (slot_idx == length)[:, None, None]
        keys_all = jnp.where(at_new, key_one[None], jnp.where(before, keys_old, jnp.zeros_like(keys_old)))
        vals_all = jnp.where(at_new, value_one[None], jnp.where(before, vals_old, jnp.zeros_like(vals_old)))
        scores = jnp.einsum('kgd,skd->kgs', query_one.reshape(KV_HEADS, GROUP, HEAD).astype(jnp.float32), keys_all.astype(jnp.float32)) * SCORE_SCALE
        scores = jnp.where(slot_idx <= length, scores, -1e30)
        row_max = jnp.max(scores, axis=-1, keepdims=True)
        weights = jnp.exp(scores - row_max)
        weight_sum = jnp.sum(weights, axis=-1, keepdims=True)
        mixed = jnp.einsum('kgs,skd->kgd', weights.astype(jnp.bfloat16).astype(jnp.float32), vals_all.astype(jnp.float32)) / weight_sum
        return keys_all, vals_all, mixed.reshape(HEADS * HEAD).astype(jnp.bfloat16)

    k_out, v_out, attended = lax.map(one_sequence, (k_cache, v_cache, query, key_new, value_new, prompt_lens))
    y_out = (x_wide + jnp.dot(attended, w_o, preferred_element_type=jnp.float32)).astype(jnp.bfloat16)
    return y_out, k_out, v_out
```

```python
import functools
import jax
import jax.numpy as jnp
from jax import lax
from jax.experimental import pallas as pl
from jax.experimental.pallas import tpu as pltpu
from jax.sharding import PartitionSpec as P

RMS_EPS = 1e-6
ROPE_THETA = 1000000.0
MESH = pl.DeviceIdType.MESH


def rotary(vectors, positions):
    head_dim = vectors.shape[-1]
    half_dim = head_dim // 2
    inv_freq = jnp.power(ROPE_THETA, -(jnp.arange(half_dim, dtype=jnp.float32) * 2.0 / head_dim))
    angle = positions.astype(jnp.float32)[:, None, None] * inv_freq
    cos_t = jnp.cos(angle)
    sin_t = jnp.sin(angle)
    first = vectors[..., :half_dim]
    second = vectors[..., half_dim:]
    return jnp.concatenate([first * cos_t - second * sin_t, second * cos_t + first * sin_t], axis=-1)


def project(x_tok, positions, norm_gain, w_q, b_q, w_k, b_k, w_v, b_v, head_dim):
    rows = x_tok.shape[0]
    x_wide = x_tok.astype(jnp.float32)
    mean_sq = jnp.mean(x_wide * x_wide, axis=-1, keepdims=True)
    normed = (x_wide * lax.rsqrt(mean_sq + RMS_EPS) * norm_gain.astype(jnp.float32)).astype(jnp.bfloat16)
    query = jnp.dot(normed, w_q, preferred_element_type=jnp.float32) + b_q.astype(jnp.float32)
    query = rotary(query.reshape(rows, -1, head_dim), positions).astype(jnp.bfloat16)
    key_new = jnp.dot(normed, w_k, preferred_element_type=jnp.float32) + b_k.astype(jnp.float32)
    key_new = rotary(key_new.reshape(rows, -1, head_dim), positions).astype(jnp.bfloat16)
    value_new = jnp.dot(normed, w_v, preferred_element_type=jnp.float32) + b_v.astype(jnp.float32)
    value_new = value_new.reshape(rows, -1, head_dim).astype(jnp.bfloat16)
    return query, key_new, value_new


def exchange_kernel(n, k_ref, v_ref, kr_ref, vr_ref, send_sem, recv_sem, local_sem):
    me = lax.axis_index("cp")
    barrier = pltpu.get_barrier_semaphore()

    def hello(d, c):
        pl.semaphore_signal(barrier, inc=1, device_id={"cp": lax.rem(me + d, n)}, device_id_type=MESH)
        return c

    lax.fori_loop(1, n, hello, 0)
    pl.semaphore_wait(barrier, n - 1)

    def remote(src, dst, a, d):
        to = lax.rem(me + d, n)
        return pltpu.make_async_remote_copy(
            src_ref=src.at[to], dst_ref=dst.at[:, me], send_sem=send_sem.at[a, d], recv_sem=recv_sem.at[a, d],
            device_id={"cp": to}, device_id_type=MESH)

    def start(d, c):
        remote(k_ref, kr_ref, 0, d).start()
        remote(v_ref, vr_ref, 1, d).start()
        return c

    lax.fori_loop(1, n, start, 0)
    own_k = pltpu.make_async_copy(k_ref.at[me], kr_ref.at[:, me], local_sem.at[0])
    own_v = pltpu.make_async_copy(v_ref.at[me], vr_ref.at[:, me], local_sem.at[1])
    own_k.start()
    own_v.start()

    def finish(d, c):
        remote(k_ref, kr_ref, 0, d).wait_send()
        remote(v_ref, vr_ref, 1, d).wait_send()
        src = lax.rem(me + n - d, n)
        pltpu.make_async_remote_copy(
            src_ref=k_ref.at[0], dst_ref=kr_ref.at[:, src], send_sem=send_sem.at[0, d], recv_sem=recv_sem.at[0, d],
            device_id={"cp": src}, device_id_type=MESH).wait_recv()
        pltpu.make_async_remote_copy(
            src_ref=v_ref.at[0], dst_ref=vr_ref.at[:, src], send_sem=send_sem.at[1, d], recv_sem=recv_sem.at[1, d],
            device_id={"cp": src}, device_id_type=MESH).wait_recv()
        return c

    lax.fori_loop(1, n, finish, 0)
    own_k.wait()
    own_v.wait()


def exchange(k, v):
    n, rows, m, d = k.shape
    out = jax.ShapeDtypeStruct((rows, n, m, d), k.dtype)
    return pl.pallas_call(
        functools.partial(exchange_kernel, n),
        out_shape=[out, out],
        in_specs=[pl.BlockSpec(memory_space=pl.ANY)] * 2,
        out_specs=[pl.BlockSpec(memory_space=pl.ANY)] * 2,
        scratch_shapes=[pltpu.SemaphoreType.DMA((2, n)), pltpu.SemaphoreType.DMA((2, n)), pltpu.SemaphoreType.DMA((2,))],
        compiler_params=pltpu.CompilerParams(collective_id=0, has_side_effects=True),
    )(k, v)


def attend_kernel(pos_ref, q_ref, kn_ref, vn_ref, kr_ref, vr_ref, ko_ref, vo_ref, o_ref):
    pos = pos_ref[pl.program_id(0)]
    heads, dim = q_ref.shape[1:]
    m = kr_ref.shape[1]
    row = lax.broadcasted_iota(jnp.int32, (m, dim), 0)
    zero = jnp.zeros((m, dim), jnp.float32)

    def merge(raw_ref, new_ref):
        new = new_ref[0].astype(jnp.float32)
        fresh = jnp.where(row % 2 == 0, new[0:1], new[1:2])
        return jnp.where(row < 2 * pos, raw_ref[0].astype(jnp.float32), jnp.where(row < 2 * pos + 2, fresh, zero)).astype(jnp.bfloat16)

    keys = merge(kr_ref, kn_ref)
    vals = merge(vr_ref, vn_ref)
    ko_ref[0] = keys
    vo_ref[0] = vals
    s = lax.dot_general(q_ref[0], keys, (((1,), (1,)), ((), ())), preferred_element_type=jnp.float32) * (dim ** -0.5)
    col = lax.broadcasted_iota(jnp.int32, (heads, m), 1)
    head = lax.broadcasted_iota(jnp.int32, (heads, m), 0)
    valid = (col < 2 * pos + 2) & (col % 2 == head // (heads // 2))
    s = jnp.where(valid, s, -1e30)
    top = jnp.max(s, axis=-1, keepdims=True)
    e = jnp.where(valid, jnp.exp(s - top), 0.0)
    total = jnp.sum(e, axis=-1, keepdims=True)
    o_ref[0] = (jnp.dot(e.astype(jnp.bfloat16), vals, preferred_element_type=jnp.float32) / total).astype(jnp.bfloat16)


def attend(positions, query, key_new, value_new, kr, vr):
    rows, heads, dim = query.shape
    m = kr.shape[1]
    big = pl.BlockSpec((1, m, dim), lambda b, p: (b, 0, 0))
    qs = pl.BlockSpec((1, heads, dim), lambda b, p: (b, 0, 0))
    ns = pl.BlockSpec((1, 2, dim), lambda b, p: (b, 0, 0))
    cache = jax.ShapeDtypeStruct(kr.shape, kr.dtype)
    return pl.pallas_call(
        attend_kernel,
        out_shape=[cache, cache, jax.ShapeDtypeStruct(query.shape, query.dtype)],
        grid_spec=pltpu.PrefetchScalarGridSpec(
            num_scalar_prefetch=1, grid=(rows,), in_specs=[qs, ns, ns, big, big], out_specs=[big, big, qs]),
    )(positions, query, key_new, value_new, kr, vr)


def solution(mesh):
    batch_spec = P(('dp', 'cp'))
    seq_spec = P('dp', 'cp')
    whole = P()

    def per_device(x_tok, prompt_lens, k_cache, v_cache, norm_gain, w_q, b_q, w_k, b_k, w_v, b_v, w_o):
        rows = x_tok.shape[0]
        batch, slots, kv_heads, dim = k_cache.shape
        n = batch // rows
        first_row = lax.axis_index('cp') * rows
        positions = lax.dynamic_slice_in_dim(prompt_lens, first_row, rows)
        query, key_new, value_new = project(x_tok, positions, norm_gain, w_q, b_q, w_k, b_k, w_v, b_v, dim)
        kr, vr = exchange(k_cache.reshape(n, rows, slots * kv_heads, dim), v_cache.reshape(n, rows, slots * kv_heads, dim))
        full = n * slots * kv_heads
        k_out, v_out, attended = attend(positions, query, key_new, value_new, kr.reshape(rows, full, dim), vr.reshape(rows, full, dim))
        attended = attended.reshape(rows, -1)
        y_out = (x_tok.astype(jnp.float32) + jnp.dot(attended, w_o, preferred_element_type=jnp.float32)).astype(jnp.bfloat16)
        shape = (rows, n * slots, kv_heads, dim)
        return y_out, k_out.reshape(shape), v_out.reshape(shape)

    return jax.shard_map(per_device, mesh=mesh, in_specs=(batch_spec, P('dp'), seq_spec, seq_spec, whole, whole, whole, whole, whole, whole, whole, whole), out_specs=(batch_spec, batch_spec, batch_spec), check_vma=False)
```

```python
import functools
import numpy as np
import jax
import jax.numpy as jnp
from jax import lax
from jax.experimental import pallas as pl
from jax.experimental.pallas import tpu as pltpu
from jax.sharding import PartitionSpec as P

RMS_EPS = 1e-6
ROPE_THETA = 1000000.0
MESH = pl.DeviceIdType.MESH
F32 = jnp.float32
BF16 = jnp.bfloat16


def flip(me, d):
    out = 0
    for k in range(4):
        bit = 1 << k
        out = out + bit * lax.rem(lax.div(me, bit) + lax.div(d, bit), 2)
    return out


def step_kernel(n, lens_ref, freq_ref, x_ref, gain_ref, bq_ref, bk_ref, bv_ref, wq_ref, wk_ref, wv_ref, wo_ref, k_ref, v_ref,
                att_ref, ko_ref, vo_ref, wo,
                k_land, v_land, wq, wk, wv, xs, gain, bq, bk, bv,
                q_s, kn_s, vn_s, s_s, e_s, l_s, acc, send_sem, recv_sem, load_sem):
    me = lax.axis_index("cp")
    rows, heads, dim = q_s.shape
    m = k_land.shape[2]
    width = heads * dim
    loads = {}
    for idx, (name, src, dst) in enumerate([
            ("x", x_ref, xs), ("gain", gain_ref, gain), ("bq", bq_ref, bq), ("bk", bk_ref, bk), ("bv", bv_ref, bv),
            ("wk", wk_ref, wk), ("wv", wv_ref, wv), ("wq", wq_ref, wq),
            ("k", k_ref.at[me], k_land.at[:, me]), ("v", v_ref.at[me], v_land.at[:, me]), ("wo", wo_ref, wo)]):
        loads[name] = pltpu.make_async_copy(src, dst, load_sem.at[idx])

    barrier = pltpu.get_barrier_semaphore()
    for d in range(1, n):
        pl.semaphore_signal(barrier, inc=1, device_id={"cp": lax.rem(me + d, n)}, device_id_type=MESH)
    for copy in loads.values():
        copy.start()
    pl.semaphore_wait(barrier, n - 1)

    pairs = ((k_ref, k_land), (v_ref, v_land))

    def send(a, d):
        to = flip(me, d)
        return pltpu.make_async_remote_copy(
            src_ref=pairs[a][0].at[to], dst_ref=pairs[a][1].at[:, me], send_sem=send_sem.at[a, d], recv_sem=recv_sem.at[a, me],
            device_id={"cp": to}, device_id_type=MESH)

    def arrive(a, d):
        src = flip(me, d)
        pltpu.make_async_remote_copy(
            src_ref=pairs[a][0].at[0], dst_ref=pairs[a][1].at[:, src], send_sem=send_sem.at[a, d], recv_sem=recv_sem.at[a, src],
            device_id={"cp": src}, device_id_type=MESH).wait_recv()
        return src

    order = (4, 5, 6, 7, 8, 9, 10, 11, 12, 13, 14, 15, 1, 2, 3)
    for a in range(2):
        for d in order:
            send(a, d).start()

    pos = [lens_ref[me * rows + b] for b in range(rows)]

    for name in ("x", "gain", "bq", "bk", "bv", "wk", "wv", "wq"):
        loads[name].wait()
    wide = xs[...].astype(F32)
    inv = lax.rsqrt(jnp.mean(wide * wide, axis=-1, keepdims=True) + RMS_EPS)
    gains = jnp.concatenate([gain[h:h + 1, :].astype(F32) for h in range(heads)], axis=1)
    normed = (wide * inv * gains).astype(BF16)
    which = lax.broadcasted_iota(jnp.int32, (rows, dim), 0)
    lane = lax.broadcasted_iota(jnp.int32, (rows, dim), 1)
    posf = jnp.zeros((rows, dim), F32)
    for b in range(rows):
        posf = jnp.where(which == b, pos[b].astype(F32), posf)
    angle = posf * freq_ref[...]
    cos_t = jnp.cos(angle)
    sin_t = jnp.sin(angle)
    sin_t = jnp.where(lane < dim // 2, -sin_t, sin_t)

    def rotate(t):
        return (t * cos_t + pltpu.roll(t, dim // 2, 1) * sin_t).astype(BF16).astype(F32)

    for h in range(2):
        cols = pl.ds(h * dim, dim)
        kn_s[:, h, :] = rotate(jnp.dot(normed, wk[:, cols], preferred_element_type=F32) + bk[h:h + 1, :].astype(F32))
        vn_s[:, h, :] = (jnp.dot(normed, wv[:, cols], preferred_element_type=F32) + bv[h:h + 1, :].astype(F32)).astype(BF16).astype(F32)
    for h in range(heads):
        q_s[:, h, :] = rotate(jnp.dot(normed, wq[:, h * dim:(h + 1) * dim], preferred_element_type=F32) + bq[h:h + 1, :].astype(F32))

    row = lax.broadcasted_iota(jnp.int32, (m, dim), 0)
    even = lax.rem(row, 2) == 0

    def merge(land, new, out, b, i):
        at = 2 * pos[b] - i * m
        fresh = jnp.where(even, new[b, 0:1, :], new[b, 1:2, :])
        merged = jnp.where(row < at, land[b, i].astype(F32), jnp.where(row < at + 2, fresh, 0.0)).astype(BF16)
        out[b, i] = merged
        return merged

    def k_block(i):
        cols = pl.ds(pl.multiple_of(i * m, m), m)
        for b in range(rows):
            keys = merge(k_land, kn_s, ko_ref, b, i)
            s_s[b, :, cols] = lax.dot_general(q_s[b].astype(BF16), keys, (((1,), (1,)), ((), ())), preferred_element_type=F32) * (dim ** -0.5)

    def v_block(i):
        cols = pl.ds(pl.multiple_of(i * m, m), m)
        for b in range(rows):
            vals = merge(v_land, vn_s, vo_ref, b, i)
            acc[b] += jnp.dot(e_s[b, :, cols], vals, preferred_element_type=F32)

    def k_step(d, c):
        k_block(arrive(0, d))
        return c

    def v_step(d, c):
        v_block(arrive(1, d))
        return c

    loads["k"].wait()
    k_block(me)
    lax.fori_loop(1, n, k_step, 0)

    col = lax.broadcasted_iota(jnp.int32, (heads, n * m), 1)
    head = lax.broadcasted_iota(jnp.int32, (heads, n * m), 0)
    mine = lax.rem(col, 2) == lax.div(head, heads // 2)
    for b in range(rows):
        valid = mine & (col < 2 * pos[b] + 2)
        s = jnp.where(valid, s_s[b], -1e30)
        e = jnp.where(valid, jnp.exp(s - jnp.max(s, axis=-1, keepdims=True)), 0.0)
        l_s[b] = jnp.broadcast_to(jnp.sum(e, axis=-1, keepdims=True), (heads, dim))
        e_s[b] = e.astype(BF16)
    acc[...] = jnp.zeros_like(acc)

    loads["v"].wait()
    v_block(me)
    loads["wo"].wait()
    lax.fori_loop(1, n, v_step, 0)

    acc[...] = acc[...] / l_s[...]
    att_ref[...] = jnp.concatenate([acc[:, h, :] for h in range(heads)], axis=1).astype(BF16)

    for a in range(2):
        for d in order:
            send(a, d).wait_send()


def step(lens, freq, x, gain, b_q, b_k, b_v, w_q, w_k, w_v, w_o, k, v):
    n, rows, m, dim = k.shape
    heads = w_q.shape[1] // dim
    kv = w_k.shape[1] // dim
    cache = pltpu.VMEM((rows, n, m, dim), BF16)
    hbm = pl.BlockSpec(memory_space=pltpu.HBM)
    vmem = pl.BlockSpec(memory_space=pltpu.VMEM)
    return pl.pallas_call(
        functools.partial(step_kernel, n),
        out_shape=[pltpu.VMEM(x.shape, BF16), cache, cache, pltpu.VMEM(w_o.shape, BF16)],
        in_specs=[pl.BlockSpec(memory_space=pltpu.SMEM), vmem] + [hbm] * 11,
        out_specs=[vmem] * 4,
        scratch_shapes=[
            pltpu.VMEM((rows, n, m, dim), BF16), pltpu.VMEM((rows, n, m, dim), BF16),
            pltpu.VMEM(w_q.shape, BF16), pltpu.VMEM(w_k.shape, BF16), pltpu.VMEM(w_v.shape, BF16),
            pltpu.VMEM(x.shape, BF16), pltpu.VMEM(gain.shape, BF16), pltpu.VMEM(b_q.shape, BF16), pltpu.VMEM(b_k.shape, BF16), pltpu.VMEM(b_v.shape, BF16),
            pltpu.VMEM((rows, heads, dim), F32), pltpu.VMEM((rows, kv, dim), F32), pltpu.VMEM((rows, kv, dim), F32),
            pltpu.VMEM((rows, heads, n * m), F32), pltpu.VMEM((rows, heads, n * m), BF16), pltpu.VMEM((rows, heads, dim), F32),
            pltpu.VMEM((rows, heads, dim), F32),
            pltpu.SemaphoreType.DMA((2, n)), pltpu.SemaphoreType.DMA((2, n)), pltpu.SemaphoreType.DMA((11,))],
        compiler_params=pltpu.CompilerParams(collective_id=0, has_side_effects=True, vmem_limit_bytes=47 * 1024 * 1024),
    )(lens, freq, x, gain, b_q, b_k, b_v, w_q, w_k, w_v, w_o, k, v)


def finish_kernel(x_ref, att_ref, wo_ref, k_ref, v_ref, y_ref, ko_ref, vo_ref, sem):
    copies = [pltpu.make_async_copy(k_ref, ko_ref, sem.at[0]), pltpu.make_async_copy(v_ref, vo_ref, sem.at[1])]
    for copy in copies:
        copy.start()
    tile = 256
    for t in range(wo_ref.shape[1] // tile):
        cols = slice(t * tile, (t + 1) * tile)
        y_ref[:, cols] = (x_ref[:, cols].astype(F32) + jnp.dot(att_ref[...], wo_ref[:, cols], preferred_element_type=F32)).astype(BF16)
    for copy in copies:
        copy.wait()


def finish(x, att, w_o, k, v):
    vmem = pl.BlockSpec(memory_space=pltpu.VMEM)
    hbm = pl.BlockSpec(memory_space=pltpu.HBM)
    cache = jax.ShapeDtypeStruct(k.shape, BF16)
    return pl.pallas_call(
        finish_kernel,
        out_shape=[jax.ShapeDtypeStruct(x.shape, BF16), cache, cache],
        in_specs=[vmem] * 5,
        out_specs=[vmem, hbm, hbm],
        scratch_shapes=[pltpu.SemaphoreType.DMA((2,))],
        compiler_params=pltpu.CompilerParams(vmem_limit_bytes=4 * 1024 * 1024),
    )(x, att, w_o, k, v)


def solution(mesh):
    batch_spec = P(('dp', 'cp'))
    seq_spec = P('dp', 'cp')
    whole = P()

    def per_device(x_tok, prompt_lens, k_cache, v_cache, norm_gain, w_q, b_q, w_k, b_k, w_v, b_v, w_o):
        rows = x_tok.shape[0]
        batch, slots, kv_heads, dim = k_cache.shape
        n = batch // rows
        inv_freq = np.power(np.float32(ROPE_THETA), -(np.arange(dim // 2, dtype=np.float32) * 2.0 / dim)).astype(np.float32)
        freq = jnp.asarray(np.concatenate([inv_freq, inv_freq])[None, :])
        pack = (n, rows, slots * kv_heads, dim)
        att, k_all, v_all, wo = step(
            prompt_lens, freq, x_tok, norm_gain.reshape(-1, dim), b_q.reshape(-1, dim), b_k.reshape(-1, dim), b_v.reshape(-1, dim),
            w_q, w_k, w_v, w_o, k_cache.reshape(pack), v_cache.reshape(pack))
        y_out, k_out, v_out = finish(x_tok, att, wo, k_all, v_all)
        shape = (rows, n * slots, kv_heads, dim)
        return y_out, k_out.reshape(shape), v_out.reshape(shape)

    return jax.shard_map(per_device, mesh=mesh, in_specs=(batch_spec, P('dp'), seq_spec, seq_spec, whole, whole, whole, whole, whole, whole, whole, whole), out_specs=(batch_spec, batch_spec, batch_spec), check_vma=False)
```

```python
import functools
import numpy as np
import jax
import jax.numpy as jnp
from jax import lax
from jax.experimental import pallas as pl
from jax.experimental.pallas import tpu as pltpu
from jax.sharding import PartitionSpec as P

RMS_EPS = 1e-6
ROPE_THETA = 1000000.0
MESH = pl.DeviceIdType.MESH
F32 = jnp.float32
BF16 = jnp.bfloat16


def flip(me, d):
    out = 0
    for k in range(4):
        bit = 1 << k
        out = out + bit * lax.rem(lax.div(me, bit) + lax.div(d, bit), 2)
    return out


def step_kernel(n, lens_ref, freq_ref, x_ref, gain_ref, bq_ref, bk_ref, bv_ref, wq_ref, wk_ref, wv_ref, wo_ref, k_ref, v_ref,
                att_ref, ko_ref, vo_ref, wo,
                k_land, v_land, wq, wk, wv, xs, gain, bq, bk, bv,
                q_s, kn_s, vn_s, s_s, e_s, l_s, acc, send_sem, recv_sem, load_sem):
    me = lax.axis_index("cp")
    rows, heads, dim = q_s.shape
    m = k_land.shape[2]
    width = heads * dim
    loads = {}
    for idx, (name, src, dst) in enumerate([
            ("x", x_ref, xs), ("gain", gain_ref, gain), ("bq", bq_ref, bq), ("bk", bk_ref, bk), ("bv", bv_ref, bv),
            ("wk", wk_ref, wk), ("wv", wv_ref, wv), ("wq", wq_ref, wq),
            ("k", k_ref.at[me], k_land.at[:, me]), ("v", v_ref.at[me], v_land.at[:, me]), ("wo", wo_ref, wo)]):
        loads[name] = pltpu.make_async_copy(src, dst, load_sem.at[idx])

    barrier = pltpu.get_barrier_semaphore()
    for d in range(1, n):
        pl.semaphore_signal(barrier, inc=1, device_id={"cp": lax.rem(me + d, n)}, device_id_type=MESH)
    for copy in loads.values():
        copy.start()
    pl.semaphore_wait(barrier, n - 1)

    pairs = ((k_ref, k_land), (v_ref, v_land))

    def send(a, d):
        to = flip(me, d)
        return pltpu.make_async_remote_copy(
            src_ref=pairs[a][0].at[to], dst_ref=pairs[a][1].at[:, me], send_sem=send_sem.at[a, d], recv_sem=recv_sem.at[a, me],
            device_id={"cp": to}, device_id_type=MESH)

    def arrive(a, d):
        src = flip(me, d)
        pltpu.make_async_remote_copy(
            src_ref=pairs[a][0].at[0], dst_ref=pairs[a][1].at[:, src], send_sem=send_sem.at[a, d], recv_sem=recv_sem.at[a, src],
            device_id={"cp": src}, device_id_type=MESH).wait_recv()
        return src

    order = (8, 9, 4, 10, 11, 5, 12, 13, 6, 14, 15, 7, 1, 2, 3)
    for a in range(2):
        for d in order:
            send(a, d).start()

    pos = [lens_ref[me * rows + b] for b in range(rows)]

    for name in ("x", "gain", "bq", "bk", "bv", "wk", "wv", "wq"):
        loads[name].wait()
    wide = xs[...].astype(F32)
    inv = lax.rsqrt(jnp.mean(wide * wide, axis=-1, keepdims=True) + RMS_EPS)
    gains = jnp.concatenate([gain[h:h + 1, :].astype(F32) for h in range(heads)], axis=1)
    normed = (wide * inv * gains).astype(BF16)
    which = lax.broadcasted_iota(jnp.int32, (rows, dim), 0)
    lane = lax.broadcasted_iota(jnp.int32, (rows, dim), 1)
    posf = jnp.zeros((rows, dim), F32)
    for b in range(rows):
        posf = jnp.where(which == b, pos[b].astype(F32), posf)
    angle = posf * freq_ref[...]
    cos_t = jnp.cos(angle)
    sin_t = jnp.sin(angle)
    sin_t = jnp.where(lane < dim // 2, -sin_t, sin_t)

    def rotate(t):
        return (t * cos_t + pltpu.roll(t, dim // 2, 1) * sin_t).astype(BF16).astype(F32)

    for h in range(2):
        cols = pl.ds(h * dim, dim)
        kn_s[:, h, :] = rotate(jnp.dot(normed, wk[:, cols], preferred_element_type=F32) + bk[h:h + 1, :].astype(F32))
        vn_s[:, h, :] = (jnp.dot(normed, wv[:, cols], preferred_element_type=F32) + bv[h:h + 1, :].astype(F32)).astype(BF16).astype(F32)
    for h in range(heads):
        q_s[:, h, :] = rotate(jnp.dot(normed, wq[:, h * dim:(h + 1) * dim], preferred_element_type=F32) + bq[h:h + 1, :].astype(F32))

    row = lax.broadcasted_iota(jnp.int32, (m, dim), 0)
    even = lax.rem(row, 2) == 0

    def merge(land, new, out, b, i):
        at = 2 * pos[b] - i * m
        fresh = jnp.where(even, new[b, 0:1, :], new[b, 1:2, :])
        merged = jnp.where(row < at, land[b, i].astype(F32), jnp.where(row < at + 2, fresh, 0.0)).astype(BF16)
        out[b, i] = merged
        return merged

    def k_block(i):
        cols = pl.ds(pl.multiple_of(i * m, m), m)
        for b in range(rows):
            keys = merge(k_land, kn_s, ko_ref, b, i)
            s_s[b, :, cols] = lax.dot_general(q_s[b].astype(BF16), keys, (((1,), (1,)), ((), ())), preferred_element_type=F32) * (dim ** -0.5)

    def v_block(i):
        cols = pl.ds(pl.multiple_of(i * m, m), m)
        for b in range(rows):
            vals = merge(v_land, vn_s, vo_ref, b, i)
            acc[b] += jnp.dot(e_s[b, :, cols], vals, preferred_element_type=F32)

    def k_step(d, c):
        k_block(arrive(0, d))
        return c

    def v_step(d, c):
        v_block(arrive(1, d))
        return c

    loads["k"].wait()
    k_block(me)
    lax.fori_loop(1, n, k_step, 0)

    col = lax.broadcasted_iota(jnp.int32, (heads, n * m), 1)
    head = lax.broadcasted_iota(jnp.int32, (heads, n * m), 0)
    mine = lax.rem(col, 2) == lax.div(head, heads // 2)
    for b in range(rows):
        valid = mine & (col < 2 * pos[b] + 2)
        s = jnp.where(valid, s_s[b], -1e30)
        e = jnp.where(valid, jnp.exp(s - jnp.max(s, axis=-1, keepdims=True)), 0.0)
        l_s[b] = jnp.broadcast_to(jnp.sum(e, axis=-1, keepdims=True), (heads, dim))
        e_s[b] = e.astype(BF16)
    acc[...] = jnp.zeros_like(acc)

    loads["v"].wait()
    v_block(me)
    loads["wo"].wait()
    lax.fori_loop(1, n, v_step, 0)

    acc[...] = acc[...] / l_s[...]
    att_ref[...] = jnp.concatenate([acc[:, h, :] for h in range(heads)], axis=1).astype(BF16)

    for a in range(2):
        for d in order:
            send(a, d).wait_send()


def step(lens, freq, x, gain, b_q, b_k, b_v, w_q, w_k, w_v, w_o, k, v):
    n, rows, m, dim = k.shape
    heads = w_q.shape[1] // dim
    kv = w_k.shape[1] // dim
    cache = pltpu.VMEM((rows, n, m, dim), BF16)
    hbm = pl.BlockSpec(memory_space=pltpu.HBM)
    vmem = pl.BlockSpec(memory_space=pltpu.VMEM)
    return pl.pallas_call(
        functools.partial(step_kernel, n),
        out_shape=[pltpu.VMEM(x.shape, BF16), cache, cache, pltpu.VMEM(w_o.shape, BF16)],
        in_specs=[pl.BlockSpec(memory_space=pltpu.SMEM), vmem] + [hbm] * 11,
        out_specs=[vmem] * 4,
        scratch_shapes=[
            pltpu.VMEM((rows, n, m, dim), BF16), pltpu.VMEM((rows, n, m, dim), BF16),
            pltpu.VMEM(w_q.shape, BF16), pltpu.VMEM(w_k.shape, BF16), pltpu.VMEM(w_v.shape, BF16),
            pltpu.VMEM(x.shape, BF16), pltpu.VMEM(gain.shape, BF16), pltpu.VMEM(b_q.shape, BF16), pltpu.VMEM(b_k.shape, BF16), pltpu.VMEM(b_v.shape, BF16),
            pltpu.VMEM((rows, heads, dim), F32), pltpu.VMEM((rows, kv, dim), F32), pltpu.VMEM((rows, kv, dim), F32),
            pltpu.VMEM((rows, heads, n * m), F32), pltpu.VMEM((rows, heads, n * m), BF16), pltpu.VMEM((rows, heads, dim), F32),
            pltpu.VMEM((rows, heads, dim), F32),
            pltpu.SemaphoreType.DMA((2, n)), pltpu.SemaphoreType.DMA((2, n)), pltpu.SemaphoreType.DMA((11,))],
        compiler_params=pltpu.CompilerParams(collective_id=0, has_side_effects=True, vmem_limit_bytes=47 * 1024 * 1024),
    )(lens, freq, x, gain, b_q, b_k, b_v, w_q, w_k, w_v, w_o, k, v)


def finish_kernel(x_ref, att_ref, wo_ref, k_ref, v_ref, y_ref, ko_ref, vo_ref, sem):
    copies = [pltpu.make_async_copy(k_ref, ko_ref, sem.at[0]), pltpu.make_async_copy(v_ref, vo_ref, sem.at[1])]
    for copy in copies:
        copy.start()
    tile = 256
    for t in range(wo_ref.shape[1] // tile):
        cols = slice(t * tile, (t + 1) * tile)
        y_ref[:, cols] = (x_ref[:, cols].astype(F32) + jnp.dot(att_ref[...], wo_ref[:, cols], preferred_element_type=F32)).astype(BF16)
    for copy in copies:
        copy.wait()


def finish(x, att, w_o, k, v):
    vmem = pl.BlockSpec(memory_space=pltpu.VMEM)
    hbm = pl.BlockSpec(memory_space=pltpu.HBM)
    cache = jax.ShapeDtypeStruct(k.shape, BF16)
    return pl.pallas_call(
        finish_kernel,
        out_shape=[jax.ShapeDtypeStruct(x.shape, BF16), cache, cache],
        in_specs=[vmem] * 5,
        out_specs=[vmem, hbm, hbm],
        scratch_shapes=[pltpu.SemaphoreType.DMA((2,))],
        compiler_params=pltpu.CompilerParams(vmem_limit_bytes=4 * 1024 * 1024),
    )(x, att, w_o, k, v)


def solution(mesh):
    batch_spec = P(('dp', 'cp'))
    seq_spec = P('dp', 'cp')
    whole = P()

    def per_device(x_tok, prompt_lens, k_cache, v_cache, norm_gain, w_q, b_q, w_k, b_k, w_v, b_v, w_o):
        rows = x_tok.shape[0]
        batch, slots, kv_heads, dim = k_cache.shape
        n = batch // rows
        inv_freq = np.power(np.float32(ROPE_THETA), -(np.arange(dim // 2, dtype=np.float32) * 2.0 / dim)).astype(np.float32)
        freq = jnp.asarray(np.concatenate([inv_freq, inv_freq])[None, :])
        pack = (n, rows, slots * kv_heads, dim)
        att, k_all, v_all, wo = step(
            prompt_lens, freq, x_tok, norm_gain.reshape(-1, dim), b_q.reshape(-1, dim), b_k.reshape(-1, dim), b_v.reshape(-1, dim),
            w_q, w_k, w_v, w_o, k_cache.reshape(pack), v_cache.reshape(pack))
        y_out, k_out, v_out = finish(x_tok, att, wo, k_all, v_all)
        shape = (rows, n * slots, kv_heads, dim)
        return y_out, k_out.reshape(shape), v_out.reshape(shape)

    return jax.shard_map(per_device, mesh=mesh, in_specs=(batch_spec, P('dp'), seq_spec, seq_spec, whole, whole, whole, whole, whole, whole, whole, whole), out_specs=(batch_spec, batch_spec, batch_spec), check_vma=False)
```

```python
import functools
import numpy as np
import jax
import jax.numpy as jnp
from jax import lax
from jax.experimental import pallas as pl
from jax.experimental.pallas import tpu as pltpu
from jax.sharding import PartitionSpec as P

RMS_EPS = 1e-6
ROPE_THETA = 1000000.0
MESH = pl.DeviceIdType.MESH
F32 = jnp.float32
BF16 = jnp.bfloat16


def flip(me, d):
    out = 0
    for k in range(4):
        bit = 1 << k
        out = out + bit * lax.rem(lax.div(me, bit) + lax.div(d, bit), 2)
    return out


def step_kernel(n, lens_ref, freq_ref, x_ref, gain_ref, bq_ref, bk_ref, bv_ref, wq_ref, wk_ref, wv_ref, wo_ref, k_ref, v_ref,
                att_ref, ko_ref, vo_ref, wo,
                k_land, v_land, wq, wk, wv, xs, gain, bq, bk, bv,
                q_s, kn_s, vn_s, s_s, e_s, l_s, acc, send_sem, recv_sem, load_sem):
    me = lax.axis_index("cp")
    rows, heads, dim = q_s.shape
    m = k_land.shape[2]
    width = heads * dim
    loads = {}
    for idx, (name, src, dst) in enumerate([
            ("x", x_ref, xs), ("gain", gain_ref, gain), ("bq", bq_ref, bq), ("bk", bk_ref, bk), ("bv", bv_ref, bv),
            ("wk", wk_ref, wk), ("wv", wv_ref, wv), ("wq", wq_ref, wq),
            ("k", k_ref.at[me], k_land.at[:, me]), ("v", v_ref.at[me], v_land.at[:, me]), ("wo", wo_ref, wo)]):
        loads[name] = pltpu.make_async_copy(src, dst, load_sem.at[idx])

    barrier = pltpu.get_barrier_semaphore()
    for d in range(1, n):
        pl.semaphore_signal(barrier, inc=1, device_id={"cp": lax.rem(me + d, n)}, device_id_type=MESH)
    for copy in loads.values():
        copy.start()
    pl.semaphore_wait(barrier, n - 1)

    pairs = ((k_ref, k_land), (v_ref, v_land))

    def send(a, d):
        to = flip(me, d)
        return pltpu.make_async_remote_copy(
            src_ref=pairs[a][0].at[to], dst_ref=pairs[a][1].at[:, me], send_sem=send_sem.at[a, d], recv_sem=recv_sem.at[a, me],
            device_id={"cp": to}, device_id_type=MESH)

    def arrive(a, d):
        src = flip(me, d)
        pltpu.make_async_remote_copy(
            src_ref=pairs[a][0].at[0], dst_ref=pairs[a][1].at[:, src], send_sem=send_sem.at[a, d], recv_sem=recv_sem.at[a, src],
            device_id={"cp": src}, device_id_type=MESH).wait_recv()
        return src

    near, far, beside = (4, 5, 6, 7), (8, 9, 10, 11, 12, 13, 14, 15), (1, 2, 3)
    plan = [(0, d, d + 8) for d in near] + [(1, d, d + 8) for d in near]
    plan += [(a, d, e) for a in range(2) for d, e in zip(far, (8, 9, 4, 10, 11, 5, 6, 7))]
    plan += [(a, d, d) for a in range(2) for d in beside]
    end = lax.rem(lax.div(lax.div(me, 4) + 1, 2) + 1, 2)
    plan = [(a, e + end * (d - e)) for a, d, e in plan]
    for a, d in plan:
        send(a, d).start()

    pos = [lens_ref[me * rows + b] for b in range(rows)]

    for name in ("x", "gain", "bq", "bk", "bv", "wk", "wv", "wq"):
        loads[name].wait()
    wide = xs[...].astype(F32)
    inv = lax.rsqrt(jnp.mean(wide * wide, axis=-1, keepdims=True) + RMS_EPS)
    gains = jnp.concatenate([gain[h:h + 1, :].astype(F32) for h in range(heads)], axis=1)
    normed = (wide * inv * gains).astype(BF16)
    which = lax.broadcasted_iota(jnp.int32, (rows, dim), 0)
    lane = lax.broadcasted_iota(jnp.int32, (rows, dim), 1)
    posf = jnp.zeros((rows, dim), F32)
    for b in range(rows):
        posf = jnp.where(which == b, pos[b].astype(F32), posf)
    angle = posf * freq_ref[...]
    cos_t = jnp.cos(angle)
    sin_t = jnp.sin(angle)
    sin_t = jnp.where(lane < dim // 2, -sin_t, sin_t)

    def rotate(t):
        return (t * cos_t + pltpu.roll(t, dim // 2, 1) * sin_t).astype(BF16).astype(F32)

    for h in range(2):
        cols = pl.ds(h * dim, dim)
        kn_s[:, h, :] = rotate(jnp.dot(normed, wk[:, cols], preferred_element_type=F32) + bk[h:h + 1, :].astype(F32))
        vn_s[:, h, :] = (jnp.dot(normed, wv[:, cols], preferred_element_type=F32) + bv[h:h + 1, :].astype(F32)).astype(BF16).astype(F32)
    for h in range(heads):
        q_s[:, h, :] = rotate(jnp.dot(normed, wq[:, h * dim:(h + 1) * dim], preferred_element_type=F32) + bq[h:h + 1, :].astype(F32))

    row = lax.broadcasted_iota(jnp.int32, (m, dim), 0)
    even = lax.rem(row, 2) == 0

    def merge(land, new, out, b, i):
        at = 2 * pos[b] - i * m
        fresh = jnp.where(even, new[b, 0:1, :], new[b, 1:2, :])
        merged = jnp.where(row < at, land[b, i].astype(F32), jnp.where(row < at + 2, fresh, 0.0)).astype(BF16)
        out[b, i] = merged
        return merged

    def k_block(i):
        cols = pl.ds(pl.multiple_of(i * m, m), m)
        for b in range(rows):
            keys = merge(k_land, kn_s, ko_ref, b, i)
            s_s[b, :, cols] = lax.dot_general(q_s[b].astype(BF16), keys, (((1,), (1,)), ((), ())), preferred_element_type=F32) * (dim ** -0.5)

    def v_block(i):
        cols = pl.ds(pl.multiple_of(i * m, m), m)
        for b in range(rows):
            vals = merge(v_land, vn_s, vo_ref, b, i)
            acc[b] += jnp.dot(e_s[b, :, cols], vals, preferred_element_type=F32)

    def k_step(d, c):
        k_block(arrive(0, d))
        return c

    def v_step(d, c):
        v_block(arrive(1, d))
        return c

    loads["k"].wait()
    k_block(me)
    lax.fori_loop(1, n, k_step, 0)

    col = lax.broadcasted_iota(jnp.int32, (heads, n * m), 1)
    head = lax.broadcasted_iota(jnp.int32, (heads, n * m), 0)
    mine = lax.rem(col, 2) == lax.div(head, heads // 2)
    for b in range(rows):
        valid = mine & (col < 2 * pos[b] + 2)
        s = jnp.where(valid, s_s[b], -1e30)
        e = jnp.where(valid, jnp.exp(s - jnp.max(s, axis=-1, keepdims=True)), 0.0)
        l_s[b] = jnp.broadcast_to(jnp.sum(e, axis=-1, keepdims=True), (heads, dim))
        e_s[b] = e.astype(BF16)
    acc[...] = jnp.zeros_like(acc)

    loads["v"].wait()
    v_block(me)
    loads["wo"].wait()
    lax.fori_loop(1, n, v_step, 0)

    acc[...] = acc[...] / l_s[...]
    att_ref[...] = jnp.concatenate([acc[:, h, :] for h in range(heads)], axis=1).astype(BF16)

    for a, d in plan:
        send(a, d).wait_send()


def step(lens, freq, x, gain, b_q, b_k, b_v, w_q, w_k, w_v, w_o, k, v):
    n, rows, m, dim = k.shape
    heads = w_q.shape[1] // dim
    kv = w_k.shape[1] // dim
    cache = pltpu.VMEM((rows, n, m, dim), BF16)
    hbm = pl.BlockSpec(memory_space=pltpu.HBM)
    vmem = pl.BlockSpec(memory_space=pltpu.VMEM)
    return pl.pallas_call(
        functools.partial(step_kernel, n),
        out_shape=[pltpu.VMEM(x.shape, BF16), cache, cache, pltpu.VMEM(w_o.shape, BF16)],
        in_specs=[pl.BlockSpec(memory_space=pltpu.SMEM), vmem] + [hbm] * 11,
        out_specs=[vmem] * 4,
        scratch_shapes=[
            pltpu.VMEM((rows, n, m, dim), BF16), pltpu.VMEM((rows, n, m, dim), BF16),
            pltpu.VMEM(w_q.shape, BF16), pltpu.VMEM(w_k.shape, BF16), pltpu.VMEM(w_v.shape, BF16),
            pltpu.VMEM(x.shape, BF16), pltpu.VMEM(gain.shape, BF16), pltpu.VMEM(b_q.shape, BF16), pltpu.VMEM(b_k.shape, BF16), pltpu.VMEM(b_v.shape, BF16),
            pltpu.VMEM((rows, heads, dim), F32), pltpu.VMEM((rows, kv, dim), F32), pltpu.VMEM((rows, kv, dim), F32),
            pltpu.VMEM((rows, heads, n * m), F32), pltpu.VMEM((rows, heads, n * m), BF16), pltpu.VMEM((rows, heads, dim), F32),
            pltpu.VMEM((rows, heads, dim), F32),
            pltpu.SemaphoreType.DMA((2, n)), pltpu.SemaphoreType.DMA((2, n)), pltpu.SemaphoreType.DMA((11,))],
        compiler_params=pltpu.CompilerParams(collective_id=0, has_side_effects=True, vmem_limit_bytes=47 * 1024 * 1024),
    )(lens, freq, x, gain, b_q, b_k, b_v, w_q, w_k, w_v, w_o, k, v)


def finish_kernel(x_ref, att_ref, wo_ref, k_ref, v_ref, y_ref, ko_ref, vo_ref, sem):
    copies = [pltpu.make_async_copy(k_ref, ko_ref, sem.at[0]), pltpu.make_async_copy(v_ref, vo_ref, sem.at[1])]
    for copy in copies:
        copy.start()
    tile = 256
    for t in range(wo_ref.shape[1] // tile):
        cols = slice(t * tile, (t + 1) * tile)
        y_ref[:, cols] = (x_ref[:, cols].astype(F32) + jnp.dot(att_ref[...], wo_ref[:, cols], preferred_element_type=F32)).astype(BF16)
    for copy in copies:
        copy.wait()


def finish(x, att, w_o, k, v):
    vmem = pl.BlockSpec(memory_space=pltpu.VMEM)
    hbm = pl.BlockSpec(memory_space=pltpu.HBM)
    cache = jax.ShapeDtypeStruct(k.shape, BF16)
    return pl.pallas_call(
        finish_kernel,
        out_shape=[jax.ShapeDtypeStruct(x.shape, BF16), cache, cache],
        in_specs=[vmem] * 5,
        out_specs=[vmem, hbm, hbm],
        scratch_shapes=[pltpu.SemaphoreType.DMA((2,))],
        compiler_params=pltpu.CompilerParams(vmem_limit_bytes=4 * 1024 * 1024),
    )(x, att, w_o, k, v)


def solution(mesh):
    batch_spec = P(('dp', 'cp'))
    seq_spec = P('dp', 'cp')
    whole = P()

    def per_device(x_tok, prompt_lens, k_cache, v_cache, norm_gain, w_q, b_q, w_k, b_k, w_v, b_v, w_o):
        rows = x_tok.shape[0]
        batch, slots, kv_heads, dim = k_cache.shape
        n = batch // rows
        inv_freq = np.power(np.float32(ROPE_THETA), -(np.arange(dim // 2, dtype=np.float32) * 2.0 / dim)).astype(np.float32)
        freq = jnp.asarray(np.concatenate([inv_freq, inv_freq])[None, :])
        pack = (n, rows, slots * kv_heads, dim)
        att, k_all, v_all, wo = step(
            prompt_lens, freq, x_tok, norm_gain.reshape(-1, dim), b_q.reshape(-1, dim), b_k.reshape(-1, dim), b_v.reshape(-1, dim),
            w_q, w_k, w_v, w_o, k_cache.reshape(pack), v_cache.reshape(pack))
        y_out, k_out, v_out = finish(x_tok, att, wo, k_all, v_all)
        shape = (rows, n * slots, kv_heads, dim)
        return y_out, k_out.reshape(shape), v_out.reshape(shape)

    return jax.shard_map(per_device, mesh=mesh, in_specs=(batch_spec, P('dp'), seq_spec, seq_spec, whole, whole, whole, whole, whole, whole, whole, whole), out_specs=(batch_spec, batch_spec, batch_spec), check_vma=False)
```

```python
import functools
import numpy as np
import jax
import jax.numpy as jnp
from jax import lax
from jax.experimental import pallas as pl
from jax.experimental.pallas import tpu as pltpu
from jax.sharding import PartitionSpec as P

RMS_EPS = 1e-6
ROPE_THETA = 1000000.0
MESH = pl.DeviceIdType.MESH
F32 = jnp.float32
BF16 = jnp.bfloat16


def flip(me, d):
    out = 0
    for k in range(4):
        bit = 1 << k
        out = out + bit * lax.rem(lax.div(me, bit) + lax.div(d, bit), 2)
    return out


def step_kernel(n, lens_ref, freq_ref, x_ref, gain_ref, bq_ref, bk_ref, bv_ref, wq_ref, wk_ref, wv_ref, wo_ref, k_ref, v_ref,
                att_ref, ko_ref, vo_ref, wo,
                k_land, v_land, wq, wk, wv, xs, gain, bq, bk, bv,
                q_s, kn_s, vn_s, s_s, e_s, l_s, acc, send_sem, recv_sem, load_sem):
    me = lax.axis_index("cp")
    rows, heads, dim = q_s.shape
    m = k_land.shape[2]
    width = heads * dim
    loads = {}
    for idx, (name, src, dst) in enumerate([
            ("x", x_ref, xs), ("gain", gain_ref, gain), ("bq", bq_ref, bq), ("bk", bk_ref, bk), ("bv", bv_ref, bv),
            ("wk", wk_ref, wk), ("wv", wv_ref, wv), ("wq", wq_ref, wq),
            ("k", k_ref.at[me], k_land.at[:, me]), ("v", v_ref.at[me], v_land.at[:, me]), ("wo", wo_ref, wo)]):
        loads[name] = pltpu.make_async_copy(src, dst, load_sem.at[idx])

    barrier = pltpu.get_barrier_semaphore()
    for d in range(1, n):
        pl.semaphore_signal(barrier, inc=1, device_id={"cp": lax.rem(me + d, n)}, device_id_type=MESH)
    for copy in loads.values():
        copy.start()
    pl.semaphore_wait(barrier, n - 1)

    pairs = ((k_ref, k_land), (v_ref, v_land))

    def send(a, d):
        to = lax.rem(me + d, n)
        return pltpu.make_async_remote_copy(
            src_ref=pairs[a][0].at[to], dst_ref=pairs[a][1].at[:, me], send_sem=send_sem.at[a, d], recv_sem=recv_sem.at[a, me],
            device_id={"cp": to}, device_id_type=MESH)

    def arrive(a, d):
        src = lax.rem(me + n - d, n)
        pltpu.make_async_remote_copy(
            src_ref=pairs[a][0].at[0], dst_ref=pairs[a][1].at[:, src], send_sem=send_sem.at[a, d], recv_sem=recv_sem.at[a, src],
            device_id={"cp": src}, device_id_type=MESH).wait_recv()
        return src

    plan = [(a, d) for d in range(1, n) for a in range(2)]
    for a, d in plan:
        send(a, d).start()

    pos = [lens_ref[me * rows + b] for b in range(rows)]

    for name in ("x", "gain", "bq", "bk", "bv", "wk", "wv", "wq"):
        loads[name].wait()
    wide = xs[...].astype(F32)
    inv = lax.rsqrt(jnp.mean(wide * wide, axis=-1, keepdims=True) + RMS_EPS)
    gains = jnp.concatenate([gain[h:h + 1, :].astype(F32) for h in range(heads)], axis=1)
    normed = (wide * inv * gains).astype(BF16)
    which = lax.broadcasted_iota(jnp.int32, (rows, dim), 0)
    lane = lax.broadcasted_iota(jnp.int32, (rows, dim), 1)
    posf = jnp.zeros((rows, dim), F32)
    for b in range(rows):
        posf = jnp.where(which == b, pos[b].astype(F32), posf)
    angle = posf * freq_ref[...]
    cos_t = jnp.cos(angle)
    sin_t = jnp.sin(angle)
    sin_t = jnp.where(lane < dim // 2, -sin_t, sin_t)

    def rotate(t):
        return (t * cos_t + pltpu.roll(t, dim // 2, 1) * sin_t).astype(BF16).astype(F32)

    for h in range(2):
        cols = pl.ds(h * dim, dim)
        kn_s[:, h, :] = rotate(jnp.dot(normed, wk[:, cols], preferred_element_type=F32) + bk[h:h + 1, :].astype(F32))
        vn_s[:, h, :] = (jnp.dot(normed, wv[:, cols], preferred_element_type=F32) + bv[h:h + 1, :].astype(F32)).astype(BF16).astype(F32)
    for h in range(heads):
        q_s[:, h, :] = rotate(jnp.dot(normed, wq[:, h * dim:(h + 1) * dim], preferred_element_type=F32) + bq[h:h + 1, :].astype(F32))

    row = lax.broadcasted_iota(jnp.int32, (m, dim), 0)
    even = lax.rem(row, 2) == 0

    def merge(land, new, out, b, i):
        at = 2 * pos[b] - i * m
        fresh = jnp.where(even, new[b, 0:1, :], new[b, 1:2, :])
        merged = jnp.where(row < at, land[b, i].astype(F32), jnp.where(row < at + 2, fresh, 0.0)).astype(BF16)
        out[b, i] = merged
        return merged

    def k_block(i):
        cols = pl.ds(pl.multiple_of(i * m, m), m)
        for b in range(rows):
            keys = merge(k_land, kn_s, ko_ref, b, i)
            s_s[b, :, cols] = lax.dot_general(q_s[b].astype(BF16), keys, (((1,), (1,)), ((), ())), preferred_element_type=F32) * (dim ** -0.5)

    def v_block(i):
        cols = pl.ds(pl.multiple_of(i * m, m), m)
        for b in range(rows):
            vals = merge(v_land, vn_s, vo_ref, b, i)
            acc[b] += jnp.dot(e_s[b, :, cols], vals, preferred_element_type=F32)

    def k_step(d, c):
        k_block(arrive(0, d))
        return c

    def v_step(d, c):
        v_block(arrive(1, d))
        return c

    loads["k"].wait()
    k_block(me)
    lax.fori_loop(1, n, k_step, 0)

    col = lax.broadcasted_iota(jnp.int32, (heads, n * m), 1)
    head = lax.broadcasted_iota(jnp.int32, (heads, n * m), 0)
    mine = lax.rem(col, 2) == lax.div(head, heads // 2)
    for b in range(rows):
        valid = mine & (col < 2 * pos[b] + 2)
        s = jnp.where(valid, s_s[b], -1e30)
        e = jnp.where(valid, jnp.exp(s - jnp.max(s, axis=-1, keepdims=True)), 0.0)
        l_s[b] = jnp.broadcast_to(jnp.sum(e, axis=-1, keepdims=True), (heads, dim))
        e_s[b] = e.astype(BF16)
    acc[...] = jnp.zeros_like(acc)

    loads["v"].wait()
    v_block(me)
    loads["wo"].wait()
    lax.fori_loop(1, n, v_step, 0)

    acc[...] = acc[...] / l_s[...]
    att_ref[...] = jnp.concatenate([acc[:, h, :] for h in range(heads)], axis=1).astype(BF16)

    for a, d in plan:
        send(a, d).wait_send()


def step(lens, freq, x, gain, b_q, b_k, b_v, w_q, w_k, w_v, w_o, k, v):
    n, rows, m, dim = k.shape
    heads = w_q.shape[1] // dim
    kv = w_k.shape[1] // dim
    cache = pltpu.VMEM((rows, n, m, dim), BF16)
    hbm = pl.BlockSpec(memory_space=pltpu.HBM)
    vmem = pl.BlockSpec(memory_space=pltpu.VMEM)
    return pl.pallas_call(
        functools.partial(step_kernel, n),
        out_shape=[pltpu.VMEM(x.shape, BF16), cache, cache, pltpu.VMEM(w_o.shape, BF16)],
        in_specs=[pl.BlockSpec(memory_space=pltpu.SMEM), vmem] + [hbm] * 11,
        out_specs=[vmem] * 4,
        scratch_shapes=[
            pltpu.VMEM((rows, n, m, dim), BF16), pltpu.VMEM((rows, n, m, dim), BF16),
            pltpu.VMEM(w_q.shape, BF16), pltpu.VMEM(w_k.shape, BF16), pltpu.VMEM(w_v.shape, BF16),
            pltpu.VMEM(x.shape, BF16), pltpu.VMEM(gain.shape, BF16), pltpu.VMEM(b_q.shape, BF16), pltpu.VMEM(b_k.shape, BF16), pltpu.VMEM(b_v.shape, BF16),
            pltpu.VMEM((rows, heads, dim), F32), pltpu.VMEM((rows, kv, dim), F32), pltpu.VMEM((rows, kv, dim), F32),
            pltpu.VMEM((rows, heads, n * m), F32), pltpu.VMEM((rows, heads, n * m), BF16), pltpu.VMEM((rows, heads, dim), F32),
            pltpu.VMEM((rows, heads, dim), F32),
            pltpu.SemaphoreType.DMA((2, n)), pltpu.SemaphoreType.DMA((2, n)), pltpu.SemaphoreType.DMA((11,))],
        compiler_params=pltpu.CompilerParams(collective_id=0, has_side_effects=True, vmem_limit_bytes=47 * 1024 * 1024),
    )(lens, freq, x, gain, b_q, b_k, b_v, w_q, w_k, w_v, w_o, k, v)


def finish_kernel(x_ref, att_ref, wo_ref, k_ref, v_ref, y_ref, ko_ref, vo_ref, sem):
    copies = [pltpu.make_async_copy(k_ref, ko_ref, sem.at[0]), pltpu.make_async_copy(v_ref, vo_ref, sem.at[1])]
    for copy in copies:
        copy.start()
    tile = 256
    for t in range(wo_ref.shape[1] // tile):
        cols = slice(t * tile, (t + 1) * tile)
        y_ref[:, cols] = (x_ref[:, cols].astype(F32) + jnp.dot(att_ref[...], wo_ref[:, cols], preferred_element_type=F32)).astype(BF16)
    for copy in copies:
        copy.wait()


def finish(x, att, w_o, k, v):
    vmem = pl.BlockSpec(memory_space=pltpu.VMEM)
    hbm = pl.BlockSpec(memory_space=pltpu.HBM)
    cache = jax.ShapeDtypeStruct(k.shape, BF16)
    return pl.pallas_call(
        finish_kernel,
        out_shape=[jax.ShapeDtypeStruct(x.shape, BF16), cache, cache],
        in_specs=[vmem] * 5,
        out_specs=[vmem, hbm, hbm],
        scratch_shapes=[pltpu.SemaphoreType.DMA((2,))],
        compiler_params=pltpu.CompilerParams(vmem_limit_bytes=4 * 1024 * 1024),
    )(x, att, w_o, k, v)


def solution(mesh):
    batch_spec = P(('dp', 'cp'))
    seq_spec = P('dp', 'cp')
    whole = P()

    def per_device(x_tok, prompt_lens, k_cache, v_cache, norm_gain, w_q, b_q, w_k, b_k, w_v, b_v, w_o):
        rows = x_tok.shape[0]
        batch, slots, kv_heads, dim = k_cache.shape
        n = batch // rows
        inv_freq = np.power(np.float32(ROPE_THETA), -(np.arange(dim // 2, dtype=np.float32) * 2.0 / dim)).astype(np.float32)
        freq = jnp.asarray(np.concatenate([inv_freq, inv_freq])[None, :])
        pack = (n, rows, slots * kv_heads, dim)
        att, k_all, v_all, wo = step(
            prompt_lens, freq, x_tok, norm_gain.reshape(-1, dim), b_q.reshape(-1, dim), b_k.reshape(-1, dim), b_v.reshape(-1, dim),
            w_q, w_k, w_v, w_o, k_cache.reshape(pack), v_cache.reshape(pack))
        y_out, k_out, v_out = finish(x_tok, att, wo, k_all, v_all)
        shape = (rows, n * slots, kv_heads, dim)
        return y_out, k_out.reshape(shape), v_out.reshape(shape)

    return jax.shard_map(per_device, mesh=mesh, in_specs=(batch_spec, P('dp'), seq_spec, seq_spec, whole, whole, whole, whole, whole, whole, whole, whole), out_specs=(batch_spec, batch_spec, batch_spec), check_vma=False)
```

```python
import functools
import numpy as np
import jax
import jax.numpy as jnp
from jax import lax
from jax.experimental import pallas as pl
from jax.experimental.pallas import tpu as pltpu
from jax.sharding import PartitionSpec as P

RMS_EPS = 1e-6
ROPE_THETA = 1000000.0
MESH = pl.DeviceIdType.MESH
F32 = jnp.float32
BF16 = jnp.bfloat16


def flip(me, d):
    out = 0
    for k in range(4):
        bit = 1 << k
        out = out + bit * lax.rem(lax.div(me, bit) + lax.div(d, bit), 2)
    return out


def step_kernel(n, lens_ref, freq_ref, x_ref, gain_ref, bq_ref, bk_ref, bv_ref, wq_ref, wk_ref, wv_ref, wo_ref, k_ref, v_ref,
                att_ref, ko_ref, vo_ref, wo,
                k_land, v_land, wq, wk, wv, xs, gain, bq, bk, bv,
                q_s, kn_s, vn_s, s_s, e_s, l_s, acc, send_sem, recv_sem, load_sem):
    me = lax.axis_index("cp")
    rows, heads, dim = q_s.shape
    m = k_land.shape[2]
    width = heads * dim
    loads = {}
    for idx, (name, src, dst) in enumerate([
            ("x", x_ref, xs), ("gain", gain_ref, gain), ("bq", bq_ref, bq), ("bk", bk_ref, bk), ("bv", bv_ref, bv),
            ("wk", wk_ref, wk), ("wv", wv_ref, wv), ("wq", wq_ref, wq),
            ("k", k_ref.at[me], k_land.at[:, me]), ("v", v_ref.at[me], v_land.at[:, me]), ("wo", wo_ref, wo)]):
        loads[name] = pltpu.make_async_copy(src, dst, load_sem.at[idx])

    barrier = pltpu.get_barrier_semaphore()
    for d in range(1, n):
        pl.semaphore_signal(barrier, inc=1, device_id={"cp": lax.rem(me + d, n)}, device_id_type=MESH)
    for copy in loads.values():
        copy.start()
    pl.semaphore_wait(barrier, n - 1)

    pairs = ((k_ref, k_land), (v_ref, v_land))

    def send(a, d):
        to = flip(me, d)
        return pltpu.make_async_remote_copy(
            src_ref=pairs[a][0].at[to], dst_ref=pairs[a][1].at[:, me], send_sem=send_sem.at[a, d], recv_sem=recv_sem.at[a, me],
            device_id={"cp": to}, device_id_type=MESH)

    def arrive(a, d):
        src = flip(me, d)
        pltpu.make_async_remote_copy(
            src_ref=pairs[a][0].at[0], dst_ref=pairs[a][1].at[:, src], send_sem=send_sem.at[a, d], recv_sem=recv_sem.at[a, src],
            device_id={"cp": src}, device_id_type=MESH).wait_recv()
        return src

    plan = [(a, d) for a in range(2) for d in (8, 4, 9, 1, 10, 5, 11, 2, 12, 6, 13, 3, 14, 7, 15)]
    for a, d in plan:
        send(a, d).start()

    pos = [lens_ref[me * rows + b] for b in range(rows)]

    for name in ("x", "gain", "bq", "bk", "bv", "wk", "wv", "wq"):
        loads[name].wait()
    wide = xs[...].astype(F32)
    inv = lax.rsqrt(jnp.mean(wide * wide, axis=-1, keepdims=True) + RMS_EPS)
    gains = jnp.concatenate([gain[h:h + 1, :].astype(F32) for h in range(heads)], axis=1)
    normed = (wide * inv * gains).astype(BF16)
    which = lax.broadcasted_iota(jnp.int32, (rows, dim), 0)
    lane = lax.broadcasted_iota(jnp.int32, (rows, dim), 1)
    posf = jnp.zeros((rows, dim), F32)
    for b in range(rows):
        posf = jnp.where(which == b, pos[b].astype(F32), posf)
    angle = posf * freq_ref[...]
    cos_t = jnp.cos(angle)
    sin_t = jnp.sin(angle)
    sin_t = jnp.where(lane < dim // 2, -sin_t, sin_t)

    def rotate(t):
        return (t * cos_t + pltpu.roll(t, dim // 2, 1) * sin_t).astype(BF16).astype(F32)

    for h in range(2):
        cols = pl.ds(h * dim, dim)
        kn_s[:, h, :] = rotate(jnp.dot(normed, wk[:, cols], preferred_element_type=F32) + bk[h:h + 1, :].astype(F32))
        vn_s[:, h, :] = (jnp.dot(normed, wv[:, cols], preferred_element_type=F32) + bv[h:h + 1, :].astype(F32)).astype(BF16).astype(F32)
    for h in range(heads):
        q_s[:, h, :] = rotate(jnp.dot(normed, wq[:, h * dim:(h + 1) * dim], preferred_element_type=F32) + bq[h:h + 1, :].astype(F32))

    row = lax.broadcasted_iota(jnp.int32, (m, dim), 0)
    even = lax.rem(row, 2) == 0

    def merge(land, new, out, b, i):
        at = 2 * pos[b] - i * m
        fresh = jnp.where(even, new[b, 0:1, :], new[b, 1:2, :])
        merged = jnp.where(row < at, land[b, i].astype(F32), jnp.where(row < at + 2, fresh, 0.0)).astype(BF16)
        out[b, i] = merged
        return merged

    def k_block(i):
        cols = pl.ds(pl.multiple_of(i * m, m), m)
        for b in range(rows):
            keys = merge(k_land, kn_s, ko_ref, b, i)
            s_s[b, :, cols] = lax.dot_general(q_s[b].astype(BF16), keys, (((1,), (1,)), ((), ())), preferred_element_type=F32) * (dim ** -0.5)

    def v_block(i):
        cols = pl.ds(pl.multiple_of(i * m, m), m)
        for b in range(rows):
            vals = merge(v_land, vn_s, vo_ref, b, i)
            acc[b] += jnp.dot(e_s[b, :, cols], vals, preferred_element_type=F32)

    def k_step(d, c):
        k_block(arrive(0, d))
        return c

    def v_step(d, c):
        v_block(arrive(1, d))
        return c

    loads["k"].wait()
    k_block(me)
    lax.fori_loop(1, n, k_step, 0)

    col = lax.broadcasted_iota(jnp.int32, (heads, n * m), 1)
    head = lax.broadcasted_iota(jnp.int32, (heads, n * m), 0)
    mine = lax.rem(col, 2) == lax.div(head, heads // 2)
    for b in range(rows):
        valid = mine & (col < 2 * pos[b] + 2)
        s = jnp.where(valid, s_s[b], -1e30)
        e = jnp.where(valid, jnp.exp(s - jnp.max(s, axis=-1, keepdims=True)), 0.0)
        l_s[b] = jnp.broadcast_to(jnp.sum(e, axis=-1, keepdims=True), (heads, dim))
        e_s[b] = e.astype(BF16)
    acc[...] = jnp.zeros_like(acc)

    loads["v"].wait()
    v_block(me)
    loads["wo"].wait()
    lax.fori_loop(1, n, v_step, 0)

    acc[...] = acc[...] / l_s[...]
    att_ref[...] = jnp.concatenate([acc[:, h, :] for h in range(heads)], axis=1).astype(BF16)

    for a, d in plan:
        send(a, d).wait_send()


def step(lens, freq, x, gain, b_q, b_k, b_v, w_q, w_k, w_v, w_o, k, v):
    n, rows, m, dim = k.shape
    heads = w_q.shape[1] // dim
    kv = w_k.shape[1] // dim
    cache = pltpu.VMEM((rows, n, m, dim), BF16)
    hbm = pl.BlockSpec(memory_space=pltpu.HBM)
    vmem = pl.BlockSpec(memory_space=pltpu.VMEM)
    return pl.pallas_call(
        functools.partial(step_kernel, n),
        out_shape=[pltpu.VMEM(x.shape, BF16), cache, cache, pltpu.VMEM(w_o.shape, BF16)],
        in_specs=[pl.BlockSpec(memory_space=pltpu.SMEM), vmem] + [hbm] * 11,
        out_specs=[vmem] * 4,
        scratch_shapes=[
            pltpu.VMEM((rows, n, m, dim), BF16), pltpu.VMEM((rows, n, m, dim), BF16),
            pltpu.VMEM(w_q.shape, BF16), pltpu.VMEM(w_k.shape, BF16), pltpu.VMEM(w_v.shape, BF16),
            pltpu.VMEM(x.shape, BF16), pltpu.VMEM(gain.shape, BF16), pltpu.VMEM(b_q.shape, BF16), pltpu.VMEM(b_k.shape, BF16), pltpu.VMEM(b_v.shape, BF16),
            pltpu.VMEM((rows, heads, dim), F32), pltpu.VMEM((rows, kv, dim), F32), pltpu.VMEM((rows, kv, dim), F32),
            pltpu.VMEM((rows, heads, n * m), F32), pltpu.VMEM((rows, heads, n * m), BF16), pltpu.VMEM((rows, heads, dim), F32),
            pltpu.VMEM((rows, heads, dim), F32),
            pltpu.SemaphoreType.DMA((2, n)), pltpu.SemaphoreType.DMA((2, n)), pltpu.SemaphoreType.DMA((11,))],
        compiler_params=pltpu.CompilerParams(collective_id=0, has_side_effects=True, vmem_limit_bytes=47 * 1024 * 1024),
    )(lens, freq, x, gain, b_q, b_k, b_v, w_q, w_k, w_v, w_o, k, v)


def finish_kernel(x_ref, att_ref, wo_ref, k_ref, v_ref, y_ref, ko_ref, vo_ref, sem):
    copies = [pltpu.make_async_copy(src.at[b], dst.at[b], sem.at[a, b]) for a, (src, dst) in enumerate(((k_ref, ko_ref), (v_ref, vo_ref))) for b in range(k_ref.shape[0])]
    for copy in copies:
        copy.start()
    tile = 256
    for t in range(wo_ref.shape[1] // tile):
        cols = slice(t * tile, (t + 1) * tile)
        y_ref[:, cols] = (x_ref[:, cols].astype(F32) + jnp.dot(att_ref[...], wo_ref[:, cols], preferred_element_type=F32)).astype(BF16)
    for copy in copies:
        copy.wait()


def finish(x, att, w_o, k, v):
    vmem = pl.BlockSpec(memory_space=pltpu.VMEM)
    hbm = pl.BlockSpec(memory_space=pltpu.HBM)
    cache = jax.ShapeDtypeStruct(k.shape, BF16)
    return pl.pallas_call(
        finish_kernel,
        out_shape=[jax.ShapeDtypeStruct(x.shape, BF16), cache, cache],
        in_specs=[vmem] * 5,
        out_specs=[vmem, hbm, hbm],
        scratch_shapes=[pltpu.SemaphoreType.DMA((2, k.shape[0]))],
        compiler_params=pltpu.CompilerParams(vmem_limit_bytes=4 * 1024 * 1024),
    )(x, att, w_o, k, v)


def solution(mesh):
    batch_spec = P(('dp', 'cp'))
    seq_spec = P('dp', 'cp')
    whole = P()

    def per_device(x_tok, prompt_lens, k_cache, v_cache, norm_gain, w_q, b_q, w_k, b_k, w_v, b_v, w_o):
        rows = x_tok.shape[0]
        batch, slots, kv_heads, dim = k_cache.shape
        n = batch // rows
        inv_freq = np.power(np.float32(ROPE_THETA), -(np.arange(dim // 2, dtype=np.float32) * 2.0 / dim)).astype(np.float32)
        freq = jnp.asarray(np.concatenate([inv_freq, inv_freq])[None, :])
        pack = (n, rows, slots * kv_heads, dim)
        att, k_all, v_all, wo = step(
            prompt_lens, freq, x_tok, norm_gain.reshape(-1, dim), b_q.reshape(-1, dim), b_k.reshape(-1, dim), b_v.reshape(-1, dim),
            w_q, w_k, w_v, w_o, k_cache.reshape(pack), v_cache.reshape(pack))
        y_out, k_out, v_out = finish(x_tok, att, wo, k_all, v_all)
        shape = (rows, n * slots, kv_heads, dim)
        return y_out, k_out.reshape(shape), v_out.reshape(shape)

    return jax.shard_map(per_device, mesh=mesh, in_specs=(batch_spec, P('dp'), seq_spec, seq_spec, whole, whole, whole, whole, whole, whole, whole, whole), out_specs=(batch_spec, batch_spec, batch_spec), check_vma=False)
```

```python
import functools
import numpy as np
import jax
import jax.numpy as jnp
from jax import lax
from jax.experimental import pallas as pl
from jax.experimental.pallas import tpu as pltpu
from jax.sharding import PartitionSpec as P

RMS_EPS = 1e-6
ROPE_THETA = 1000000.0
MESH = pl.DeviceIdType.MESH
F32 = jnp.float32
BF16 = jnp.bfloat16


def flip(me, d):
    out = 0
    for k in range(4):
        bit = 1 << k
        out = out + bit * lax.rem(lax.div(me, bit) + lax.div(d, bit), 2)
    return out


def step_kernel(n, lens_hbm, freq_hbm, x_ref, gain_ref, bq_ref, bk_ref, bv_ref, wq_ref, wk_ref, wv_ref, wo_ref, k_ref, v_ref,
                att_ref, ko_ref, vo_ref, wo,
                lens_ref, freq_ref, k_land, v_land, wq, wk, wv, xs, gain, bq, bk, bv,
                q_s, kn_s, vn_s, s_s, e_s, l_s, acc, send_sem, recv_sem, load_sem):
    me = lax.axis_index("cp")
    rows, heads, dim = q_s.shape
    m = k_land.shape[2]
    width = heads * dim
    loads = {}
    for idx, (name, src, dst) in enumerate([
            ("lens", lens_hbm, lens_ref), ("freq", freq_hbm, freq_ref), ("x", x_ref, xs), ("gain", gain_ref, gain), ("bq", bq_ref, bq), ("bk", bk_ref, bk), ("bv", bv_ref, bv),
            ("wk", wk_ref, wk), ("wv", wv_ref, wv), ("wq", wq_ref, wq),
            ("k", k_ref.at[me], k_land.at[:, me]), ("v", v_ref.at[me], v_land.at[:, me]), ("wo", wo_ref, wo)]):
        loads[name] = pltpu.make_async_copy(src, dst, load_sem.at[idx])

    barrier = pltpu.get_barrier_semaphore()
    for d in range(1, n):
        pl.semaphore_signal(barrier, inc=1, device_id={"cp": lax.rem(me + d, n)}, device_id_type=MESH)
    for copy in loads.values():
        copy.start()
    pl.semaphore_wait(barrier, n - 1)

    pairs = ((k_ref, k_land), (v_ref, v_land))

    def send(a, d):
        to = lax.rem(me + d, n)
        return pltpu.make_async_remote_copy(
            src_ref=pairs[a][0].at[to], dst_ref=pairs[a][1].at[:, me], send_sem=send_sem.at[a, d], recv_sem=recv_sem.at[a, me],
            device_id={"cp": to}, device_id_type=MESH)

    def arrive(a, d):
        src = lax.rem(me + n - d, n)
        pltpu.make_async_remote_copy(
            src_ref=pairs[a][0].at[0], dst_ref=pairs[a][1].at[:, src], send_sem=send_sem.at[a, d], recv_sem=recv_sem.at[a, src],
            device_id={"cp": src}, device_id_type=MESH).wait_recv()
        return src

    plan = [(a, d) for d in range(1, n) for a in range(2)]
    for a, d in plan:
        send(a, d).start()

    loads["lens"].wait()
    pos = [lens_ref[me * rows + b] for b in range(rows)]

    for name in ("freq", "x", "gain", "bq", "bk", "bv", "wk", "wv", "wq"):
        loads[name].wait()
    wide = xs[...].astype(F32)
    inv = lax.rsqrt(jnp.mean(wide * wide, axis=-1, keepdims=True) + RMS_EPS)
    gains = jnp.concatenate([gain[h:h + 1, :].astype(F32) for h in range(heads)], axis=1)
    normed = (wide * inv * gains).astype(BF16)
    which = lax.broadcasted_iota(jnp.int32, (rows, dim), 0)
    lane = lax.broadcasted_iota(jnp.int32, (rows, dim), 1)
    posf = jnp.zeros((rows, dim), F32)
    for b in range(rows):
        posf = jnp.where(which == b, pos[b].astype(F32), posf)
    angle = posf * freq_ref[...]
    cos_t = jnp.cos(angle)
    sin_t = jnp.sin(angle)
    sin_t = jnp.where(lane < dim // 2, -sin_t, sin_t)

    def rotate(t):
        return (t * cos_t + pltpu.roll(t, dim // 2, 1) * sin_t).astype(BF16).astype(F32)

    for h in range(2):
        cols = pl.ds(h * dim, dim)
        kn_s[:, h, :] = rotate(jnp.dot(normed, wk[:, cols], preferred_element_type=F32) + bk[h:h + 1, :].astype(F32))
        vn_s[:, h, :] = (jnp.dot(normed, wv[:, cols], preferred_element_type=F32) + bv[h:h + 1, :].astype(F32)).astype(BF16).astype(F32)
    for h in range(heads):
        q_s[:, h, :] = rotate(jnp.dot(normed, wq[:, h * dim:(h + 1) * dim], preferred_element_type=F32) + bq[h:h + 1, :].astype(F32))

    row = lax.broadcasted_iota(jnp.int32, (m, dim), 0)
    even = lax.rem(row, 2) == 0

    def merge(land, new, out, b, i):
        at = 2 * pos[b] - i * m
        fresh = jnp.where(even, new[b, 0:1, :], new[b, 1:2, :])
        merged = jnp.where(row < at, land[b, i].astype(F32), jnp.where(row < at + 2, fresh, 0.0)).astype(BF16)
        out[b, i] = merged
        return merged

    def k_block(i):
        cols = pl.ds(pl.multiple_of(i * m, m), m)
        for b in range(rows):
            keys = merge(k_land, kn_s, ko_ref, b, i)
            s_s[b, :, cols] = lax.dot_general(q_s[b].astype(BF16), keys, (((1,), (1,)), ((), ())), preferred_element_type=F32) * (dim ** -0.5)

    def v_block(i):
        cols = pl.ds(pl.multiple_of(i * m, m), m)
        for b in range(rows):
            vals = merge(v_land, vn_s, vo_ref, b, i)
            acc[b] += jnp.dot(e_s[b, :, cols], vals, preferred_element_type=F32)

    def k_step(d, c):
        k_block(arrive(0, d))
        return c

    def v_step(d, c):
        v_block(arrive(1, d))
        return c

    loads["k"].wait()
    k_block(me)
    lax.fori_loop(1, n, k_step, 0)

    col = lax.broadcasted_iota(jnp.int32, (heads, n * m), 1)
    head = lax.broadcasted_iota(jnp.int32, (heads, n * m), 0)
    mine = lax.rem(col, 2) == lax.div(head, heads // 2)
    for b in range(rows):
        valid = mine & (col < 2 * pos[b] + 2)
        s = jnp.where(valid, s_s[b], -1e30)
        e = jnp.where(valid, jnp.exp(s - jnp.max(s, axis=-1, keepdims=True)), 0.0)
        l_s[b] = jnp.broadcast_to(jnp.sum(e, axis=-1, keepdims=True), (heads, dim))
        e_s[b] = e.astype(BF16)
    acc[...] = jnp.zeros_like(acc)

    loads["v"].wait()
    v_block(me)
    loads["wo"].wait()
    lax.fori_loop(1, n, v_step, 0)

    acc[...] = acc[...] / l_s[...]
    att_ref[...] = jnp.concatenate([acc[:, h, :] for h in range(heads)], axis=1).astype(BF16)

    for a, d in plan:
        send(a, d).wait_send()


def step(lens, freq, x, gain, b_q, b_k, b_v, w_q, w_k, w_v, w_o, k, v):
    n, rows, m, dim = k.shape
    heads = w_q.shape[1] // dim
    kv = w_k.shape[1] // dim
    cache = pltpu.VMEM((rows, n, m, dim), BF16)
    hbm = pl.BlockSpec(memory_space=pltpu.HBM)
    vmem = pl.BlockSpec(memory_space=pltpu.VMEM)
    return pl.pallas_call(
        functools.partial(step_kernel, n),
        out_shape=[pltpu.VMEM(x.shape, BF16), cache, cache, pltpu.VMEM(w_o.shape, BF16)],
        in_specs=[hbm] * 13,
        out_specs=[vmem] * 4,
        scratch_shapes=[
            pltpu.SMEM(lens.shape, jnp.int32), pltpu.VMEM(freq.shape, F32),
            pltpu.VMEM((rows, n, m, dim), BF16), pltpu.VMEM((rows, n, m, dim), BF16),
            pltpu.VMEM(w_q.shape, BF16), pltpu.VMEM(w_k.shape, BF16), pltpu.VMEM(w_v.shape, BF16),
            pltpu.VMEM(x.shape, BF16), pltpu.VMEM(gain.shape, BF16), pltpu.VMEM(b_q.shape, BF16), pltpu.VMEM(b_k.shape, BF16), pltpu.VMEM(b_v.shape, BF16),
            pltpu.VMEM((rows, heads, dim), F32), pltpu.VMEM((rows, kv, dim), F32), pltpu.VMEM((rows, kv, dim), F32),
            pltpu.VMEM((rows, heads, n * m), F32), pltpu.VMEM((rows, heads, n * m), BF16), pltpu.VMEM((rows, heads, dim), F32),
            pltpu.VMEM((rows, heads, dim), F32),
            pltpu.SemaphoreType.DMA((2, n)), pltpu.SemaphoreType.DMA((2, n)), pltpu.SemaphoreType.DMA((13,))],
        compiler_params=pltpu.CompilerParams(collective_id=0, has_side_effects=True, vmem_limit_bytes=47 * 1024 * 1024),
    )(lens, freq, x, gain, b_q, b_k, b_v, w_q, w_k, w_v, w_o, k, v)


def finish_kernel(x_ref, att_ref, wo_ref, k_ref, v_ref, y_ref, ko_ref, vo_ref, sem):
    copies = [pltpu.make_async_copy(k_ref, ko_ref, sem.at[0]), pltpu.make_async_copy(v_ref, vo_ref, sem.at[1])]
    for copy in copies:
        copy.start()
    tile = 256
    for t in range(wo_ref.shape[1] // tile):
        cols = slice(t * tile, (t + 1) * tile)
        y_ref[:, cols] = (x_ref[:, cols].astype(F32) + jnp.dot(att_ref[...], wo_ref[:, cols], preferred_element_type=F32)).astype(BF16)
    for copy in copies:
        copy.wait()


def finish(x, att, w_o, k, v):
    vmem = pl.BlockSpec(memory_space=pltpu.VMEM)
    hbm = pl.BlockSpec(memory_space=pltpu.HBM)
    cache = jax.ShapeDtypeStruct(k.shape, BF16)
    return pl.pallas_call(
        finish_kernel,
        out_shape=[jax.ShapeDtypeStruct(x.shape, BF16), cache, cache],
        in_specs=[vmem] * 5,
        out_specs=[vmem, hbm, hbm],
        scratch_shapes=[pltpu.SemaphoreType.DMA((2,))],
        compiler_params=pltpu.CompilerParams(vmem_limit_bytes=4 * 1024 * 1024),
    )(x, att, w_o, k, v)


def solution(mesh):
    batch_spec = P(('dp', 'cp'))
    seq_spec = P('dp', 'cp')
    whole = P()

    def per_device(x_tok, prompt_lens, k_cache, v_cache, norm_gain, w_q, b_q, w_k, b_k, w_v, b_v, w_o):
        rows = x_tok.shape[0]
        batch, slots, kv_heads, dim = k_cache.shape
        n = batch // rows
        inv_freq = np.power(np.float32(ROPE_THETA), -(np.arange(dim // 2, dtype=np.float32) * 2.0 / dim)).astype(np.float32)
        freq = jnp.asarray(np.concatenate([inv_freq, inv_freq])[None, :])
        pack = (n, rows, slots * kv_heads, dim)
        att, k_all, v_all, wo = step(
            prompt_lens, freq, x_tok, norm_gain.reshape(-1, dim), b_q.reshape(-1, dim), b_k.reshape(-1, dim), b_v.reshape(-1, dim),
            w_q, w_k, w_v, w_o, k_cache.reshape(pack), v_cache.reshape(pack))
        y_out, k_out, v_out = finish(x_tok, att, wo, k_all, v_all)
        shape = (rows, n * slots, kv_heads, dim)
        return y_out, k_out.reshape(shape), v_out.reshape(shape)

    return jax.shard_map(per_device, mesh=mesh, in_specs=(batch_spec, P('dp'), seq_spec, seq_spec, whole, whole, whole, whole, whole, whole, whole, whole), out_specs=(batch_spec, batch_spec, batch_spec), check_vma=False)
```

```python
import functools
import numpy as np
import jax
import jax.numpy as jnp
from jax import lax
from jax.experimental import pallas as pl
from jax.experimental.pallas import tpu as pltpu
from jax.sharding import PartitionSpec as P

RMS_EPS = 1e-6
ROPE_THETA = 1000000.0
MESH = pl.DeviceIdType.MESH
F32 = jnp.float32
BF16 = jnp.bfloat16


def flip(me, d):
    out = 0
    for k in range(4):
        bit = 1 << k
        out = out + bit * lax.rem(lax.div(me, bit) + lax.div(d, bit), 2)
    return out


PIECE = (7, 7, 6, 6)


def step_kernel(n, pooled, lens_hbm, freq_hbm, x_ref, gain_ref, bq_ref, bk_ref, bv_ref, wq_ref, wk_ref, wv_ref, wo_ref, k_ref, v_ref,
                att_ref, ko_ref, vo_ref, wo,
                lens_ref, freq_ref, k_land, v_land, wq, wk, wv, xs, gain, bq, bk, bv,
                q_s, kn_s, vn_s, s_s, e_s, l_s, acc, send_sem, recv_sem, load_sem, *pool):
    me = lax.axis_index("cp")
    rows, heads, dim = q_s.shape
    m = k_land.shape[2]
    half = n // 2
    high = lax.div(me, half)
    h = lax.rem(me, half)
    other = (1 - high) * half
    inner = lax.rem(lax.div(me, 4) + high, 2) == 1
    outer = lax.rem(lax.div(me, 4) + high, 2) == 0
    loads = {}
    for idx, (name, src, dst) in enumerate([
            ("lens", lens_hbm, lens_ref), ("freq", freq_hbm, freq_ref), ("x", x_ref, xs), ("gain", gain_ref, gain), ("bq", bq_ref, bq), ("bk", bk_ref, bk), ("bv", bv_ref, bv),
            ("wk", wk_ref, wk), ("wv", wv_ref, wv), ("wq", wq_ref, wq),
            ("k", k_ref.at[me], k_land.at[:, me]), ("v", v_ref.at[me], v_land.at[:, me]), ("wo", wo_ref, wo)]):
        loads[name] = pltpu.make_async_copy(src, dst, load_sem.at[idx])

    pairs = ((k_ref, k_land), (v_ref, v_land))

    def send(a, to):
        return pltpu.make_async_remote_copy(
            src_ref=pairs[a][0].at[to], dst_ref=pairs[a][1].at[:, me], send_sem=send_sem.at[a, to], recv_sem=recv_sem.at[a, me],
            device_id={"cp": to}, device_id_type=MESH)

    def arrive(a, src):
        pltpu.make_async_remote_copy(
            src_ref=pairs[a][0].at[0], dst_ref=pairs[a][1].at[:, src], send_sem=send_sem.at[a, src], recv_sem=recv_sem.at[a, src],
            device_id={"cp": src}, device_id_type=MESH).wait_recv()

    def both(to, act):
        for a in range(2):
            act(send(a, to))

    def start(copy):
        copy.start()

    def sent(copy):
        copy.wait_send()

    barrier = pltpu.get_barrier_semaphore()
    for d in range(1, n):
        pl.semaphore_signal(barrier, inc=1, device_id={"cp": lax.rem(me + d, n)}, device_id_type=MESH)
    loads["lens"].start()
    if pooled:
        (k_all, v_all, k_pack, v_pack, next_s, pick_s, place_s, gather_sem, st_send, st_recv, fw_send, fw_recv), land = pool[:12], (pool[12:16], pool[16:20])
        caches, packs = (k_all, v_all), (k_pack, v_pack)

        def gather(a, j):
            return pltpu.make_async_copy(pairs[a][0].at[other + j], caches[a].at[pl.ds(j * rows, rows)], gather_sem.at[a, j])

        @pl.when(inner)
        def _():
            for a in range(2):
                for j in range(half):
                    gather(a, j).start()

    for name, copy in loads.items():
        if name != "lens":
            copy.start()
    pl.semaphore_wait(barrier, n - 1)

    if not pooled:
        for d in range(1, n):
            both(lax.rem(me + d, n), start)
        loads["lens"].wait()
    else:
        near = [high * half + lax.rem(h + t, half) for t in range(1, half)]
        far = [other + lax.rem(h + t, half) for t in range(half)]
        beside = [lax.div(to, 4) == lax.div(me, 4) for to in near]
        apart = [lax.div(to, 4) != lax.div(me, 4) for to in near]
        for to, ok in zip(near, beside):
            @pl.when(outer | ok)
            def _():
                both(to, start)

        @pl.when(outer)
        def _():
            send(0, far[0]).start()

        loads["lens"].wait()
        mine = jnp.where(lax.rem(me, 4) < 2, PIECE[0], PIECE[2])

        @pl.when(inner)
        def _():
            next_s[half * rows] = half * rows

            def back(t, carry):
                b = half * rows - 1 - t
                nx = jnp.where(lens_ref[other * rows + b] > (m // 2) * me, b, carry)
                next_s[b] = nx
                return nx

            lax.fori_loop(0, half * rows, back, half * rows, unroll=8)

            def fill(s, cur):
                cand = next_s[cur]
                ok = s >= (lax.shift_right_logical(cand, 3) - 1) * mine
                pick_s[s] = jnp.minimum(cand, half * rows - 1)
                return jnp.where(ok, jnp.minimum(cand + 1, half * rows), cur)

            lax.fori_loop(0, half * max(PIECE), fill, 0, unroll=8)
            for a in range(2):
                for j in range(half):
                    gather(a, j).wait()

            def pack(s, c):
                b = pick_s[s]
                for a in range(2):
                    packs[a][s] = caches[a][b]
                return c

            lax.fori_loop(0, half * max(PIECE), pack, 0, unroll=4)

        def place(b, ends):
            length = lens_ref[high * half * rows + b]
            out = []
            for u in range(4):
                at = jnp.maximum(ends[u], (lax.div(b, rows) - 1) * PIECE[u])
                place_s[u, b] = at
                out.append(jnp.where(length > (m // 2) * (half - 4 * high + u), at + 1, ends[u]))
            return tuple(out)

        lax.fori_loop(0, half * rows, place, (0, 0, 0, 0), unroll=4)

        def stream(a, t, y):
            c = PIECE[2 * y]
            u = lax.rem(me, 4)
            j = lax.rem(2 * u + t, half)
            return [pltpu.make_async_remote_copy(
                src_ref=packs[a].at[pl.ds(j * c, c)], dst_ref=land[a][2 * y + core].at[pl.ds(c, c)], send_sem=st_send.at[a, t], recv_sem=st_recv.at[a, 2 * y + core],
                device_id={"cp": other + j}, device_id_type=MESH) for core in range(2)]

        def streams(act):
            for y in range(2):
                for core in range(2):
                    @pl.when(inner & (lax.rem(me, 4) == 2 * y + core))
                    def _():
                        for a in range(2):
                            for t in range(half):
                                act(stream(a, t, y)[core])

        streams(start)
        for to, ok in zip(near, apart):
            @pl.when(inner & ok)
            def _():
                both(to, start)

    pos = [lens_ref[me * rows + b] for b in range(rows)]

    for name in ("freq", "x", "gain", "bq", "bk", "bv", "wk", "wv", "wq"):
        loads[name].wait()
    wide = xs[...].astype(F32)
    inv = lax.rsqrt(jnp.mean(wide * wide, axis=-1, keepdims=True) + RMS_EPS)
    gains = jnp.concatenate([gain[i:i + 1, :].astype(F32) for i in range(heads)], axis=1)
    normed = (wide * inv * gains).astype(BF16)
    which = lax.broadcasted_iota(jnp.int32, (rows, dim), 0)
    lane = lax.broadcasted_iota(jnp.int32, (rows, dim), 1)
    posf = jnp.zeros((rows, dim), F32)
    for b in range(rows):
        posf = jnp.where(which == b, pos[b].astype(F32), posf)
    angle = posf * freq_ref[...]
    cos_t = jnp.cos(angle)
    sin_t = jnp.sin(angle)
    sin_t = jnp.where(lane < dim // 2, -sin_t, sin_t)

    def rotate(t):
        return (t * cos_t + pltpu.roll(t, dim // 2, 1) * sin_t).astype(BF16).astype(F32)

    for i in range(2):
        cols = pl.ds(i * dim, dim)
        kn_s[:, i, :] = rotate(jnp.dot(normed, wk[:, cols], preferred_element_type=F32) + bk[i:i + 1, :].astype(F32))
        vn_s[:, i, :] = (jnp.dot(normed, wv[:, cols], preferred_element_type=F32) + bv[i:i + 1, :].astype(F32)).astype(BF16).astype(F32)
    for i in range(heads):
        q_s[:, i, :] = rotate(jnp.dot(normed, wq[:, i * dim:(i + 1) * dim], preferred_element_type=F32) + bq[i:i + 1, :].astype(F32))

    row = lax.broadcasted_iota(jnp.int32, (m, dim), 0)
    even = lax.rem(row, 2) == 0

    def merge(raw, new, out, b, i):
        at = 2 * pos[b] - i * m
        fresh = jnp.where(even, new[b, 0:1, :], new[b, 1:2, :])
        merged = jnp.where(row < at, raw.astype(F32), jnp.where(row < at + 2, fresh, 0.0)).astype(BF16)
        out[b, i] = merged
        return merged

    def k_block(i, get):
        cols = pl.ds(pl.multiple_of(i * m, m), m)
        for b in range(rows):
            keys = merge(get(b), kn_s, ko_ref, b, i)
            s_s[b, :, cols] = lax.dot_general(q_s[b].astype(BF16), keys, (((1,), (1,)), ((), ())), preferred_element_type=F32) * (dim ** -0.5)

    def v_block(i, get):
        cols = pl.ds(pl.multiple_of(i * m, m), m)
        for b in range(rows):
            vals = merge(get(b), vn_s, vo_ref, b, i)
            acc[b] += jnp.dot(e_s[b, :, cols], vals, preferred_element_type=F32)

    def direct(a, block):
        def visit(d, c):
            src = lax.rem(me + n - d, n)

            def go():
                arrive(a, src)
                block(src, lambda b: pairs[a][1][b, src])

            if pooled:
                pl.when((lax.div(src, half) == high) | (lax.rem(lax.div(src, 4) + lax.div(src, half), 2) == 0))(go)
            else:
                go()
            return c

        lax.fori_loop(1, n, visit, 0)

    def pooled_blocks(a, block):
        for u in range(4):
            c = PIECE[u]
            for side in range(2):
                @pl.when(h > 0 if side == 0 else h < half - 1)
                def _():
                    forward(a, u, 1 - side).wait_recv()
        for u in range(4):
            c = PIECE[u]
            i = half - 4 * high + u

            def get(b):
                loc = place_s[u, h * rows + b] - (h - 1) * c
                return land[a][u][jnp.clip(loc, 0, 3 * c - 1)]

            block(i, get)

    def forward(a, u, side):
        c = PIECE[u]
        to = high * half + lax.rem(h + (1 if side else half - 1), half)
        return pltpu.make_async_remote_copy(
            src_ref=land[a][u].at[pl.ds(c, c)], dst_ref=land[a][u].at[pl.ds(0 if side else 2 * c, c)], send_sem=fw_send.at[a, u, side], recv_sem=fw_recv.at[a, u, side],
            device_id={"cp": to}, device_id_type=MESH)

    def forwards(a, u, act):
        @pl.when(h < half - 1)
        def _():
            act(forward(a, u, 1))

        @pl.when(h > 0)
        def _():
            act(forward(a, u, 0))

    if pooled:
        for a in range(2):
            for u in range(4):
                c = PIECE[u]
                pltpu.make_async_remote_copy(
                    src_ref=packs[a].at[pl.ds(0, c)], dst_ref=land[a][u].at[pl.ds(c, c)], send_sem=st_send.at[a, 0], recv_sem=st_recv.at[a, u],
                    device_id={"cp": me}, device_id_type=MESH).wait_recv()
                forwards(a, u, start)

        @pl.when(outer)
        def _():
            send(1, far[0]).start()
            for to in far[1:]:
                both(to, start)

    loads["k"].wait()
    k_block(me, lambda b: k_land[b, me])
    direct(0, k_block)
    if pooled:
        pooled_blocks(0, k_block)

    col = lax.broadcasted_iota(jnp.int32, (heads, n * m), 1)
    head = lax.broadcasted_iota(jnp.int32, (heads, n * m), 0)
    own = lax.rem(col, 2) == lax.div(head, heads // 2)
    for b in range(rows):
        valid = own & (col < 2 * pos[b] + 2)
        s = jnp.where(valid, s_s[b], -1e30)
        e = jnp.where(valid, jnp.exp(s - jnp.max(s, axis=-1, keepdims=True)), 0.0)
        l_s[b] = jnp.broadcast_to(jnp.sum(e, axis=-1, keepdims=True), (heads, dim))
        e_s[b] = e.astype(BF16)
    acc[...] = jnp.zeros_like(acc)

    loads["v"].wait()
    v_block(me, lambda b: v_land[b, me])
    loads["wo"].wait()
    if pooled:
        pooled_blocks(1, v_block)
    direct(1, v_block)

    acc[...] = acc[...] / l_s[...]
    att_ref[...] = jnp.concatenate([acc[:, i, :] for i in range(heads)], axis=1).astype(BF16)

    if not pooled:
        for d in range(1, n):
            both(lax.rem(me + d, n), sent)
    else:
        for to in near:
            both(to, sent)

        @pl.when(outer)
        def _():
            for to in far:
                both(to, sent)

        streams(sent)
        for a in range(2):
            for u in range(4):
                forwards(a, u, sent)


def step(pooled, lens, freq, x, gain, b_q, b_k, b_v, w_q, w_k, w_v, w_o, k, v):
    n, rows, m, dim = k.shape
    heads = w_q.shape[1] // dim
    kv = w_k.shape[1] // dim
    half = n // 2
    cache = pltpu.VMEM((rows, n, m, dim), BF16)
    hbm = pl.BlockSpec(memory_space=pltpu.HBM)
    vmem = pl.BlockSpec(memory_space=pltpu.VMEM)
    dma = pltpu.SemaphoreType.DMA
    scratch = [
        pltpu.SMEM(lens.shape, jnp.int32), pltpu.VMEM(freq.shape, F32),
        pltpu.VMEM((rows, n, m, dim), BF16), pltpu.VMEM((rows, n, m, dim), BF16),
        pltpu.VMEM(w_q.shape, BF16), pltpu.VMEM(w_k.shape, BF16), pltpu.VMEM(w_v.shape, BF16),
        pltpu.VMEM(x.shape, BF16), pltpu.VMEM(gain.shape, BF16), pltpu.VMEM(b_q.shape, BF16), pltpu.VMEM(b_k.shape, BF16), pltpu.VMEM(b_v.shape, BF16),
        pltpu.VMEM((rows, heads, dim), F32), pltpu.VMEM((rows, kv, dim), F32), pltpu.VMEM((rows, kv, dim), F32),
        pltpu.VMEM((rows, heads, n * m), F32), pltpu.VMEM((rows, heads, n * m), BF16), pltpu.VMEM((rows, heads, dim), F32),
        pltpu.VMEM((rows, heads, dim), F32),
        dma((2, n)), dma((2, n)), dma((13,))]
    if pooled:
        scratch += [pltpu.VMEM((half * rows, m, dim), BF16)] * 2 + [pltpu.VMEM((half * max(PIECE), m, dim), BF16)] * 2
        scratch += [pltpu.SMEM((half * rows + 1,), jnp.int32), pltpu.SMEM((half * max(PIECE),), jnp.int32), pltpu.SMEM((4, half * rows), jnp.int32)]
        scratch += [dma((2, half)), dma((2, half)), dma((2, 4)), dma((2, 4, 2)), dma((2, 4, 2))]
        scratch += [pltpu.VMEM((3 * c, m, dim), BF16) for _ in range(2) for c in PIECE]
    return pl.pallas_call(
        functools.partial(step_kernel, n, pooled),
        out_shape=[pltpu.VMEM(x.shape, BF16), cache, cache, pltpu.VMEM(w_o.shape, BF16)],
        in_specs=[hbm] * 13,
        out_specs=[vmem] * 4,
        scratch_shapes=scratch,
        compiler_params=pltpu.CompilerParams(collective_id=int(pooled), has_side_effects=True, vmem_limit_bytes=47 * 1024 * 1024),
    )(lens, freq, x, gain, b_q, b_k, b_v, w_q, w_k, w_v, w_o, k, v)


def fits(lens, n, rows, slots):
    half = n // 2
    c = np.array(PIECE * 2)[:, None, None]
    src = np.arange(n // 4, n - n // 4)
    k, j = np.arange(half)[None, :, None], np.arange(half)[None, None, :]
    room = np.minimum((j + 2) * c, half * c) - np.maximum(k - 1, 0) * c
    room = np.where(k <= j, room, n * rows)
    owner = np.arange(half * rows) // rows
    between = (owner >= np.arange(half)[:, None, None]) & (owner <= np.arange(half)[None, :, None])
    seqs = jnp.concatenate([jnp.broadcast_to(lens[half * rows:], (half // 2, half * rows)), jnp.broadcast_to(lens[:half * rows], (half // 2, half * rows))])
    need = (seqs > jnp.asarray(src * slots)[:, None]).astype(F32)
    used = jnp.dot(need, jnp.asarray(between.reshape(half * half, -1).T.astype(np.float32)))
    return jnp.all(used <= jnp.asarray(room.reshape(half, -1).astype(np.float32)))


def finish_kernel(x_ref, att_ref, wo_ref, k_ref, v_ref, y_ref, ko_ref, vo_ref, sem):
    copies = [pltpu.make_async_copy(k_ref, ko_ref, sem.at[0]), pltpu.make_async_copy(v_ref, vo_ref, sem.at[1])]
    for copy in copies:
        copy.start()
    tile = 256
    for t in range(wo_ref.shape[1] // tile):
        cols = slice(t * tile, (t + 1) * tile)
        y_ref[:, cols] = (x_ref[:, cols].astype(F32) + jnp.dot(att_ref[...], wo_ref[:, cols], preferred_element_type=F32)).astype(BF16)
    for copy in copies:
        copy.wait()


def finish(x, att, w_o, k, v):
    vmem = pl.BlockSpec(memory_space=pltpu.VMEM)
    hbm = pl.BlockSpec(memory_space=pltpu.HBM)
    cache = jax.ShapeDtypeStruct(k.shape, BF16)
    return pl.pallas_call(
        finish_kernel,
        out_shape=[jax.ShapeDtypeStruct(x.shape, BF16), cache, cache],
        in_specs=[vmem] * 5,
        out_specs=[vmem, hbm, hbm],
        scratch_shapes=[pltpu.SemaphoreType.DMA((2,))],
        compiler_params=pltpu.CompilerParams(vmem_limit_bytes=4 * 1024 * 1024),
    )(x, att, w_o, k, v)


def solution(mesh):
    batch_spec = P(('dp', 'cp'))
    seq_spec = P('dp', 'cp')
    whole = P()

    def per_device(x_tok, prompt_lens, k_cache, v_cache, norm_gain, w_q, b_q, w_k, b_k, w_v, b_v, w_o):
        rows = x_tok.shape[0]
        batch, slots, kv_heads, dim = k_cache.shape
        n = batch // rows
        inv_freq = np.power(np.float32(ROPE_THETA), -(np.arange(dim // 2, dtype=np.float32) * 2.0 / dim)).astype(np.float32)
        freq = jnp.asarray(np.concatenate([inv_freq, inv_freq])[None, :])
        pack = (n, rows, slots * kv_heads, dim)
        args = (prompt_lens, freq, x_tok, norm_gain.reshape(-1, dim), b_q.reshape(-1, dim), b_k.reshape(-1, dim), b_v.reshape(-1, dim),
                w_q, w_k, w_v, w_o, k_cache.reshape(pack), v_cache.reshape(pack))

        def run(pooled, *args):
            att, k_all, v_all, wo = step(pooled, *args)
            return finish(x_tok, att, wo, k_all, v_all)

        y_out, k_out, v_out = lax.cond(fits(prompt_lens, n, rows, slots), functools.partial(run, True), functools.partial(run, False), *args)
        shape = (rows, n * slots, kv_heads, dim)
        return y_out, k_out.reshape(shape), v_out.reshape(shape)

    return jax.shard_map(per_device, mesh=mesh, in_specs=(batch_spec, P('dp'), seq_spec, seq_spec, whole, whole, whole, whole, whole, whole, whole, whole), out_specs=(batch_spec, batch_spec, batch_spec), check_vma=False)
```

```python
import functools
import numpy as np
import jax
import jax.numpy as jnp
from jax import lax
from jax.experimental import pallas as pl
from jax.experimental.pallas import tpu as pltpu
from jax.sharding import PartitionSpec as P

RMS_EPS = 1e-6
ROPE_THETA = 1000000.0
MESH = pl.DeviceIdType.MESH
F32 = jnp.float32
BF16 = jnp.bfloat16


def flip(me, d):
    out = 0
    for k in range(4):
        bit = 1 << k
        out = out + bit * lax.rem(lax.div(me, bit) + lax.div(d, bit), 2)
    return out


PIECE = (7, 7, 6, 6)


def step_kernel(n, pooled, lens_hbm, freq_hbm, x_ref, gain_ref, bq_ref, bk_ref, bv_ref, wq_ref, wk_ref, wv_ref, wo_ref, k_ref, v_ref,
                att_ref, ko_ref, vo_ref, wo,
                lens_ref, freq_ref, k_land, v_land, wq, wk, wv, xs, gain, bq, bk, bv,
                q_s, kn_s, vn_s, s_s, e_s, l_s, acc, send_sem, recv_sem, load_sem, *pool):
    me = lax.axis_index("cp")
    rows, heads, dim = q_s.shape
    m = k_land.shape[2]
    half = n // 2
    high = lax.div(me, half)
    h = lax.rem(me, half)
    other = (1 - high) * half
    inner = lax.rem(lax.div(me, 4) + high, 2) == 1
    outer = lax.rem(lax.div(me, 4) + high, 2) == 0
    loads = {}
    for idx, (name, src, dst) in enumerate([
            ("lens", lens_hbm, lens_ref), ("freq", freq_hbm, freq_ref), ("x", x_ref, xs), ("gain", gain_ref, gain), ("bq", bq_ref, bq), ("bk", bk_ref, bk), ("bv", bv_ref, bv),
            ("wk", wk_ref, wk), ("wv", wv_ref, wv), ("wq", wq_ref, wq),
            ("k", k_ref.at[me], k_land.at[:, me]), ("v", v_ref.at[me], v_land.at[:, me]), ("wo", wo_ref, wo)]):
        loads[name] = pltpu.make_async_copy(src, dst, load_sem.at[idx])

    pairs = ((k_ref, k_land), (v_ref, v_land))

    def send(a, to):
        return pltpu.make_async_remote_copy(
            src_ref=pairs[a][0].at[to], dst_ref=pairs[a][1].at[:, me], send_sem=send_sem.at[a, to], recv_sem=recv_sem.at[a, me],
            device_id={"cp": to}, device_id_type=MESH)

    def arrive(a, src):
        pltpu.make_async_remote_copy(
            src_ref=pairs[a][0].at[0], dst_ref=pairs[a][1].at[:, src], send_sem=send_sem.at[a, src], recv_sem=recv_sem.at[a, src],
            device_id={"cp": src}, device_id_type=MESH).wait_recv()

    def both(to, act):
        for a in range(2):
            act(send(a, to))

    def start(copy):
        copy.start()

    def sent(copy):
        copy.wait_send()

    barrier = pltpu.get_barrier_semaphore()
    for d in range(1, n):
        pl.semaphore_signal(barrier, inc=1, device_id={"cp": lax.rem(me + d, n)}, device_id_type=MESH)
    loads["lens"].start()
    if pooled:
        (k_all, v_all, k_pack, v_pack, next_s, pick_s, place_s, gather_sem, st_send, st_recv, fw_send, fw_recv, gate), land = pool[:13], (pool[13:17], pool[17:21])
        caches, packs = (k_all, v_all), (k_pack, v_pack)

        def gather(a, j):
            return pltpu.make_async_copy(pairs[a][0].at[other + j], caches[a].at[pl.ds(j * rows, rows)], gather_sem.at[a, j])

        @pl.when(inner)
        def _():
            for a in range(2):
                for j in range(half):
                    gather(a, j).start()

    for name, copy in loads.items():
        if name != "lens":
            copy.start()
    pl.semaphore_wait(barrier, n - 1)

    if not pooled:
        for d in range(1, n):
            both(lax.rem(me + d, n), start)
        loads["lens"].wait()
    else:
        near = [high * half + lax.rem(h + t, half) for t in range(1, half)]
        far = [other + lax.rem(h + t, half) for t in range(half)]
        beside = [lax.div(to, 4) == lax.div(me, 4) for to in near]
        apart = [lax.div(to, 4) != lax.div(me, 4) for to in near]
        for to, ok in zip(near, beside):
            @pl.when(outer | ok)
            def _():
                both(to, start)

        @pl.when(outer)
        def _():
            send(0, far[0]).start()

        loads["lens"].wait()
        mine = jnp.where(lax.rem(me, 4) < 2, PIECE[0], PIECE[2])

        @pl.when(inner)
        def _():
            next_s[half * rows] = half * rows

            def back(t, carry):
                b = half * rows - 1 - t
                nx = jnp.where(lens_ref[other * rows + b] > (m // 2) * me, b, carry)
                next_s[b] = nx
                return nx

            lax.fori_loop(0, half * rows, back, half * rows, unroll=8)

            def fill(s, cur):
                cand = next_s[cur]
                ok = s >= (lax.shift_right_logical(cand, 3) - 1) * mine
                pick_s[s] = jnp.minimum(cand, half * rows - 1)
                return jnp.where(ok, jnp.minimum(cand + 1, half * rows), cur)

            lax.fori_loop(0, half * max(PIECE), fill, 0, unroll=8)
            for a in range(2):
                for j in range(half):
                    gather(a, j).wait()

            def pack(s, c):
                b = pick_s[s]
                for a in range(2):
                    packs[a][s] = caches[a][b]
                return c

            lax.fori_loop(0, half * max(PIECE), pack, 0, unroll=4)

        def place(b, ends):
            length = lens_ref[high * half * rows + b]
            out = []
            for u in range(4):
                at = jnp.maximum(ends[u], (lax.div(b, rows) - 1) * PIECE[u])
                place_s[u, b] = at
                out.append(jnp.where(length > (m // 2) * (half - 4 * high + u), at + 1, ends[u]))
            return tuple(out)

        lax.fori_loop(0, half * rows, place, (0, 0, 0, 0), unroll=4)

        def stream(a, t, y):
            c = PIECE[2 * y]
            u = lax.rem(me, 4)
            j = lax.rem(2 * u + t, half)
            return [pltpu.make_async_remote_copy(
                src_ref=packs[a].at[pl.ds(j * c, c)], dst_ref=land[a][2 * y + core].at[pl.ds(c, c)], send_sem=st_send.at[a, t], recv_sem=st_recv.at[a, 2 * y + core],
                device_id={"cp": other + j}, device_id_type=MESH) for core in range(2)]

        def streams(act):
            for y in range(2):
                for core in range(2):
                    @pl.when(inner & (lax.rem(me, 4) == 2 * y + core))
                    def _():
                        for a in range(2):
                            for t in range(half):
                                act(stream(a, t, y)[core])

        streams(start)
        for to, ok in zip(near, apart):
            @pl.when(inner & ok)
            def _():
                both(to, start)

    pos = [lens_ref[me * rows + b] for b in range(rows)]

    for name in ("freq", "x", "gain", "bq", "bk", "bv", "wk", "wv", "wq"):
        loads[name].wait()
    wide = xs[...].astype(F32)
    inv = lax.rsqrt(jnp.mean(wide * wide, axis=-1, keepdims=True) + RMS_EPS)
    gains = jnp.concatenate([gain[i:i + 1, :].astype(F32) for i in range(heads)], axis=1)
    normed = (wide * inv * gains).astype(BF16)
    which = lax.broadcasted_iota(jnp.int32, (rows, dim), 0)
    lane = lax.broadcasted_iota(jnp.int32, (rows, dim), 1)
    posf = jnp.zeros((rows, dim), F32)
    for b in range(rows):
        posf = jnp.where(which == b, pos[b].astype(F32), posf)
    angle = posf * freq_ref[...]
    cos_t = jnp.cos(angle)
    sin_t = jnp.sin(angle)
    sin_t = jnp.where(lane < dim // 2, -sin_t, sin_t)

    def rotate(t):
        return (t * cos_t + pltpu.roll(t, dim // 2, 1) * sin_t).astype(BF16).astype(F32)

    for i in range(2):
        cols = pl.ds(i * dim, dim)
        kn_s[:, i, :] = rotate(jnp.dot(normed, wk[:, cols], preferred_element_type=F32) + bk[i:i + 1, :].astype(F32))
        vn_s[:, i, :] = (jnp.dot(normed, wv[:, cols], preferred_element_type=F32) + bv[i:i + 1, :].astype(F32)).astype(BF16).astype(F32)
    for i in range(heads):
        q_s[:, i, :] = rotate(jnp.dot(normed, wq[:, i * dim:(i + 1) * dim], preferred_element_type=F32) + bq[i:i + 1, :].astype(F32))

    row = lax.broadcasted_iota(jnp.int32, (m, dim), 0)
    even = lax.rem(row, 2) == 0

    def merge(raw, new, out, b, i):
        at = 2 * pos[b] - i * m
        fresh = jnp.where(even, new[b, 0:1, :], new[b, 1:2, :])
        merged = jnp.where(row < at, raw.astype(F32), jnp.where(row < at + 2, fresh, 0.0)).astype(BF16)
        out[b, i] = merged
        return merged

    def k_block(i, get):
        cols = pl.ds(pl.multiple_of(i * m, m), m)
        for b in range(rows):
            keys = merge(get(b), kn_s, ko_ref, b, i)
            s_s[b, :, cols] = lax.dot_general(q_s[b].astype(BF16), keys, (((1,), (1,)), ((), ())), preferred_element_type=F32) * (dim ** -0.5)

    def v_block(i, get):
        cols = pl.ds(pl.multiple_of(i * m, m), m)
        for b in range(rows):
            vals = merge(get(b), vn_s, vo_ref, b, i)
            acc[b] += jnp.dot(e_s[b, :, cols], vals, preferred_element_type=F32)

    def direct(a, block):
        def visit(d, c):
            src = lax.rem(me + n - d, n)

            def go():
                arrive(a, src)
                block(src, lambda b: pairs[a][1][b, src])

            if pooled:
                pl.when((lax.div(src, half) == high) | (lax.rem(lax.div(src, 4) + lax.div(src, half), 2) == 0))(go)
            else:
                go()
            return c

        lax.fori_loop(1, n, visit, 0)

    def pooled_blocks(a, block):
        for u in range(4):
            c = PIECE[u]
            for side in range(2):
                @pl.when(h > 0 if side == 0 else h < half - 1)
                def _():
                    forward(a, u, 1 - side).wait_recv()
        for u in range(4):
            c = PIECE[u]
            i = half - 4 * high + u

            def get(b):
                loc = place_s[u, h * rows + b] - (h - 1) * c
                return land[a][u][jnp.clip(loc, 0, 3 * c - 1)]

            block(i, get)

    def forward(a, u, side):
        c = PIECE[u]
        to = high * half + lax.rem(h + (1 if side else half - 1), half)
        return pltpu.make_async_remote_copy(
            src_ref=land[a][u].at[pl.ds(c, c)], dst_ref=land[a][u].at[pl.ds(0 if side else 2 * c, c)], send_sem=fw_send.at[a, u, side], recv_sem=fw_recv.at[a, u, side],
            device_id={"cp": to}, device_id_type=MESH)

    def forwards(a, u, act):
        @pl.when(h < half - 1)
        def _():
            act(forward(a, u, 1))

        @pl.when(h > 0)
        def _():
            act(forward(a, u, 0))

    if pooled:
        for a in range(2):
            for u in range(4):
                c = PIECE[u]
                pltpu.make_async_remote_copy(
                    src_ref=packs[a].at[pl.ds(0, c)], dst_ref=land[a][u].at[pl.ds(c, c)], send_sem=st_send.at[a, 0], recv_sem=st_recv.at[a, u],
                    device_id={"cp": me}, device_id_type=MESH).wait_recv()
                forwards(a, u, start)

        streams(sent)

        @pl.when(inner)
        def _():
            for u in range(4):
                pl.semaphore_signal(gate, inc=1, device_id={"cp": 3 * half * high // 2 + u}, device_id_type=MESH)

        @pl.when(outer)
        def _():
            pl.semaphore_wait(gate, 4)
            send(1, far[0]).start()
            for to in far[1:]:
                both(to, start)

    loads["k"].wait()
    k_block(me, lambda b: k_land[b, me])
    direct(0, k_block)
    if pooled:
        pooled_blocks(0, k_block)

    col = lax.broadcasted_iota(jnp.int32, (heads, n * m), 1)
    head = lax.broadcasted_iota(jnp.int32, (heads, n * m), 0)
    own = lax.rem(col, 2) == lax.div(head, heads // 2)
    for b in range(rows):
        valid = own & (col < 2 * pos[b] + 2)
        s = jnp.where(valid, s_s[b], -1e30)
        e = jnp.where(valid, jnp.exp(s - jnp.max(s, axis=-1, keepdims=True)), 0.0)
        l_s[b] = jnp.broadcast_to(jnp.sum(e, axis=-1, keepdims=True), (heads, dim))
        e_s[b] = e.astype(BF16)
    acc[...] = jnp.zeros_like(acc)

    loads["v"].wait()
    v_block(me, lambda b: v_land[b, me])
    loads["wo"].wait()
    if pooled:
        pooled_blocks(1, v_block)
    direct(1, v_block)

    acc[...] = acc[...] / l_s[...]
    att_ref[...] = jnp.concatenate([acc[:, i, :] for i in range(heads)], axis=1).astype(BF16)

    if not pooled:
        for d in range(1, n):
            both(lax.rem(me + d, n), sent)
    else:
        for to in near:
            both(to, sent)

        @pl.when(outer)
        def _():
            for to in far:
                both(to, sent)

        for a in range(2):
            for u in range(4):
                forwards(a, u, sent)


def step(pooled, lens, freq, x, gain, b_q, b_k, b_v, w_q, w_k, w_v, w_o, k, v):
    n, rows, m, dim = k.shape
    heads = w_q.shape[1] // dim
    kv = w_k.shape[1] // dim
    half = n // 2
    cache = pltpu.VMEM((rows, n, m, dim), BF16)
    hbm = pl.BlockSpec(memory_space=pltpu.HBM)
    vmem = pl.BlockSpec(memory_space=pltpu.VMEM)
    dma = pltpu.SemaphoreType.DMA
    scratch = [
        pltpu.SMEM(lens.shape, jnp.int32), pltpu.VMEM(freq.shape, F32),
        pltpu.VMEM((rows, n, m, dim), BF16), pltpu.VMEM((rows, n, m, dim), BF16),
        pltpu.VMEM(w_q.shape, BF16), pltpu.VMEM(w_k.shape, BF16), pltpu.VMEM(w_v.shape, BF16),
        pltpu.VMEM(x.shape, BF16), pltpu.VMEM(gain.shape, BF16), pltpu.VMEM(b_q.shape, BF16), pltpu.VMEM(b_k.shape, BF16), pltpu.VMEM(b_v.shape, BF16),
        pltpu.VMEM((rows, heads, dim), F32), pltpu.VMEM((rows, kv, dim), F32), pltpu.VMEM((rows, kv, dim), F32),
        pltpu.VMEM((rows, heads, n * m), F32), pltpu.VMEM((rows, heads, n * m), BF16), pltpu.VMEM((rows, heads, dim), F32),
        pltpu.VMEM((rows, heads, dim), F32),
        dma((2, n)), dma((2, n)), dma((13,))]
    if pooled:
        scratch += [pltpu.VMEM((half * rows, m, dim), BF16)] * 2 + [pltpu.VMEM((half * max(PIECE), m, dim), BF16)] * 2
        scratch += [pltpu.SMEM((half * rows + 1,), jnp.int32), pltpu.SMEM((half * max(PIECE),), jnp.int32), pltpu.SMEM((4, half * rows), jnp.int32)]
        scratch += [dma((2, half)), dma((2, half)), dma((2, 4)), dma((2, 4, 2)), dma((2, 4, 2)), pltpu.SemaphoreType.REGULAR]
        scratch += [pltpu.VMEM((3 * c, m, dim), BF16) for _ in range(2) for c in PIECE]
    return pl.pallas_call(
        functools.partial(step_kernel, n, pooled),
        out_shape=[pltpu.VMEM(x.shape, BF16), cache, cache, pltpu.VMEM(w_o.shape, BF16)],
        in_specs=[hbm] * 13,
        out_specs=[vmem] * 4,
        scratch_shapes=scratch,
        compiler_params=pltpu.CompilerParams(collective_id=int(pooled), has_side_effects=True, vmem_limit_bytes=47 * 1024 * 1024),
    )(lens, freq, x, gain, b_q, b_k, b_v, w_q, w_k, w_v, w_o, k, v)


def fits(lens, n, rows, slots):
    half = n // 2
    c = np.array(PIECE * 2)[:, None, None]
    src = np.arange(n // 4, n - n // 4)
    k, j = np.arange(half)[None, :, None], np.arange(half)[None, None, :]
    room = np.minimum((j + 2) * c, half * c) - np.maximum(k - 1, 0) * c
    room = np.where(k <= j, room, n * rows)
    owner = np.arange(half * rows) // rows
    between = (owner >= np.arange(half)[:, None, None]) & (owner <= np.arange(half)[None, :, None])
    seqs = jnp.concatenate([jnp.broadcast_to(lens[half * rows:], (half // 2, half * rows)), jnp.broadcast_to(lens[:half * rows], (half // 2, half * rows))])
    need = (seqs > jnp.asarray(src * slots)[:, None]).astype(F32)
    used = jnp.dot(need, jnp.asarray(between.reshape(half * half, -1).T.astype(np.float32)))
    return jnp.all(used <= jnp.asarray(room.reshape(half, -1).astype(np.float32)))


def finish_kernel(x_ref, att_ref, wo_ref, k_ref, v_ref, y_ref, ko_ref, vo_ref, sem):
    copies = [pltpu.make_async_copy(k_ref, ko_ref, sem.at[0]), pltpu.make_async_copy(v_ref, vo_ref, sem.at[1])]
    for copy in copies:
        copy.start()
    tile = 256
    for t in range(wo_ref.shape[1] // tile):
        cols = slice(t * tile, (t + 1) * tile)
        y_ref[:, cols] = (x_ref[:, cols].astype(F32) + jnp.dot(att_ref[...], wo_ref[:, cols], preferred_element_type=F32)).astype(BF16)
    for copy in copies:
        copy.wait()


def finish(x, att, w_o, k, v):
    vmem = pl.BlockSpec(memory_space=pltpu.VMEM)
    hbm = pl.BlockSpec(memory_space=pltpu.HBM)
    cache = jax.ShapeDtypeStruct(k.shape, BF16)
    return pl.pallas_call(
        finish_kernel,
        out_shape=[jax.ShapeDtypeStruct(x.shape, BF16), cache, cache],
        in_specs=[vmem] * 5,
        out_specs=[vmem, hbm, hbm],
        scratch_shapes=[pltpu.SemaphoreType.DMA((2,))],
        compiler_params=pltpu.CompilerParams(vmem_limit_bytes=4 * 1024 * 1024),
    )(x, att, w_o, k, v)


def solution(mesh):
    batch_spec = P(('dp', 'cp'))
    seq_spec = P('dp', 'cp')
    whole = P()

    def per_device(x_tok, prompt_lens, k_cache, v_cache, norm_gain, w_q, b_q, w_k, b_k, w_v, b_v, w_o):
        rows = x_tok.shape[0]
        batch, slots, kv_heads, dim = k_cache.shape
        n = batch // rows
        inv_freq = np.power(np.float32(ROPE_THETA), -(np.arange(dim // 2, dtype=np.float32) * 2.0 / dim)).astype(np.float32)
        freq = jnp.asarray(np.concatenate([inv_freq, inv_freq])[None, :])
        pack = (n, rows, slots * kv_heads, dim)
        args = (prompt_lens, freq, x_tok, norm_gain.reshape(-1, dim), b_q.reshape(-1, dim), b_k.reshape(-1, dim), b_v.reshape(-1, dim),
                w_q, w_k, w_v, w_o, k_cache.reshape(pack), v_cache.reshape(pack))

        def run(pooled, *args):
            att, k_all, v_all, wo = step(pooled, *args)
            return finish(x_tok, att, wo, k_all, v_all)

        y_out, k_out, v_out = lax.cond(fits(prompt_lens, n, rows, slots), functools.partial(run, True), functools.partial(run, False), *args)
        shape = (rows, n * slots, kv_heads, dim)
        return y_out, k_out.reshape(shape), v_out.reshape(shape)

    return jax.shard_map(per_device, mesh=mesh, in_specs=(batch_spec, P('dp'), seq_spec, seq_spec, whole, whole, whole, whole, whole, whole, whole, whole), out_specs=(batch_spec, batch_spec, batch_spec), check_vma=False)
```

```python
import functools
import numpy as np
import jax
import jax.numpy as jnp
from jax import lax
from jax.experimental import pallas as pl
from jax.experimental.pallas import tpu as pltpu
from jax.sharding import PartitionSpec as P

RMS_EPS = 1e-6
ROPE_THETA = 1000000.0
MESH = pl.DeviceIdType.MESH
F32 = jnp.float32
BF16 = jnp.bfloat16


def flip(me, d):
    out = 0
    for k in range(4):
        bit = 1 << k
        out = out + bit * lax.rem(lax.div(me, bit) + lax.div(d, bit), 2)
    return out


PIECE = (7, 7, 6, 6)


def step_kernel(n, pooled, lens_hbm, freq_hbm, x_ref, gain_ref, bq_ref, bk_ref, bv_ref, wq_ref, wk_ref, wv_ref, wo_ref, k_ref, v_ref,
                att_ref, ko_ref, vo_ref, wo,
                lens_ref, freq_ref, k_land, v_land, wq, wk, wv, xs, gain, bq, bk, bv,
                q_s, kn_s, vn_s, s_s, e_s, l_s, acc, send_sem, recv_sem, load_sem, *pool):
    me = lax.axis_index("cp")
    rows, heads, dim = q_s.shape
    m = k_land.shape[2]
    half = n // 2
    high = lax.div(me, half)
    h = lax.rem(me, half)
    other = (1 - high) * half
    inner = lax.rem(lax.div(me, 4) + high, 2) == 1
    outer = lax.rem(lax.div(me, 4) + high, 2) == 0
    loads = {}
    for idx, (name, src, dst) in enumerate([
            ("lens", lens_hbm, lens_ref), ("freq", freq_hbm, freq_ref), ("x", x_ref, xs), ("gain", gain_ref, gain), ("bq", bq_ref, bq), ("bk", bk_ref, bk), ("bv", bv_ref, bv),
            ("wk", wk_ref, wk), ("wv", wv_ref, wv), ("wq", wq_ref, wq),
            ("k", k_ref.at[me], k_land.at[:, me]), ("v", v_ref.at[me], v_land.at[:, me]), ("wo", wo_ref, wo)]):
        loads[name] = pltpu.make_async_copy(src, dst, load_sem.at[idx])

    pairs = ((k_ref, k_land), (v_ref, v_land))

    def send(a, to):
        return pltpu.make_async_remote_copy(
            src_ref=pairs[a][0].at[to], dst_ref=pairs[a][1].at[:, me], send_sem=send_sem.at[a, to], recv_sem=recv_sem.at[a, me],
            device_id={"cp": to}, device_id_type=MESH)

    def arrive(a, src):
        pltpu.make_async_remote_copy(
            src_ref=pairs[a][0].at[0], dst_ref=pairs[a][1].at[:, src], send_sem=send_sem.at[a, src], recv_sem=recv_sem.at[a, src],
            device_id={"cp": src}, device_id_type=MESH).wait_recv()

    def both(to, act):
        for a in range(2):
            act(send(a, to))

    def start(copy):
        copy.start()

    def sent(copy):
        copy.wait_send()

    barrier = pltpu.get_barrier_semaphore()
    for d in range(1, n):
        pl.semaphore_signal(barrier, inc=1, device_id={"cp": lax.rem(me + d, n)}, device_id_type=MESH)
    loads["lens"].start()
    if pooled:
        (k_all, v_all, k_pack, v_pack, next_s, pick_s, place_s, gather_sem, st_send, st_recv, fw_send, fw_recv), land = pool[:12], (pool[12:16], pool[16:20])
        caches, packs = (k_all, v_all), (k_pack, v_pack)

        def gather(a, j):
            return pltpu.make_async_copy(pairs[a][0].at[other + j], caches[a].at[pl.ds(j * rows, rows)], gather_sem.at[a, j])

        @pl.when(inner)
        def _():
            for a in range(2):
                for j in range(half):
                    gather(a, j).start()

    for name, copy in loads.items():
        if name != "lens":
            copy.start()
    pl.semaphore_wait(barrier, n - 1)

    if not pooled:
        for d in range(1, n):
            both(lax.rem(me + d, n), start)
        loads["lens"].wait()
    else:
        near = [high * half + lax.rem(h + t, half) for t in range(1, half)]
        far = [other + lax.rem(h + t, half) for t in range(half)]

        @pl.when(outer)
        def _():
            for to in far:
                both(to, start)

        for to in near:
            both(to, start)

        loads["lens"].wait()
        mine = jnp.where(lax.rem(me, 4) < 2, PIECE[0], PIECE[2])

        @pl.when(inner)
        def _():
            next_s[half * rows] = half * rows

            def back(t, carry):
                b = half * rows - 1 - t
                nx = jnp.where(lens_ref[other * rows + b] > (m // 2) * me, b, carry)
                next_s[b] = nx
                return nx

            lax.fori_loop(0, half * rows, back, half * rows, unroll=8)

            def fill(s, cur):
                cand = next_s[cur]
                ok = s >= (lax.shift_right_logical(cand, 3) - 1) * mine
                pick_s[s] = jnp.minimum(cand, half * rows - 1)
                return jnp.where(ok, jnp.minimum(cand + 1, half * rows), cur)

            lax.fori_loop(0, half * max(PIECE), fill, 0, unroll=8)
            for a in range(2):
                for j in range(half):
                    gather(a, j).wait()

            def pack(s, c):
                b = pick_s[s]
                for a in range(2):
                    packs[a][s] = caches[a][b]
                return c

            lax.fori_loop(0, half * max(PIECE), pack, 0, unroll=4)

        def place(b, ends):
            length = lens_ref[high * half * rows + b]
            out = []
            for u in range(4):
                at = jnp.maximum(ends[u], (lax.div(b, rows) - 1) * PIECE[u])
                place_s[u, b] = at
                out.append(jnp.where(length > (m // 2) * (half - 4 * high + u), at + 1, ends[u]))
            return tuple(out)

        lax.fori_loop(0, half * rows, place, (0, 0, 0, 0), unroll=4)

        def stream(a, t, y):
            c = PIECE[2 * y]
            u = lax.rem(me, 4)
            j = lax.rem(2 * u + t, half)
            return [pltpu.make_async_remote_copy(
                src_ref=packs[a].at[pl.ds(j * c, c)], dst_ref=land[a][2 * y + core].at[pl.ds(c, c)], send_sem=st_send.at[a, t], recv_sem=st_recv.at[a, 2 * y + core],
                device_id={"cp": other + j}, device_id_type=MESH) for core in range(2)]

        def streams(act):
            for y in range(2):
                for core in range(2):
                    @pl.when(inner & (lax.rem(me, 4) == 2 * y + core))
                    def _():
                        for a in range(2):
                            for t in range(half):
                                act(stream(a, t, y)[core])

        streams(start)

    pos = [lens_ref[me * rows + b] for b in range(rows)]

    for name in ("freq", "x", "gain", "bq", "bk", "bv", "wk", "wv", "wq"):
        loads[name].wait()
    wide = xs[...].astype(F32)
    inv = lax.rsqrt(jnp.mean(wide * wide, axis=-1, keepdims=True) + RMS_EPS)
    gains = jnp.concatenate([gain[i:i + 1, :].astype(F32) for i in range(heads)], axis=1)
    normed = (wide * inv * gains).astype(BF16)
    which = lax.broadcasted_iota(jnp.int32, (rows, dim), 0)
    lane = lax.broadcasted_iota(jnp.int32, (rows, dim), 1)
    posf = jnp.zeros((rows, dim), F32)
    for b in range(rows):
        posf = jnp.where(which == b, pos[b].astype(F32), posf)
    angle = posf * freq_ref[...]
    cos_t = jnp.cos(angle)
    sin_t = jnp.sin(angle)
    sin_t = jnp.where(lane < dim // 2, -sin_t, sin_t)

    def rotate(t):
        return (t * cos_t + pltpu.roll(t, dim // 2, 1) * sin_t).astype(BF16).astype(F32)

    for i in range(2):
        cols = pl.ds(i * dim, dim)
        kn_s[:, i, :] = rotate(jnp.dot(normed, wk[:, cols], preferred_element_type=F32) + bk[i:i + 1, :].astype(F32))
        vn_s[:, i, :] = (jnp.dot(normed, wv[:, cols], preferred_element_type=F32) + bv[i:i + 1, :].astype(F32)).astype(BF16).astype(F32)
    for i in range(heads):
        q_s[:, i, :] = rotate(jnp.dot(normed, wq[:, i * dim:(i + 1) * dim], preferred_element_type=F32) + bq[i:i + 1, :].astype(F32))

    row = lax.broadcasted_iota(jnp.int32, (m, dim), 0)
    even = lax.rem(row, 2) == 0

    def merge(raw, new, out, b, i):
        at = 2 * pos[b] - i * m
        fresh = jnp.where(even, new[b, 0:1, :], new[b, 1:2, :])
        merged = jnp.where(row < at, raw.astype(F32), jnp.where(row < at + 2, fresh, 0.0)).astype(BF16)
        out[b, i] = merged
        return merged

    def k_block(i, get):
        cols = pl.ds(pl.multiple_of(i * m, m), m)
        for b in range(rows):
            keys = merge(get(b), kn_s, ko_ref, b, i)
            s_s[b, :, cols] = lax.dot_general(q_s[b].astype(BF16), keys, (((1,), (1,)), ((), ())), preferred_element_type=F32) * (dim ** -0.5)

    def v_block(i, get):
        cols = pl.ds(pl.multiple_of(i * m, m), m)
        for b in range(rows):
            vals = merge(get(b), vn_s, vo_ref, b, i)
            acc[b] += jnp.dot(e_s[b, :, cols], vals, preferred_element_type=F32)

    def direct(a, block):
        def visit(d, c):
            src = lax.rem(me + n - d, n)

            def go():
                arrive(a, src)
                block(src, lambda b: pairs[a][1][b, src])

            if pooled:
                pl.when((lax.div(src, half) == high) | (lax.rem(lax.div(src, 4) + lax.div(src, half), 2) == 0))(go)
            else:
                go()
            return c

        lax.fori_loop(1, n, visit, 0)

    def pooled_blocks(a, block):
        for u in range(4):
            c = PIECE[u]
            for side in range(2):
                @pl.when(h > 0 if side == 0 else h < half - 1)
                def _():
                    forward(a, u, 1 - side).wait_recv()
        for u in range(4):
            c = PIECE[u]
            i = half - 4 * high + u

            def get(b):
                loc = place_s[u, h * rows + b] - (h - 1) * c
                return land[a][u][jnp.clip(loc, 0, 3 * c - 1)]

            block(i, get)

    def forward(a, u, side):
        c = PIECE[u]
        to = high * half + lax.rem(h + (1 if side else half - 1), half)
        return pltpu.make_async_remote_copy(
            src_ref=land[a][u].at[pl.ds(c, c)], dst_ref=land[a][u].at[pl.ds(0 if side else 2 * c, c)], send_sem=fw_send.at[a, u, side], recv_sem=fw_recv.at[a, u, side],
            device_id={"cp": to}, device_id_type=MESH)

    def forwards(a, u, act):
        @pl.when(h < half - 1)
        def _():
            act(forward(a, u, 1))

        @pl.when(h > 0)
        def _():
            act(forward(a, u, 0))

    def relay(a):
        for r in range(4):
            for u in range(4):
                @pl.when(lax.rem(lax.div(h, 2) + 4 - r, 4) == u)
                def _():
                    c = PIECE[u]
                    pltpu.make_async_remote_copy(
                        src_ref=packs[a].at[pl.ds(0, c)], dst_ref=land[a][u].at[pl.ds(c, c)], send_sem=st_send.at[a, 0], recv_sem=st_recv.at[a, u],
                        device_id={"cp": me}, device_id_type=MESH).wait_recv()
                    forwards(a, u, start)

    loads["k"].wait()
    k_block(me, lambda b: k_land[b, me])
    direct(0, k_block)
    if pooled:
        relay(0)
        pooled_blocks(0, k_block)

    col = lax.broadcasted_iota(jnp.int32, (heads, n * m), 1)
    head = lax.broadcasted_iota(jnp.int32, (heads, n * m), 0)
    own = lax.rem(col, 2) == lax.div(head, heads // 2)
    for b in range(rows):
        valid = own & (col < 2 * pos[b] + 2)
        s = jnp.where(valid, s_s[b], -1e30)
        e = jnp.where(valid, jnp.exp(s - jnp.max(s, axis=-1, keepdims=True)), 0.0)
        l_s[b] = jnp.broadcast_to(jnp.sum(e, axis=-1, keepdims=True), (heads, dim))
        e_s[b] = e.astype(BF16)
    acc[...] = jnp.zeros_like(acc)

    loads["v"].wait()
    v_block(me, lambda b: v_land[b, me])
    loads["wo"].wait()
    direct(1, v_block)
    if pooled:
        relay(1)
        pooled_blocks(1, v_block)

    acc[...] = acc[...] / l_s[...]
    att_ref[...] = jnp.concatenate([acc[:, i, :] for i in range(heads)], axis=1).astype(BF16)

    if not pooled:
        for d in range(1, n):
            both(lax.rem(me + d, n), sent)
    else:
        for to in near:
            both(to, sent)

        @pl.when(outer)
        def _():
            for to in far:
                both(to, sent)

        streams(sent)
        for a in range(2):
            for u in range(4):
                forwards(a, u, sent)


def step(pooled, lens, freq, x, gain, b_q, b_k, b_v, w_q, w_k, w_v, w_o, k, v):
    n, rows, m, dim = k.shape
    heads = w_q.shape[1] // dim
    kv = w_k.shape[1] // dim
    half = n // 2
    cache = pltpu.VMEM((rows, n, m, dim), BF16)
    hbm = pl.BlockSpec(memory_space=pltpu.HBM)
    vmem = pl.BlockSpec(memory_space=pltpu.VMEM)
    dma = pltpu.SemaphoreType.DMA
    scratch = [
        pltpu.SMEM(lens.shape, jnp.int32), pltpu.VMEM(freq.shape, F32),
        pltpu.VMEM((rows, n, m, dim), BF16), pltpu.VMEM((rows, n, m, dim), BF16),
        pltpu.VMEM(w_q.shape, BF16), pltpu.VMEM(w_k.shape, BF16), pltpu.VMEM(w_v.shape, BF16),
        pltpu.VMEM(x.shape, BF16), pltpu.VMEM(gain.shape, BF16), pltpu.VMEM(b_q.shape, BF16), pltpu.VMEM(b_k.shape, BF16), pltpu.VMEM(b_v.shape, BF16),
        pltpu.VMEM((rows, heads, dim), F32), pltpu.VMEM((rows, kv, dim), F32), pltpu.VMEM((rows, kv, dim), F32),
        pltpu.VMEM((rows, heads, n * m), F32), pltpu.VMEM((rows, heads, n * m), BF16), pltpu.VMEM((rows, heads, dim), F32),
        pltpu.VMEM((rows, heads, dim), F32),
        dma((2, n)), dma((2, n)), dma((13,))]
    if pooled:
        scratch += [pltpu.VMEM((half * rows, m, dim), BF16)] * 2 + [pltpu.VMEM((half * max(PIECE), m, dim), BF16)] * 2
        scratch += [pltpu.SMEM((half * rows + 1,), jnp.int32), pltpu.SMEM((half * max(PIECE),), jnp.int32), pltpu.SMEM((4, half * rows), jnp.int32)]
        scratch += [dma((2, half)), dma((2, half)), dma((2, 4)), dma((2, 4, 2)), dma((2, 4, 2))]
        scratch += [pltpu.VMEM((3 * c, m, dim), BF16) for _ in range(2) for c in PIECE]
    return pl.pallas_call(
        functools.partial(step_kernel, n, pooled),
        out_shape=[pltpu.VMEM(x.shape, BF16), cache, cache, pltpu.VMEM(w_o.shape, BF16)],
        in_specs=[hbm] * 13,
        out_specs=[vmem] * 4,
        scratch_shapes=scratch,
        compiler_params=pltpu.CompilerParams(collective_id=int(pooled), has_side_effects=True, vmem_limit_bytes=47 * 1024 * 1024),
    )(lens, freq, x, gain, b_q, b_k, b_v, w_q, w_k, w_v, w_o, k, v)


def fits(lens, n, rows, slots):
    half = n // 2
    c = np.array(PIECE * 2)[:, None, None]
    src = np.arange(n // 4, n - n // 4)
    k, j = np.arange(half)[None, :, None], np.arange(half)[None, None, :]
    room = np.minimum((j + 2) * c, half * c) - np.maximum(k - 1, 0) * c
    room = np.where(k <= j, room, n * rows)
    owner = np.arange(half * rows) // rows
    between = (owner >= np.arange(half)[:, None, None]) & (owner <= np.arange(half)[None, :, None])
    seqs = jnp.concatenate([jnp.broadcast_to(lens[half * rows:], (half // 2, half * rows)), jnp.broadcast_to(lens[:half * rows], (half // 2, half * rows))])
    need = (seqs > jnp.asarray(src * slots)[:, None]).astype(F32)
    used = jnp.dot(need, jnp.asarray(between.reshape(half * half, -1).T.astype(np.float32)))
    return jnp.all(used <= jnp.asarray(room.reshape(half, -1).astype(np.float32)))


def finish_kernel(x_ref, att_ref, wo_ref, k_ref, v_ref, y_ref, ko_ref, vo_ref, sem):
    copies = [pltpu.make_async_copy(k_ref, ko_ref, sem.at[0]), pltpu.make_async_copy(v_ref, vo_ref, sem.at[1])]
    for copy in copies:
        copy.start()
    tile = 256
    for t in range(wo_ref.shape[1] // tile):
        cols = slice(t * tile, (t + 1) * tile)
        y_ref[:, cols] = (x_ref[:, cols].astype(F32) + jnp.dot(att_ref[...], wo_ref[:, cols], preferred_element_type=F32)).astype(BF16)
    for copy in copies:
        copy.wait()


def finish(x, att, w_o, k, v):
    vmem = pl.BlockSpec(memory_space=pltpu.VMEM)
    hbm = pl.BlockSpec(memory_space=pltpu.HBM)
    cache = jax.ShapeDtypeStruct(k.shape, BF16)
    return pl.pallas_call(
        finish_kernel,
        out_shape=[jax.ShapeDtypeStruct(x.shape, BF16), cache, cache],
        in_specs=[vmem] * 5,
        out_specs=[vmem, hbm, hbm],
        scratch_shapes=[pltpu.SemaphoreType.DMA((2,))],
        compiler_params=pltpu.CompilerParams(vmem_limit_bytes=4 * 1024 * 1024),
    )(x, att, w_o, k, v)


def solution(mesh):
    batch_spec = P(('dp', 'cp'))
    seq_spec = P('dp', 'cp')
    whole = P()

    def per_device(x_tok, prompt_lens, k_cache, v_cache, norm_gain, w_q, b_q, w_k, b_k, w_v, b_v, w_o):
        rows = x_tok.shape[0]
        batch, slots, kv_heads, dim = k_cache.shape
        n = batch // rows
        inv_freq = np.power(np.float32(ROPE_THETA), -(np.arange(dim // 2, dtype=np.float32) * 2.0 / dim)).astype(np.float32)
        freq = jnp.asarray(np.concatenate([inv_freq, inv_freq])[None, :])
        pack = (n, rows, slots * kv_heads, dim)
        args = (prompt_lens, freq, x_tok, norm_gain.reshape(-1, dim), b_q.reshape(-1, dim), b_k.reshape(-1, dim), b_v.reshape(-1, dim),
                w_q, w_k, w_v, w_o, k_cache.reshape(pack), v_cache.reshape(pack))

        def run(pooled, *args):
            att, k_all, v_all, wo = step(pooled, *args)
            return finish(x_tok, att, wo, k_all, v_all)

        y_out, k_out, v_out = lax.cond(fits(prompt_lens, n, rows, slots), functools.partial(run, True), functools.partial(run, False), *args)
        shape = (rows, n * slots, kv_heads, dim)
        return y_out, k_out.reshape(shape), v_out.reshape(shape)

    return jax.shard_map(per_device, mesh=mesh, in_specs=(batch_spec, P('dp'), seq_spec, seq_spec, whole, whole, whole, whole, whole, whole, whole, whole), out_specs=(batch_spec, batch_spec, batch_spec), check_vma=False)
```

```python
import functools
import numpy as np
import jax
import jax.numpy as jnp
from jax import lax
from jax.experimental import pallas as pl
from jax.experimental.pallas import tpu as pltpu
from jax.sharding import PartitionSpec as P

RMS_EPS = 1e-6
ROPE_THETA = 1000000.0
MESH = pl.DeviceIdType.MESH
F32 = jnp.float32
BF16 = jnp.bfloat16


def flip(me, d):
    out = 0
    for k in range(4):
        bit = 1 << k
        out = out + bit * lax.rem(lax.div(me, bit) + lax.div(d, bit), 2)
    return out


def step_kernel(n, lens_hbm, freq_hbm, x_ref, gain_ref, bq_ref, bk_ref, bv_ref, wq_ref, wk_ref, wv_ref, wo_ref, k_ref, v_ref,
                att_ref, ko_ref, vo_ref, wo,
                lens_ref, freq_ref, k_land, v_land, wq, wk, wv, xs, gain, bq, bk, bv,
                q_s, kn_s, vn_s, s_s, e_s, l_s, acc, send_sem, recv_sem, load_sem, turn):
    me = lax.axis_index("cp")
    rows, heads, dim = q_s.shape
    m = k_land.shape[2]
    width = heads * dim
    loads = {}
    for idx, (name, src, dst) in enumerate([
            ("lens", lens_hbm, lens_ref), ("freq", freq_hbm, freq_ref), ("x", x_ref, xs), ("gain", gain_ref, gain), ("bq", bq_ref, bq), ("bk", bk_ref, bk), ("bv", bv_ref, bv),
            ("wk", wk_ref, wk), ("wv", wv_ref, wv), ("wq", wq_ref, wq),
            ("k", k_ref.at[me], k_land.at[:, me]), ("v", v_ref.at[me], v_land.at[:, me]), ("wo", wo_ref, wo)]):
        loads[name] = pltpu.make_async_copy(src, dst, load_sem.at[idx])

    barrier = pltpu.get_barrier_semaphore()
    for d in range(1, n):
        pl.semaphore_signal(barrier, inc=1, device_id={"cp": lax.rem(me + d, n)}, device_id_type=MESH)
    for copy in loads.values():
        copy.start()
    pl.semaphore_wait(barrier, n - 1)

    pairs = ((k_ref, k_land), (v_ref, v_land))

    def send(a, to):
        return pltpu.make_async_remote_copy(
            src_ref=pairs[a][0].at[to], dst_ref=pairs[a][1].at[:, me], send_sem=send_sem.at[a, to], recv_sem=recv_sem.at[a, me],
            device_id={"cp": to}, device_id_type=MESH)

    def arrive(a, d):
        src = lax.rem(me + n - d, n)
        pltpu.make_async_remote_copy(
            src_ref=pairs[a][0].at[0], dst_ref=pairs[a][1].at[:, src], send_sem=send_sem.at[a, src], recv_sem=recv_sem.at[a, src],
            device_id={"cp": src}, device_id_type=MESH).wait_recv()
        return src

    half, layer = n // 2, n // 4
    z = lax.div(me, layer)
    high = lax.div(me, half)
    end = lax.rem(z + high, 2) == 0
    middle = lax.rem(z + high, 2) == 1
    second = lax.rem(me, 2) == 1
    beside = [z * layer + lax.rem(me + t, layer) for t in range(1, layer)]
    near = [(4 * high + 1 - z) * layer + lax.rem(me + t, layer) for t in range(layer)]
    far = [(1 - high) * half + lax.rem(me + t, half) for t in range(half)]

    def each(targets, act):
        for to in targets:
            for a in range(2):
                act(send(a, to))

    def start(copy):
        copy.start()

    def sent(copy):
        copy.wait_send()

    each(beside, start)

    def along():
        pl.when(end)(lambda: each(near, start))
        each(far, start)
        pl.when(middle)(lambda: each(near, start))

    @pl.when(middle | (lax.rem(me, 2) == 0))
    def _():
        along()

    loads["lens"].wait()
    pos = [lens_ref[me * rows + b] for b in range(rows)]

    for name in ("freq", "x", "gain", "bq", "bk", "bv", "wk", "wv", "wq"):
        loads[name].wait()
    wide = xs[...].astype(F32)
    inv = lax.rsqrt(jnp.mean(wide * wide, axis=-1, keepdims=True) + RMS_EPS)
    gains = jnp.concatenate([gain[h:h + 1, :].astype(F32) for h in range(heads)], axis=1)
    normed = (wide * inv * gains).astype(BF16)
    which = lax.broadcasted_iota(jnp.int32, (rows, dim), 0)
    lane = lax.broadcasted_iota(jnp.int32, (rows, dim), 1)
    posf = jnp.zeros((rows, dim), F32)
    for b in range(rows):
        posf = jnp.where(which == b, pos[b].astype(F32), posf)
    angle = posf * freq_ref[...]
    cos_t = jnp.cos(angle)
    sin_t = jnp.sin(angle)
    sin_t = jnp.where(lane < dim // 2, -sin_t, sin_t)

    def rotate(t):
        return (t * cos_t + pltpu.roll(t, dim // 2, 1) * sin_t).astype(BF16).astype(F32)

    for h in range(2):
        cols = pl.ds(h * dim, dim)
        kn_s[:, h, :] = rotate(jnp.dot(normed, wk[:, cols], preferred_element_type=F32) + bk[h:h + 1, :].astype(F32))
        vn_s[:, h, :] = (jnp.dot(normed, wv[:, cols], preferred_element_type=F32) + bv[h:h + 1, :].astype(F32)).astype(BF16).astype(F32)
    for h in range(heads):
        q_s[:, h, :] = rotate(jnp.dot(normed, wq[:, h * dim:(h + 1) * dim], preferred_element_type=F32) + bq[h:h + 1, :].astype(F32))

    @pl.when(end & (lax.rem(me, 2) == 0))
    def _():
        each(near + far[:-1], sent)
        pl.semaphore_signal(turn, inc=1, device_id={"cp": me + 1}, device_id_type=MESH)

    @pl.when(end & second)
    def _():
        pl.semaphore_wait(turn, 1)
        along()

    row = lax.broadcasted_iota(jnp.int32, (m, dim), 0)
    even = lax.rem(row, 2) == 0

    def merge(land, new, out, b, i):
        at = 2 * pos[b] - i * m
        fresh = jnp.where(even, new[b, 0:1, :], new[b, 1:2, :])
        merged = jnp.where(row < at, land[b, i].astype(F32), jnp.where(row < at + 2, fresh, 0.0)).astype(BF16)
        out[b, i] = merged
        return merged

    def k_block(i):
        cols = pl.ds(pl.multiple_of(i * m, m), m)
        for b in range(rows):
            keys = merge(k_land, kn_s, ko_ref, b, i)
            s_s[b, :, cols] = lax.dot_general(q_s[b].astype(BF16), keys, (((1,), (1,)), ((), ())), preferred_element_type=F32) * (dim ** -0.5)

    def v_block(i):
        cols = pl.ds(pl.multiple_of(i * m, m), m)
        for b in range(rows):
            vals = merge(v_land, vn_s, vo_ref, b, i)
            acc[b] += jnp.dot(e_s[b, :, cols], vals, preferred_element_type=F32)

    def k_step(d, c):
        k_block(arrive(0, d))
        return c

    def v_step(d, c):
        v_block(arrive(1, d))
        return c

    loads["k"].wait()
    k_block(me)
    lax.fori_loop(1, n, k_step, 0)

    col = lax.broadcasted_iota(jnp.int32, (heads, n * m), 1)
    head = lax.broadcasted_iota(jnp.int32, (heads, n * m), 0)
    mine = lax.rem(col, 2) == lax.div(head, heads // 2)
    for b in range(rows):
        valid = mine & (col < 2 * pos[b] + 2)
        s = jnp.where(valid, s_s[b], -1e30)
        e = jnp.where(valid, jnp.exp(s - jnp.max(s, axis=-1, keepdims=True)), 0.0)
        l_s[b] = jnp.broadcast_to(jnp.sum(e, axis=-1, keepdims=True), (heads, dim))
        e_s[b] = e.astype(BF16)
    acc[...] = jnp.zeros_like(acc)

    loads["v"].wait()
    v_block(me)
    loads["wo"].wait()
    lax.fori_loop(1, n, v_step, 0)

    acc[...] = acc[...] / l_s[...]
    att_ref[...] = jnp.concatenate([acc[:, h, :] for h in range(heads)], axis=1).astype(BF16)

    each(beside + far[-1:], sent)

    @pl.when(middle | second)
    def _():
        each(near + far[:-1], sent)


def step(lens, freq, x, gain, b_q, b_k, b_v, w_q, w_k, w_v, w_o, k, v):
    n, rows, m, dim = k.shape
    heads = w_q.shape[1] // dim
    kv = w_k.shape[1] // dim
    cache = pltpu.VMEM((rows, n, m, dim), BF16)
    hbm = pl.BlockSpec(memory_space=pltpu.HBM)
    vmem = pl.BlockSpec(memory_space=pltpu.VMEM)
    return pl.pallas_call(
        functools.partial(step_kernel, n),
        out_shape=[pltpu.VMEM(x.shape, BF16), cache, cache, pltpu.VMEM(w_o.shape, BF16)],
        in_specs=[hbm] * 13,
        out_specs=[vmem] * 4,
        scratch_shapes=[
            pltpu.SMEM(lens.shape, jnp.int32), pltpu.VMEM(freq.shape, F32),
            pltpu.VMEM((rows, n, m, dim), BF16), pltpu.VMEM((rows, n, m, dim), BF16),
            pltpu.VMEM(w_q.shape, BF16), pltpu.VMEM(w_k.shape, BF16), pltpu.VMEM(w_v.shape, BF16),
            pltpu.VMEM(x.shape, BF16), pltpu.VMEM(gain.shape, BF16), pltpu.VMEM(b_q.shape, BF16), pltpu.VMEM(b_k.shape, BF16), pltpu.VMEM(b_v.shape, BF16),
            pltpu.VMEM((rows, heads, dim), F32), pltpu.VMEM((rows, kv, dim), F32), pltpu.VMEM((rows, kv, dim), F32),
            pltpu.VMEM((rows, heads, n * m), F32), pltpu.VMEM((rows, heads, n * m), BF16), pltpu.VMEM((rows, heads, dim), F32),
            pltpu.VMEM((rows, heads, dim), F32),
            pltpu.SemaphoreType.DMA((2, n)), pltpu.SemaphoreType.DMA((2, n)), pltpu.SemaphoreType.DMA((13,)), pltpu.SemaphoreType.REGULAR],
        compiler_params=pltpu.CompilerParams(collective_id=0, has_side_effects=True, vmem_limit_bytes=47 * 1024 * 1024),
    )(lens, freq, x, gain, b_q, b_k, b_v, w_q, w_k, w_v, w_o, k, v)


def finish_kernel(x_ref, att_ref, wo_ref, k_ref, v_ref, y_ref, ko_ref, vo_ref, sem):
    copies = [pltpu.make_async_copy(k_ref, ko_ref, sem.at[0]), pltpu.make_async_copy(v_ref, vo_ref, sem.at[1])]
    for copy in copies:
        copy.start()
    tile = 256
    for t in range(wo_ref.shape[1] // tile):
        cols = slice(t * tile, (t + 1) * tile)
        y_ref[:, cols] = (x_ref[:, cols].astype(F32) + jnp.dot(att_ref[...], wo_ref[:, cols], preferred_element_type=F32)).astype(BF16)
    for copy in copies:
        copy.wait()


def finish(x, att, w_o, k, v):
    vmem = pl.BlockSpec(memory_space=pltpu.VMEM)
    hbm = pl.BlockSpec(memory_space=pltpu.HBM)
    cache = jax.ShapeDtypeStruct(k.shape, BF16)
    return pl.pallas_call(
        finish_kernel,
        out_shape=[jax.ShapeDtypeStruct(x.shape, BF16), cache, cache],
        in_specs=[vmem] * 5,
        out_specs=[vmem, hbm, hbm],
        scratch_shapes=[pltpu.SemaphoreType.DMA((2,))],
        compiler_params=pltpu.CompilerParams(vmem_limit_bytes=4 * 1024 * 1024),
    )(x, att, w_o, k, v)


def solution(mesh):
    batch_spec = P(('dp', 'cp'))
    seq_spec = P('dp', 'cp')
    whole = P()

    def per_device(x_tok, prompt_lens, k_cache, v_cache, norm_gain, w_q, b_q, w_k, b_k, w_v, b_v, w_o):
        rows = x_tok.shape[0]
        batch, slots, kv_heads, dim = k_cache.shape
        n = batch // rows
        inv_freq = np.power(np.float32(ROPE_THETA), -(np.arange(dim // 2, dtype=np.float32) * 2.0 / dim)).astype(np.float32)
        freq = jnp.asarray(np.concatenate([inv_freq, inv_freq])[None, :])
        pack = (n, rows, slots * kv_heads, dim)
        att, k_all, v_all, wo = step(
            prompt_lens, freq, x_tok, norm_gain.reshape(-1, dim), b_q.reshape(-1, dim), b_k.reshape(-1, dim), b_v.reshape(-1, dim),
            w_q, w_k, w_v, w_o, k_cache.reshape(pack), v_cache.reshape(pack))
        y_out, k_out, v_out = finish(x_tok, att, wo, k_all, v_all)
        shape = (rows, n * slots, kv_heads, dim)
        return y_out, k_out.reshape(shape), v_out.reshape(shape)

    return jax.shard_map(per_device, mesh=mesh, in_specs=(batch_spec, P('dp'), seq_spec, seq_spec, whole, whole, whole, whole, whole, whole, whole, whole), out_specs=(batch_spec, batch_spec, batch_spec), check_vma=False)
```

```python
import functools
import numpy as np
import jax
import jax.numpy as jnp
from jax import lax
from jax.experimental import pallas as pl
from jax.experimental.pallas import tpu as pltpu
from jax.sharding import PartitionSpec as P

RMS_EPS = 1e-6
ROPE_THETA = 1000000.0
MESH = pl.DeviceIdType.MESH
F32 = jnp.float32
BF16 = jnp.bfloat16


def flip(me, d):
    out = 0
    for k in range(4):
        bit = 1 << k
        out = out + bit * lax.rem(lax.div(me, bit) + lax.div(d, bit), 2)
    return out


def step_kernel(n, lens_hbm, freq_hbm, x_ref, gain_ref, bq_ref, bk_ref, bv_ref, wq_ref, wk_ref, wv_ref, wo_ref, k_ref, v_ref,
                att_ref, ko_ref, vo_ref, wo,
                lens_ref, freq_ref, k_land, v_land, wq, wk, wv, xs, gain, bq, bk, bv,
                q_s, kn_s, vn_s, s_s, e_s, l_s, acc, send_sem, recv_sem, load_sem, turn):
    me = lax.axis_index("cp")
    rows, heads, dim = q_s.shape
    m = k_land.shape[2]
    width = heads * dim
    loads = {}
    for idx, (name, src, dst) in enumerate([
            ("lens", lens_hbm, lens_ref), ("freq", freq_hbm, freq_ref), ("x", x_ref, xs), ("gain", gain_ref, gain), ("bq", bq_ref, bq), ("bk", bk_ref, bk), ("bv", bv_ref, bv),
            ("wk", wk_ref, wk), ("wv", wv_ref, wv), ("wq", wq_ref, wq),
            ("k", k_ref.at[me], k_land.at[:, me]), ("v", v_ref.at[me], v_land.at[:, me]), ("wo", wo_ref, wo)]):
        loads[name] = pltpu.make_async_copy(src, dst, load_sem.at[idx])

    barrier = pltpu.get_barrier_semaphore()
    for d in range(1, n):
        pl.semaphore_signal(barrier, inc=1, device_id={"cp": lax.rem(me + d, n)}, device_id_type=MESH)
    for copy in loads.values():
        copy.start()
    pl.semaphore_wait(barrier, n - 1)

    pairs = ((k_ref, k_land), (v_ref, v_land))

    def send(a, to):
        return pltpu.make_async_remote_copy(
            src_ref=pairs[a][0].at[to], dst_ref=pairs[a][1].at[:, me], send_sem=send_sem.at[a, to], recv_sem=recv_sem.at[a, me],
            device_id={"cp": to}, device_id_type=MESH)

    def arrive(a, d):
        src = lax.rem(me + n - d, n)
        pltpu.make_async_remote_copy(
            src_ref=pairs[a][0].at[0], dst_ref=pairs[a][1].at[:, src], send_sem=send_sem.at[a, src], recv_sem=recv_sem.at[a, src],
            device_id={"cp": src}, device_id_type=MESH).wait_recv()
        return src

    half, layer = n // 2, n // 4
    z = lax.div(me, layer)
    high = lax.div(me, half)
    end = lax.rem(z + high, 2) == 0
    middle = lax.rem(z + high, 2) == 1
    second = lax.rem(me, 2) == 1
    beside = [z * layer + lax.rem(me + t, layer) for t in range(1, layer)]
    near = [(4 * high + 1 - z) * layer + lax.rem(me + t, layer) for t in range(layer)]
    far = [(1 - high) * half + lax.rem(me + t, half) for t in range(half)]

    def each(targets, act):
        for to in targets:
            for a in range(2):
                act(send(a, to))

    def start(copy):
        copy.start()

    def sent(copy):
        copy.wait_send()

    each(beside, start)

    @pl.when(middle)
    def _():
        each(far, start)

    each(near, start)

    loads["lens"].wait()
    pos = [lens_ref[me * rows + b] for b in range(rows)]

    for name in ("freq", "x", "gain", "bq", "bk", "bv", "wk", "wv", "wq"):
        loads[name].wait()
    wide = xs[...].astype(F32)
    inv = lax.rsqrt(jnp.mean(wide * wide, axis=-1, keepdims=True) + RMS_EPS)
    gains = jnp.concatenate([gain[h:h + 1, :].astype(F32) for h in range(heads)], axis=1)
    normed = (wide * inv * gains).astype(BF16)
    which = lax.broadcasted_iota(jnp.int32, (rows, dim), 0)
    lane = lax.broadcasted_iota(jnp.int32, (rows, dim), 1)
    posf = jnp.zeros((rows, dim), F32)
    for b in range(rows):
        posf = jnp.where(which == b, pos[b].astype(F32), posf)
    angle = posf * freq_ref[...]
    cos_t = jnp.cos(angle)
    sin_t = jnp.sin(angle)
    sin_t = jnp.where(lane < dim // 2, -sin_t, sin_t)

    def rotate(t):
        return (t * cos_t + pltpu.roll(t, dim // 2, 1) * sin_t).astype(BF16).astype(F32)

    for h in range(2):
        cols = pl.ds(h * dim, dim)
        kn_s[:, h, :] = rotate(jnp.dot(normed, wk[:, cols], preferred_element_type=F32) + bk[h:h + 1, :].astype(F32))
        vn_s[:, h, :] = (jnp.dot(normed, wv[:, cols], preferred_element_type=F32) + bv[h:h + 1, :].astype(F32)).astype(BF16).astype(F32)
    for h in range(heads):
        q_s[:, h, :] = rotate(jnp.dot(normed, wq[:, h * dim:(h + 1) * dim], preferred_element_type=F32) + bq[h:h + 1, :].astype(F32))

    @pl.when(middle)
    def _():
        each(far[:-1], sent)
        pl.semaphore_signal(turn, inc=1, device_id={"cp": 3 * layer * high + lax.rem(me, layer) - lax.rem(me, 2)}, device_id_type=MESH)

    @pl.when(end & (lax.rem(me, 2) == 0))
    def _():
        pl.semaphore_wait(turn, 2)
        each(far, start)
        each(far[:-1], sent)
        pl.semaphore_signal(turn, inc=1, device_id={"cp": me + 1}, device_id_type=MESH)

    @pl.when(end & second)
    def _():
        pl.semaphore_wait(turn, 1)
        each(far, start)

    row = lax.broadcasted_iota(jnp.int32, (m, dim), 0)
    even = lax.rem(row, 2) == 0

    def merge(land, new, out, b, i):
        at = 2 * pos[b] - i * m
        fresh = jnp.where(even, new[b, 0:1, :], new[b, 1:2, :])
        merged = jnp.where(row < at, land[b, i].astype(F32), jnp.where(row < at + 2, fresh, 0.0)).astype(BF16)
        out[b, i] = merged
        return merged

    def k_block(i):
        cols = pl.ds(pl.multiple_of(i * m, m), m)
        for b in range(rows):
            keys = merge(k_land, kn_s, ko_ref, b, i)
            s_s[b, :, cols] = lax.dot_general(q_s[b].astype(BF16), keys, (((1,), (1,)), ((), ())), preferred_element_type=F32) * (dim ** -0.5)

    def v_block(i):
        cols = pl.ds(pl.multiple_of(i * m, m), m)
        for b in range(rows):
            vals = merge(v_land, vn_s, vo_ref, b, i)
            acc[b] += jnp.dot(e_s[b, :, cols], vals, preferred_element_type=F32)

    def k_step(d, c):
        k_block(arrive(0, d))
        return c

    def v_step(d, c):
        v_block(arrive(1, d))
        return c

    loads["k"].wait()
    k_block(me)
    lax.fori_loop(1, n, k_step, 0)

    col = lax.broadcasted_iota(jnp.int32, (heads, n * m), 1)
    head = lax.broadcasted_iota(jnp.int32, (heads, n * m), 0)
    mine = lax.rem(col, 2) == lax.div(head, heads // 2)
    for b in range(rows):
        valid = mine & (col < 2 * pos[b] + 2)
        s = jnp.where(valid, s_s[b], -1e30)
        e = jnp.where(valid, jnp.exp(s - jnp.max(s, axis=-1, keepdims=True)), 0.0)
        l_s[b] = jnp.broadcast_to(jnp.sum(e, axis=-1, keepdims=True), (heads, dim))
        e_s[b] = e.astype(BF16)
    acc[...] = jnp.zeros_like(acc)

    loads["v"].wait()
    v_block(me)
    loads["wo"].wait()
    lax.fori_loop(1, n, v_step, 0)

    acc[...] = acc[...] / l_s[...]
    att_ref[...] = jnp.concatenate([acc[:, h, :] for h in range(heads)], axis=1).astype(BF16)

    each(beside + near + far[-1:], sent)

    @pl.when(end & second)
    def _():
        each(far[:-1], sent)


def step(lens, freq, x, gain, b_q, b_k, b_v, w_q, w_k, w_v, w_o, k, v):
    n, rows, m, dim = k.shape
    heads = w_q.shape[1] // dim
    kv = w_k.shape[1] // dim
    cache = pltpu.VMEM((rows, n, m, dim), BF16)
    hbm = pl.BlockSpec(memory_space=pltpu.HBM)
    vmem = pl.BlockSpec(memory_space=pltpu.VMEM)
    return pl.pallas_call(
        functools.partial(step_kernel, n),
        out_shape=[pltpu.VMEM(x.shape, BF16), cache, cache, pltpu.VMEM(w_o.shape, BF16)],
        in_specs=[hbm] * 13,
        out_specs=[vmem] * 4,
        scratch_shapes=[
            pltpu.SMEM(lens.shape, jnp.int32), pltpu.VMEM(freq.shape, F32),
            pltpu.VMEM((rows, n, m, dim), BF16), pltpu.VMEM((rows, n, m, dim), BF16),
            pltpu.VMEM(w_q.shape, BF16), pltpu.VMEM(w_k.shape, BF16), pltpu.VMEM(w_v.shape, BF16),
            pltpu.VMEM(x.shape, BF16), pltpu.VMEM(gain.shape, BF16), pltpu.VMEM(b_q.shape, BF16), pltpu.VMEM(b_k.shape, BF16), pltpu.VMEM(b_v.shape, BF16),
            pltpu.VMEM((rows, heads, dim), F32), pltpu.VMEM((rows, kv, dim), F32), pltpu.VMEM((rows, kv, dim), F32),
            pltpu.VMEM((rows, heads, n * m), F32), pltpu.VMEM((rows, heads, n * m), BF16), pltpu.VMEM((rows, heads, dim), F32),
            pltpu.VMEM((rows, heads, dim), F32),
            pltpu.SemaphoreType.DMA((2, n)), pltpu.SemaphoreType.DMA((2, n)), pltpu.SemaphoreType.DMA((13,)), pltpu.SemaphoreType.REGULAR],
        compiler_params=pltpu.CompilerParams(collective_id=0, has_side_effects=True, vmem_limit_bytes=47 * 1024 * 1024),
    )(lens, freq, x, gain, b_q, b_k, b_v, w_q, w_k, w_v, w_o, k, v)


def finish_kernel(x_ref, att_ref, wo_ref, k_ref, v_ref, y_ref, ko_ref, vo_ref, sem):
    copies = [pltpu.make_async_copy(k_ref, ko_ref, sem.at[0]), pltpu.make_async_copy(v_ref, vo_ref, sem.at[1])]
    for copy in copies:
        copy.start()
    tile = 256
    for t in range(wo_ref.shape[1] // tile):
        cols = slice(t * tile, (t + 1) * tile)
        y_ref[:, cols] = (x_ref[:, cols].astype(F32) + jnp.dot(att_ref[...], wo_ref[:, cols], preferred_element_type=F32)).astype(BF16)
    for copy in copies:
        copy.wait()


def finish(x, att, w_o, k, v):
    vmem = pl.BlockSpec(memory_space=pltpu.VMEM)
    hbm = pl.BlockSpec(memory_space=pltpu.HBM)
    cache = jax.ShapeDtypeStruct(k.shape, BF16)
    return pl.pallas_call(
        finish_kernel,
        out_shape=[jax.ShapeDtypeStruct(x.shape, BF16), cache, cache],
        in_specs=[vmem] * 5,
        out_specs=[vmem, hbm, hbm],
        scratch_shapes=[pltpu.SemaphoreType.DMA((2,))],
        compiler_params=pltpu.CompilerParams(vmem_limit_bytes=4 * 1024 * 1024),
    )(x, att, w_o, k, v)


def solution(mesh):
    batch_spec = P(('dp', 'cp'))
    seq_spec = P('dp', 'cp')
    whole = P()

    def per_device(x_tok, prompt_lens, k_cache, v_cache, norm_gain, w_q, b_q, w_k, b_k, w_v, b_v, w_o):
        rows = x_tok.shape[0]
        batch, slots, kv_heads, dim = k_cache.shape
        n = batch // rows
        inv_freq = np.power(np.float32(ROPE_THETA), -(np.arange(dim // 2, dtype=np.float32) * 2.0 / dim)).astype(np.float32)
        freq = jnp.asarray(np.concatenate([inv_freq, inv_freq])[None, :])
        pack = (n, rows, slots * kv_heads, dim)
        att, k_all, v_all, wo = step(
            prompt_lens, freq, x_tok, norm_gain.reshape(-1, dim), b_q.reshape(-1, dim), b_k.reshape(-1, dim), b_v.reshape(-1, dim),
            w_q, w_k, w_v, w_o, k_cache.reshape(pack), v_cache.reshape(pack))
        y_out, k_out, v_out = finish(x_tok, att, wo, k_all, v_all)
        shape = (rows, n * slots, kv_heads, dim)
        return y_out, k_out.reshape(shape), v_out.reshape(shape)

    return jax.shard_map(per_device, mesh=mesh, in_specs=(batch_spec, P('dp'), seq_spec, seq_spec, whole, whole, whole, whole, whole, whole, whole, whole), out_specs=(batch_spec, batch_spec, batch_spec), check_vma=False)
```

```python
import functools
import numpy as np
import jax
import jax.numpy as jnp
from jax import lax
from jax.experimental import pallas as pl
from jax.experimental.pallas import tpu as pltpu
from jax.sharding import PartitionSpec as P

RMS_EPS = 1e-6
ROPE_THETA = 1000000.0
MESH = pl.DeviceIdType.MESH
F32 = jnp.float32
BF16 = jnp.bfloat16


def flip(me, d):
    out = 0
    for k in range(4):
        bit = 1 << k
        out = out + bit * lax.rem(lax.div(me, bit) + lax.div(d, bit), 2)
    return out


def step_kernel(n, lens_hbm, freq_hbm, x_ref, gain_ref, bq_ref, bk_ref, bv_ref, wq_ref, wk_ref, wv_ref, wo_ref, k_ref, v_ref,
                att_ref, ko_ref, vo_ref, wo,
                lens_ref, freq_ref, k_land, v_land, wq, wk, wv, xs, gain, bq, bk, bv,
                q_s, kn_s, vn_s, s_s, e_s, l_s, acc, send_sem, recv_sem, load_sem, turn):
    me = lax.axis_index("cp")
    rows, heads, dim = q_s.shape
    m = k_land.shape[2]
    width = heads * dim
    loads = {}
    for idx, (name, src, dst) in enumerate([
            ("lens", lens_hbm, lens_ref), ("freq", freq_hbm, freq_ref), ("x", x_ref, xs), ("gain", gain_ref, gain), ("bq", bq_ref, bq), ("bk", bk_ref, bk), ("bv", bv_ref, bv),
            ("wk", wk_ref, wk), ("wv", wv_ref, wv), ("wq", wq_ref, wq),
            ("k", k_ref.at[me], k_land.at[:, me]), ("v", v_ref.at[me], v_land.at[:, me]), ("wo", wo_ref, wo)]):
        loads[name] = pltpu.make_async_copy(src, dst, load_sem.at[idx])

    barrier = pltpu.get_barrier_semaphore()
    for d in range(1, n):
        pl.semaphore_signal(barrier, inc=1, device_id={"cp": lax.rem(me + d, n)}, device_id_type=MESH)
    for copy in loads.values():
        copy.start()
    pl.semaphore_wait(barrier, n - 1)

    pairs = ((k_ref, k_land), (v_ref, v_land))

    def send(a, to):
        return pltpu.make_async_remote_copy(
            src_ref=pairs[a][0].at[to], dst_ref=pairs[a][1].at[:, me], send_sem=send_sem.at[a, to], recv_sem=recv_sem.at[a, me],
            device_id={"cp": to}, device_id_type=MESH)

    def arrive(a, d):
        src = lax.rem(me + n - d, n)
        pltpu.make_async_remote_copy(
            src_ref=pairs[a][0].at[0], dst_ref=pairs[a][1].at[:, src], send_sem=send_sem.at[a, src], recv_sem=recv_sem.at[a, src],
            device_id={"cp": src}, device_id_type=MESH).wait_recv()
        return src

    half, layer = n // 2, n // 4
    z = lax.div(me, layer)
    high = lax.div(me, half)
    end = lax.rem(z + high, 2) == 0
    middle = lax.rem(z + high, 2) == 1
    second = lax.rem(me, 2) == 1
    beside = [z * layer + lax.rem(me + t, layer) for t in range(1, layer)]
    near = [(4 * high + 1 - z) * layer + t for t in range(layer)]
    far = [(1 - high) * half + t for t in range(half)]

    def each(targets, act):
        for to in targets:
            for a in range(2):
                act(send(a, to))

    def start(copy):
        copy.start()

    def sent(copy):
        copy.wait_send()

    each(beside, start)

    @pl.when(middle)
    def _():
        each(far, start)

    each(near, start)

    loads["lens"].wait()
    pos = [lens_ref[me * rows + b] for b in range(rows)]

    for name in ("freq", "x", "gain", "bq", "bk", "bv", "wk", "wv", "wq"):
        loads[name].wait()
    wide = xs[...].astype(F32)
    inv = lax.rsqrt(jnp.mean(wide * wide, axis=-1, keepdims=True) + RMS_EPS)
    gains = jnp.concatenate([gain[h:h + 1, :].astype(F32) for h in range(heads)], axis=1)
    normed = (wide * inv * gains).astype(BF16)
    which = lax.broadcasted_iota(jnp.int32, (rows, dim), 0)
    lane = lax.broadcasted_iota(jnp.int32, (rows, dim), 1)
    posf = jnp.zeros((rows, dim), F32)
    for b in range(rows):
        posf = jnp.where(which == b, pos[b].astype(F32), posf)
    angle = posf * freq_ref[...]
    cos_t = jnp.cos(angle)
    sin_t = jnp.sin(angle)
    sin_t = jnp.where(lane < dim // 2, -sin_t, sin_t)

    def rotate(t):
        return (t * cos_t + pltpu.roll(t, dim // 2, 1) * sin_t).astype(BF16).astype(F32)

    for h in range(2):
        cols = pl.ds(h * dim, dim)
        kn_s[:, h, :] = rotate(jnp.dot(normed, wk[:, cols], preferred_element_type=F32) + bk[h:h + 1, :].astype(F32))
        vn_s[:, h, :] = (jnp.dot(normed, wv[:, cols], preferred_element_type=F32) + bv[h:h + 1, :].astype(F32)).astype(BF16).astype(F32)
    for h in range(heads):
        q_s[:, h, :] = rotate(jnp.dot(normed, wq[:, h * dim:(h + 1) * dim], preferred_element_type=F32) + bq[h:h + 1, :].astype(F32))

    @pl.when(middle)
    def _():
        each(far[:-1], sent)
        pl.semaphore_signal(turn, inc=1, device_id={"cp": 3 * layer * high + lax.rem(me, layer) - lax.rem(me, 2)}, device_id_type=MESH)

    @pl.when(end & (lax.rem(me, 2) == 0))
    def _():
        pl.semaphore_wait(turn, 2)
        each(far, start)
        each(far[:-1], sent)
        pl.semaphore_signal(turn, inc=1, device_id={"cp": me + 1}, device_id_type=MESH)

    @pl.when(end & second)
    def _():
        pl.semaphore_wait(turn, 1)
        each(far, start)

    row = lax.broadcasted_iota(jnp.int32, (m, dim), 0)
    even = lax.rem(row, 2) == 0

    def merge(land, new, out, b, i):
        at = 2 * pos[b] - i * m
        fresh = jnp.where(even, new[b, 0:1, :], new[b, 1:2, :])
        merged = jnp.where(row < at, land[b, i].astype(F32), jnp.where(row < at + 2, fresh, 0.0)).astype(BF16)
        out[b, i] = merged
        return merged

    def k_block(i):
        cols = pl.ds(pl.multiple_of(i * m, m), m)
        for b in range(rows):
            keys = merge(k_land, kn_s, ko_ref, b, i)
            s_s[b, :, cols] = lax.dot_general(q_s[b].astype(BF16), keys, (((1,), (1,)), ((), ())), preferred_element_type=F32) * (dim ** -0.5)

    def v_block(i):
        cols = pl.ds(pl.multiple_of(i * m, m), m)
        for b in range(rows):
            vals = merge(v_land, vn_s, vo_ref, b, i)
            acc[b] += jnp.dot(e_s[b, :, cols], vals, preferred_element_type=F32)

    def k_step(d, c):
        k_block(arrive(0, d))
        return c

    def v_step(d, c):
        v_block(arrive(1, d))
        return c

    loads["k"].wait()
    k_block(me)
    lax.fori_loop(1, n, k_step, 0)

    col = lax.broadcasted_iota(jnp.int32, (heads, n * m), 1)
    head = lax.broadcasted_iota(jnp.int32, (heads, n * m), 0)
    mine = lax.rem(col, 2) == lax.div(head, heads // 2)
    for b in range(rows):
        valid = mine & (col < 2 * pos[b] + 2)
        s = jnp.where(valid, s_s[b], -1e30)
        e = jnp.where(valid, jnp.exp(s - jnp.max(s, axis=-1, keepdims=True)), 0.0)
        l_s[b] = jnp.broadcast_to(jnp.sum(e, axis=-1, keepdims=True), (heads, dim))
        e_s[b] = e.astype(BF16)
    acc[...] = jnp.zeros_like(acc)

    loads["v"].wait()
    v_block(me)
    loads["wo"].wait()
    lax.fori_loop(1, n, v_step, 0)

    acc[...] = acc[...] / l_s[...]
    att_ref[...] = jnp.concatenate([acc[:, h, :] for h in range(heads)], axis=1).astype(BF16)

    each(beside + near + far[-1:], sent)

    @pl.when(end & second)
    def _():
        each(far[:-1], sent)


def step(lens, freq, x, gain, b_q, b_k, b_v, w_q, w_k, w_v, w_o, k, v):
    n, rows, m, dim = k.shape
    heads = w_q.shape[1] // dim
    kv = w_k.shape[1] // dim
    cache = pltpu.VMEM((rows, n, m, dim), BF16)
    hbm = pl.BlockSpec(memory_space=pltpu.HBM)
    vmem = pl.BlockSpec(memory_space=pltpu.VMEM)
    return pl.pallas_call(
        functools.partial(step_kernel, n),
        out_shape=[pltpu.VMEM(x.shape, BF16), cache, cache, pltpu.VMEM(w_o.shape, BF16)],
        in_specs=[hbm] * 13,
        out_specs=[vmem] * 4,
        scratch_shapes=[
            pltpu.SMEM(lens.shape, jnp.int32), pltpu.VMEM(freq.shape, F32),
            pltpu.VMEM((rows, n, m, dim), BF16), pltpu.VMEM((rows, n, m, dim), BF16),
            pltpu.VMEM(w_q.shape, BF16), pltpu.VMEM(w_k.shape, BF16), pltpu.VMEM(w_v.shape, BF16),
            pltpu.VMEM(x.shape, BF16), pltpu.VMEM(gain.shape, BF16), pltpu.VMEM(b_q.shape, BF16), pltpu.VMEM(b_k.shape, BF16), pltpu.VMEM(b_v.shape, BF16),
            pltpu.VMEM((rows, heads, dim), F32), pltpu.VMEM((rows, kv, dim), F32), pltpu.VMEM((rows, kv, dim), F32),
            pltpu.VMEM((rows, heads, n * m), F32), pltpu.VMEM((rows, heads, n * m), BF16), pltpu.VMEM((rows, heads, dim), F32),
            pltpu.VMEM((rows, heads, dim), F32),
            pltpu.SemaphoreType.DMA((2, n)), pltpu.SemaphoreType.DMA((2, n)), pltpu.SemaphoreType.DMA((13,)), pltpu.SemaphoreType.REGULAR],
        compiler_params=pltpu.CompilerParams(collective_id=0, has_side_effects=True, vmem_limit_bytes=47 * 1024 * 1024),
    )(lens, freq, x, gain, b_q, b_k, b_v, w_q, w_k, w_v, w_o, k, v)


def finish_kernel(x_ref, att_ref, wo_ref, k_ref, v_ref, y_ref, ko_ref, vo_ref, sem):
    copies = [pltpu.make_async_copy(k_ref, ko_ref, sem.at[0]), pltpu.make_async_copy(v_ref, vo_ref, sem.at[1])]
    for copy in copies:
        copy.start()
    tile = 256
    for t in range(wo_ref.shape[1] // tile):
        cols = slice(t * tile, (t + 1) * tile)
        y_ref[:, cols] = (x_ref[:, cols].astype(F32) + jnp.dot(att_ref[...], wo_ref[:, cols], preferred_element_type=F32)).astype(BF16)
    for copy in copies:
        copy.wait()


def finish(x, att, w_o, k, v):
    vmem = pl.BlockSpec(memory_space=pltpu.VMEM)
    hbm = pl.BlockSpec(memory_space=pltpu.HBM)
    cache = jax.ShapeDtypeStruct(k.shape, BF16)
    return pl.pallas_call(
        finish_kernel,
        out_shape=[jax.ShapeDtypeStruct(x.shape, BF16), cache, cache],
        in_specs=[vmem] * 5,
        out_specs=[vmem, hbm, hbm],
        scratch_shapes=[pltpu.SemaphoreType.DMA((2,))],
        compiler_params=pltpu.CompilerParams(vmem_limit_bytes=4 * 1024 * 1024),
    )(x, att, w_o, k, v)


def solution(mesh):
    batch_spec = P(('dp', 'cp'))
    seq_spec = P('dp', 'cp')
    whole = P()

    def per_device(x_tok, prompt_lens, k_cache, v_cache, norm_gain, w_q, b_q, w_k, b_k, w_v, b_v, w_o):
        rows = x_tok.shape[0]
        batch, slots, kv_heads, dim = k_cache.shape
        n = batch // rows
        inv_freq = np.power(np.float32(ROPE_THETA), -(np.arange(dim // 2, dtype=np.float32) * 2.0 / dim)).astype(np.float32)
        freq = jnp.asarray(np.concatenate([inv_freq, inv_freq])[None, :])
        pack = (n, rows, slots * kv_heads, dim)
        att, k_all, v_all, wo = step(
            prompt_lens, freq, x_tok, norm_gain.reshape(-1, dim), b_q.reshape(-1, dim), b_k.reshape(-1, dim), b_v.reshape(-1, dim),
            w_q, w_k, w_v, w_o, k_cache.reshape(pack), v_cache.reshape(pack))
        y_out, k_out, v_out = finish(x_tok, att, wo, k_all, v_all)
        shape = (rows, n * slots, kv_heads, dim)
        return y_out, k_out.reshape(shape), v_out.reshape(shape)

    return jax.shard_map(per_device, mesh=mesh, in_specs=(batch_spec, P('dp'), seq_spec, seq_spec, whole, whole, whole, whole, whole, whole, whole, whole), out_specs=(batch_spec, batch_spec, batch_spec), check_vma=False)
```

```python
import functools
import numpy as np
import jax
import jax.numpy as jnp
from jax import lax
from jax.experimental import pallas as pl
from jax.experimental.pallas import tpu as pltpu
from jax.sharding import PartitionSpec as P

RMS_EPS = 1e-6
ROPE_THETA = 1000000.0
MESH = pl.DeviceIdType.MESH
F32 = jnp.float32
BF16 = jnp.bfloat16


def flip(me, d):
    out = 0
    for k in range(4):
        bit = 1 << k
        out = out + bit * lax.rem(lax.div(me, bit) + lax.div(d, bit), 2)
    return out


def step_kernel(n, lens_hbm, freq_hbm, x_ref, gain_ref, bq_ref, bk_ref, bv_ref, wq_ref, wk_ref, wv_ref, wo_ref, k_ref, v_ref,
                att_ref, ko_ref, vo_ref, wo,
                lens_ref, freq_ref, k_land, v_land, wq, wk, wv, xs, gain, bq, bk, bv,
                q_s, kn_s, vn_s, s_s, e_s, l_s, acc, send_sem, recv_sem, load_sem):
    me = lax.axis_index("cp")
    rows, heads, dim = q_s.shape
    m = k_land.shape[2]
    width = heads * dim
    loads = {}
    for idx, (name, src, dst) in enumerate([
            ("lens", lens_hbm, lens_ref), ("freq", freq_hbm, freq_ref), ("x", x_ref, xs), ("gain", gain_ref, gain), ("bq", bq_ref, bq), ("bk", bk_ref, bk), ("bv", bv_ref, bv),
            ("wk", wk_ref, wk), ("wv", wv_ref, wv), ("wq", wq_ref, wq),
            ("k", k_ref.at[me], k_land.at[:, me]), ("v", v_ref.at[me], v_land.at[:, me]), ("wo", wo_ref, wo)]):
        loads[name] = pltpu.make_async_copy(src, dst, load_sem.at[idx])

    barrier = pltpu.get_barrier_semaphore()
    for d in range(1, n):
        pl.semaphore_signal(barrier, inc=1, device_id={"cp": lax.rem(me + d, n)}, device_id_type=MESH)
    for copy in loads.values():
        copy.start()
    pl.semaphore_wait(barrier, n - 1)

    pairs = ((k_ref, k_land), (v_ref, v_land))

    def send(a, to):
        return pltpu.make_async_remote_copy(
            src_ref=pairs[a][0].at[to], dst_ref=pairs[a][1].at[:, me], send_sem=send_sem.at[a, to], recv_sem=recv_sem.at[a, me],
            device_id={"cp": to}, device_id_type=MESH)

    def arrive(a, d):
        src = lax.rem(me + n - d, n)
        pltpu.make_async_remote_copy(
            src_ref=pairs[a][0].at[0], dst_ref=pairs[a][1].at[:, src], send_sem=send_sem.at[a, src], recv_sem=recv_sem.at[a, src],
            device_id={"cp": src}, device_id_type=MESH).wait_recv()
        return src

    half, layer = n // 2, n // 4
    z = lax.div(me, layer)
    high = lax.div(me, half)
    end = lax.rem(z + high, 2) == 0
    middle = lax.rem(z + high, 2) == 1
    beside = [z * layer + lax.rem(me + t, layer) for t in range(1, layer)]
    near = [(4 * high + 1 - z) * layer + t for t in range(layer)]
    far = [(1 - high) * half + t for t in range(half)]

    def each(targets, act):
        for to in targets:
            for a in range(2):
                act(send(a, to))

    def start(copy):
        copy.start()

    def sent(copy):
        copy.wait_send()

    @pl.when(middle)
    def _():
        each(far[:6] + beside + near + far[6:], start)

    @pl.when(end)
    def _():
        each(beside + near + far, start)

    loads["lens"].wait()
    pos = [lens_ref[me * rows + b] for b in range(rows)]

    for name in ("freq", "x", "gain", "bq", "bk", "bv", "wk", "wv", "wq"):
        loads[name].wait()
    wide = xs[...].astype(F32)
    inv = lax.rsqrt(jnp.mean(wide * wide, axis=-1, keepdims=True) + RMS_EPS)
    gains = jnp.concatenate([gain[h:h + 1, :].astype(F32) for h in range(heads)], axis=1)
    normed = (wide * inv * gains).astype(BF16)
    which = lax.broadcasted_iota(jnp.int32, (rows, dim), 0)
    lane = lax.broadcasted_iota(jnp.int32, (rows, dim), 1)
    posf = jnp.zeros((rows, dim), F32)
    for b in range(rows):
        posf = jnp.where(which == b, pos[b].astype(F32), posf)
    angle = posf * freq_ref[...]
    cos_t = jnp.cos(angle)
    sin_t = jnp.sin(angle)
    sin_t = jnp.where(lane < dim // 2, -sin_t, sin_t)

    def rotate(t):
        return (t * cos_t + pltpu.roll(t, dim // 2, 1) * sin_t).astype(BF16).astype(F32)

    for h in range(2):
        cols = pl.ds(h * dim, dim)
        kn_s[:, h, :] = rotate(jnp.dot(normed, wk[:, cols], preferred_element_type=F32) + bk[h:h + 1, :].astype(F32))
        vn_s[:, h, :] = (jnp.dot(normed, wv[:, cols], preferred_element_type=F32) + bv[h:h + 1, :].astype(F32)).astype(BF16).astype(F32)
    for h in range(heads):
        q_s[:, h, :] = rotate(jnp.dot(normed, wq[:, h * dim:(h + 1) * dim], preferred_element_type=F32) + bq[h:h + 1, :].astype(F32))

    row = lax.broadcasted_iota(jnp.int32, (m, dim), 0)
    even = lax.rem(row, 2) == 0

    def merge(land, new, out, b, i):
        at = 2 * pos[b] - i * m
        fresh = jnp.where(even, new[b, 0:1, :], new[b, 1:2, :])
        merged = jnp.where(row < at, land[b, i].astype(F32), jnp.where(row < at + 2, fresh, 0.0)).astype(BF16)
        out[b, i] = merged
        return merged

    def k_block(i):
        cols = pl.ds(pl.multiple_of(i * m, m), m)
        for b in range(rows):
            keys = merge(k_land, kn_s, ko_ref, b, i)
            s_s[b, :, cols] = lax.dot_general(q_s[b].astype(BF16), keys, (((1,), (1,)), ((), ())), preferred_element_type=F32) * (dim ** -0.5)

    def v_block(i):
        cols = pl.ds(pl.multiple_of(i * m, m), m)
        for b in range(rows):
            vals = merge(v_land, vn_s, vo_ref, b, i)
            acc[b] += jnp.dot(e_s[b, :, cols], vals, preferred_element_type=F32)

    def k_step(d, c):
        k_block(arrive(0, d))
        return c

    def v_step(d, c):
        v_block(arrive(1, d))
        return c

    loads["k"].wait()
    k_block(me)
    lax.fori_loop(1, n, k_step, 0)

    col = lax.broadcasted_iota(jnp.int32, (heads, n * m), 1)
    head = lax.broadcasted_iota(jnp.int32, (heads, n * m), 0)
    mine = lax.rem(col, 2) == lax.div(head, heads // 2)
    for b in range(rows):
        valid = mine & (col < 2 * pos[b] + 2)
        s = jnp.where(valid, s_s[b], -1e30)
        e = jnp.where(valid, jnp.exp(s - jnp.max(s, axis=-1, keepdims=True)), 0.0)
        l_s[b] = jnp.broadcast_to(jnp.sum(e, axis=-1, keepdims=True), (heads, dim))
        e_s[b] = e.astype(BF16)
    acc[...] = jnp.zeros_like(acc)

    loads["v"].wait()
    v_block(me)
    loads["wo"].wait()
    lax.fori_loop(1, n, v_step, 0)

    acc[...] = acc[...] / l_s[...]
    att_ref[...] = jnp.concatenate([acc[:, h, :] for h in range(heads)], axis=1).astype(BF16)

    each(beside + near + far, sent)


def step(lens, freq, x, gain, b_q, b_k, b_v, w_q, w_k, w_v, w_o, k, v):
    n, rows, m, dim = k.shape
    heads = w_q.shape[1] // dim
    kv = w_k.shape[1] // dim
    cache = pltpu.VMEM((rows, n, m, dim), BF16)
    hbm = pl.BlockSpec(memory_space=pltpu.HBM)
    vmem = pl.BlockSpec(memory_space=pltpu.VMEM)
    return pl.pallas_call(
        functools.partial(step_kernel, n),
        out_shape=[pltpu.VMEM(x.shape, BF16), cache, cache, pltpu.VMEM(w_o.shape, BF16)],
        in_specs=[hbm] * 13,
        out_specs=[vmem] * 4,
        scratch_shapes=[
            pltpu.SMEM(lens.shape, jnp.int32), pltpu.VMEM(freq.shape, F32),
            pltpu.VMEM((rows, n, m, dim), BF16), pltpu.VMEM((rows, n, m, dim), BF16),
            pltpu.VMEM(w_q.shape, BF16), pltpu.VMEM(w_k.shape, BF16), pltpu.VMEM(w_v.shape, BF16),
            pltpu.VMEM(x.shape, BF16), pltpu.VMEM(gain.shape, BF16), pltpu.VMEM(b_q.shape, BF16), pltpu.VMEM(b_k.shape, BF16), pltpu.VMEM(b_v.shape, BF16),
            pltpu.VMEM((rows, heads, dim), F32), pltpu.VMEM((rows, kv, dim), F32), pltpu.VMEM((rows, kv, dim), F32),
            pltpu.VMEM((rows, heads, n * m), F32), pltpu.VMEM((rows, heads, n * m), BF16), pltpu.VMEM((rows, heads, dim), F32),
            pltpu.VMEM((rows, heads, dim), F32),
            pltpu.SemaphoreType.DMA((2, n)), pltpu.SemaphoreType.DMA((2, n)), pltpu.SemaphoreType.DMA((13,))],
        compiler_params=pltpu.CompilerParams(collective_id=0, has_side_effects=True, vmem_limit_bytes=47 * 1024 * 1024),
    )(lens, freq, x, gain, b_q, b_k, b_v, w_q, w_k, w_v, w_o, k, v)


def finish_kernel(x_ref, att_ref, wo_ref, k_ref, v_ref, y_ref, ko_ref, vo_ref, sem):
    copies = [pltpu.make_async_copy(k_ref, ko_ref, sem.at[0]), pltpu.make_async_copy(v_ref, vo_ref, sem.at[1])]
    for copy in copies:
        copy.start()
    tile = 256
    for t in range(wo_ref.shape[1] // tile):
        cols = slice(t * tile, (t + 1) * tile)
        y_ref[:, cols] = (x_ref[:, cols].astype(F32) + jnp.dot(att_ref[...], wo_ref[:, cols], preferred_element_type=F32)).astype(BF16)
    for copy in copies:
        copy.wait()


def finish(x, att, w_o, k, v):
    vmem = pl.BlockSpec(memory_space=pltpu.VMEM)
    hbm = pl.BlockSpec(memory_space=pltpu.HBM)
    cache = jax.ShapeDtypeStruct(k.shape, BF16)
    return pl.pallas_call(
        finish_kernel,
        out_shape=[jax.ShapeDtypeStruct(x.shape, BF16), cache, cache],
        in_specs=[vmem] * 5,
        out_specs=[vmem, hbm, hbm],
        scratch_shapes=[pltpu.SemaphoreType.DMA((2,))],
        compiler_params=pltpu.CompilerParams(vmem_limit_bytes=4 * 1024 * 1024),
    )(x, att, w_o, k, v)


def solution(mesh):
    batch_spec = P(('dp', 'cp'))
    seq_spec = P('dp', 'cp')
    whole = P()

    def per_device(x_tok, prompt_lens, k_cache, v_cache, norm_gain, w_q, b_q, w_k, b_k, w_v, b_v, w_o):
        rows = x_tok.shape[0]
        batch, slots, kv_heads, dim = k_cache.shape
        n = batch // rows
        inv_freq = np.power(np.float32(ROPE_THETA), -(np.arange(dim // 2, dtype=np.float32) * 2.0 / dim)).astype(np.float32)
        freq = jnp.asarray(np.concatenate([inv_freq, inv_freq])[None, :])
        pack = (n, rows, slots * kv_heads, dim)
        att, k_all, v_all, wo = step(
            prompt_lens, freq, x_tok, norm_gain.reshape(-1, dim), b_q.reshape(-1, dim), b_k.reshape(-1, dim), b_v.reshape(-1, dim),
            w_q, w_k, w_v, w_o, k_cache.reshape(pack), v_cache.reshape(pack))
        y_out, k_out, v_out = finish(x_tok, att, wo, k_all, v_all)
        shape = (rows, n * slots, kv_heads, dim)
        return y_out, k_out.reshape(shape), v_out.reshape(shape)

    return jax.shard_map(per_device, mesh=mesh, in_specs=(batch_spec, P('dp'), seq_spec, seq_spec, whole, whole, whole, whole, whole, whole, whole, whole), out_specs=(batch_spec, batch_spec, batch_spec), check_vma=False)
```

```python
import functools
import numpy as np
import jax
import jax.numpy as jnp
from jax import lax
from jax.experimental import pallas as pl
from jax.experimental.pallas import tpu as pltpu
from jax.sharding import PartitionSpec as P

RMS_EPS = 1e-6
ROPE_THETA = 1000000.0
MESH = pl.DeviceIdType.MESH
F32 = jnp.float32
BF16 = jnp.bfloat16


def flip(me, d):
    out = 0
    for k in range(4):
        bit = 1 << k
        out = out + bit * lax.rem(lax.div(me, bit) + lax.div(d, bit), 2)
    return out


def step_kernel(n, lens_hbm, freq_hbm, x_ref, gain_ref, bq_ref, bk_ref, bv_ref, wq_ref, wk_ref, wv_ref, wo_ref, k_ref, v_ref,
                att_ref, ko_ref, vo_ref, wo,
                lens_ref, freq_ref, k_land, v_land, wq, wk, wv, xs, gain, bq, bk, bv,
                q_s, kn_s, vn_s, s_s, e_s, l_s, acc, send_sem, recv_sem, load_sem, turn):
    me = lax.axis_index("cp")
    rows, heads, dim = q_s.shape
    m = k_land.shape[2]
    width = heads * dim
    loads = {}
    for idx, (name, src, dst) in enumerate([
            ("lens", lens_hbm, lens_ref), ("freq", freq_hbm, freq_ref), ("x", x_ref, xs), ("gain", gain_ref, gain), ("bq", bq_ref, bq), ("bk", bk_ref, bk), ("bv", bv_ref, bv),
            ("wk", wk_ref, wk), ("wv", wv_ref, wv), ("wq", wq_ref, wq),
            ("k", k_ref.at[me], k_land.at[:, me]), ("v", v_ref.at[me], v_land.at[:, me]), ("wo", wo_ref, wo)]):
        loads[name] = pltpu.make_async_copy(src, dst, load_sem.at[idx])

    barrier = pltpu.get_barrier_semaphore()
    for d in range(1, n):
        pl.semaphore_signal(barrier, inc=1, device_id={"cp": lax.rem(me + d, n)}, device_id_type=MESH)
    for copy in loads.values():
        copy.start()
    pl.semaphore_wait(barrier, n - 1)

    pairs = ((k_ref, k_land), (v_ref, v_land))

    def send(a, to):
        return pltpu.make_async_remote_copy(
            src_ref=pairs[a][0].at[to], dst_ref=pairs[a][1].at[:, me], send_sem=send_sem.at[a, to], recv_sem=recv_sem.at[a, me],
            device_id={"cp": to}, device_id_type=MESH)

    def arrive(a, d):
        src = lax.rem(me + n - d, n)
        pltpu.make_async_remote_copy(
            src_ref=pairs[a][0].at[0], dst_ref=pairs[a][1].at[:, src], send_sem=send_sem.at[a, src], recv_sem=recv_sem.at[a, src],
            device_id={"cp": src}, device_id_type=MESH).wait_recv()
        return src

    half, layer = n // 2, n // 4
    z = lax.div(me, layer)
    high = lax.div(me, half)
    end = lax.rem(z + high, 2) == 0
    middle = lax.rem(z + high, 2) == 1
    second = lax.rem(me, 2) == 1
    beside = [z * layer + lax.rem(me + t, layer) for t in range(1, layer)]
    near = [(4 * high + 1 - z) * layer + lax.rem(me + t, layer) for t in range(layer)]
    far = [(2 - high) * layer + lax.rem(me + t, layer) for t in range(layer)]
    far += [3 * (1 - high) * layer + lax.rem(me + t, layer) for t in range(layer)]

    def each(targets, act):
        for to in targets:
            for a in range(2):
                act(send(a, to))

    def start(copy):
        copy.start()

    def sent(copy):
        copy.wait_send()

    @pl.when(middle)
    def _():
        each(far, start)

    each(near + beside, start)

    loads["lens"].wait()
    pos = [lens_ref[me * rows + b] for b in range(rows)]

    for name in ("freq", "x", "gain", "bq", "bk", "bv", "wk", "wv", "wq"):
        loads[name].wait()
    wide = xs[...].astype(F32)
    inv = lax.rsqrt(jnp.mean(wide * wide, axis=-1, keepdims=True) + RMS_EPS)
    gains = jnp.concatenate([gain[h:h + 1, :].astype(F32) for h in range(heads)], axis=1)
    normed = (wide * inv * gains).astype(BF16)
    which = lax.broadcasted_iota(jnp.int32, (rows, dim), 0)
    lane = lax.broadcasted_iota(jnp.int32, (rows, dim), 1)
    posf = jnp.zeros((rows, dim), F32)
    for b in range(rows):
        posf = jnp.where(which == b, pos[b].astype(F32), posf)
    angle = posf * freq_ref[...]
    cos_t = jnp.cos(angle)
    sin_t = jnp.sin(angle)
    sin_t = jnp.where(lane < dim // 2, -sin_t, sin_t)

    def rotate(t):
        return (t * cos_t + pltpu.roll(t, dim // 2, 1) * sin_t).astype(BF16).astype(F32)

    for h in range(2):
        cols = pl.ds(h * dim, dim)
        kn_s[:, h, :] = rotate(jnp.dot(normed, wk[:, cols], preferred_element_type=F32) + bk[h:h + 1, :].astype(F32))
        vn_s[:, h, :] = (jnp.dot(normed, wv[:, cols], preferred_element_type=F32) + bv[h:h + 1, :].astype(F32)).astype(BF16).astype(F32)
    for h in range(heads):
        q_s[:, h, :] = rotate(jnp.dot(normed, wq[:, h * dim:(h + 1) * dim], preferred_element_type=F32) + bq[h:h + 1, :].astype(F32))

    @pl.when(middle)
    def _():
        each(far[:-1], sent)
        pl.semaphore_signal(turn, inc=1, device_id={"cp": 3 * layer * high + lax.rem(me, layer) - lax.rem(me, 2)}, device_id_type=MESH)

    @pl.when(end & (lax.rem(me, 2) == 0))
    def _():
        pl.semaphore_wait(turn, 2)
        each(far, start)
        each(far[:-1], sent)
        pl.semaphore_signal(turn, inc=1, device_id={"cp": me + 1}, device_id_type=MESH)

    @pl.when(end & second)
    def _():
        pl.semaphore_wait(turn, 1)
        each(far, start)

    row = lax.broadcasted_iota(jnp.int32, (m, dim), 0)
    even = lax.rem(row, 2) == 0

    def merge(land, new, out, b, i):
        at = 2 * pos[b] - i * m
        fresh = jnp.where(even, new[b, 0:1, :], new[b, 1:2, :])
        merged = jnp.where(row < at, land[b, i].astype(F32), jnp.where(row < at + 2, fresh, 0.0)).astype(BF16)
        out[b, i] = merged
        return merged

    def k_block(i):
        cols = pl.ds(pl.multiple_of(i * m, m), m)
        for b in range(rows):
            keys = merge(k_land, kn_s, ko_ref, b, i)
            s_s[b, :, cols] = lax.dot_general(q_s[b].astype(BF16), keys, (((1,), (1,)), ((), ())), preferred_element_type=F32) * (dim ** -0.5)

    def v_block(i):
        cols = pl.ds(pl.multiple_of(i * m, m), m)
        for b in range(rows):
            vals = merge(v_land, vn_s, vo_ref, b, i)
            acc[b] += jnp.dot(e_s[b, :, cols], vals, preferred_element_type=F32)

    def k_step(d, c):
        k_block(arrive(0, d))
        return c

    def v_step(d, c):
        v_block(arrive(1, d))
        return c

    loads["k"].wait()
    k_block(me)
    lax.fori_loop(1, n, k_step, 0)

    col = lax.broadcasted_iota(jnp.int32, (heads, n * m), 1)
    head = lax.broadcasted_iota(jnp.int32, (heads, n * m), 0)
    mine = lax.rem(col, 2) == lax.div(head, heads // 2)
    for b in range(rows):
        valid = mine & (col < 2 * pos[b] + 2)
        s = jnp.where(valid, s_s[b], -1e30)
        e = jnp.where(valid, jnp.exp(s - jnp.max(s, axis=-1, keepdims=True)), 0.0)
        l_s[b] = jnp.broadcast_to(jnp.sum(e, axis=-1, keepdims=True), (heads, dim))
        e_s[b] = e.astype(BF16)
    acc[...] = jnp.zeros_like(acc)

    loads["v"].wait()
    v_block(me)
    loads["wo"].wait()
    lax.fori_loop(1, n, v_step, 0)

    acc[...] = acc[...] / l_s[...]
    att_ref[...] = jnp.concatenate([acc[:, h, :] for h in range(heads)], axis=1).astype(BF16)

    each(beside + near + far[-1:], sent)

    @pl.when(end & second)
    def _():
        each(far[:-1], sent)


def step(lens, freq, x, gain, b_q, b_k, b_v, w_q, w_k, w_v, w_o, k, v):
    n, rows, m, dim = k.shape
    heads = w_q.shape[1] // dim
    kv = w_k.shape[1] // dim
    cache = pltpu.VMEM((rows, n, m, dim), BF16)
    hbm = pl.BlockSpec(memory_space=pltpu.HBM)
    vmem = pl.BlockSpec(memory_space=pltpu.VMEM)
    return pl.pallas_call(
        functools.partial(step_kernel, n),
        out_shape=[pltpu.VMEM(x.shape, BF16), cache, cache, pltpu.VMEM(w_o.shape, BF16)],
        in_specs=[hbm] * 13,
        out_specs=[vmem] * 4,
        scratch_shapes=[
            pltpu.SMEM(lens.shape, jnp.int32), pltpu.VMEM(freq.shape, F32),
            pltpu.VMEM((rows, n, m, dim), BF16), pltpu.VMEM((rows, n, m, dim), BF16),
            pltpu.VMEM(w_q.shape, BF16), pltpu.VMEM(w_k.shape, BF16), pltpu.VMEM(w_v.shape, BF16),
            pltpu.VMEM(x.shape, BF16), pltpu.VMEM(gain.shape, BF16), pltpu.VMEM(b_q.shape, BF16), pltpu.VMEM(b_k.shape, BF16), pltpu.VMEM(b_v.shape, BF16),
            pltpu.VMEM((rows, heads, dim), F32), pltpu.VMEM((rows, kv, dim), F32), pltpu.VMEM((rows, kv, dim), F32),
            pltpu.VMEM((rows, heads, n * m), F32), pltpu.VMEM((rows, heads, n * m), BF16), pltpu.VMEM((rows, heads, dim), F32),
            pltpu.VMEM((rows, heads, dim), F32),
            pltpu.SemaphoreType.DMA((2, n)), pltpu.SemaphoreType.DMA((2, n)), pltpu.SemaphoreType.DMA((13,)), pltpu.SemaphoreType.REGULAR],
        compiler_params=pltpu.CompilerParams(collective_id=0, has_side_effects=True, vmem_limit_bytes=47 * 1024 * 1024),
    )(lens, freq, x, gain, b_q, b_k, b_v, w_q, w_k, w_v, w_o, k, v)


def finish_kernel(x_ref, att_ref, wo_ref, k_ref, v_ref, y_ref, ko_ref, vo_ref, sem):
    copies = [pltpu.make_async_copy(k_ref, ko_ref, sem.at[0]), pltpu.make_async_copy(v_ref, vo_ref, sem.at[1])]
    for copy in copies:
        copy.start()
    tile = 256
    for t in range(wo_ref.shape[1] // tile):
        cols = slice(t * tile, (t + 1) * tile)
        y_ref[:, cols] = (x_ref[:, cols].astype(F32) + jnp.dot(att_ref[...], wo_ref[:, cols], preferred_element_type=F32)).astype(BF16)
    for copy in copies:
        copy.wait()


def finish(x, att, w_o, k, v):
    vmem = pl.BlockSpec(memory_space=pltpu.VMEM)
    hbm = pl.BlockSpec(memory_space=pltpu.HBM)
    cache = jax.ShapeDtypeStruct(k.shape, BF16)
    return pl.pallas_call(
        finish_kernel,
        out_shape=[jax.ShapeDtypeStruct(x.shape, BF16), cache, cache],
        in_specs=[vmem] * 5,
        out_specs=[vmem, hbm, hbm],
        scratch_shapes=[pltpu.SemaphoreType.DMA((2,))],
        compiler_params=pltpu.CompilerParams(vmem_limit_bytes=4 * 1024 * 1024),
    )(x, att, w_o, k, v)


def solution(mesh):
    batch_spec = P(('dp', 'cp'))
    seq_spec = P('dp', 'cp')
    whole = P()

    def per_device(x_tok, prompt_lens, k_cache, v_cache, norm_gain, w_q, b_q, w_k, b_k, w_v, b_v, w_o):
        rows = x_tok.shape[0]
        batch, slots, kv_heads, dim = k_cache.shape
        n = batch // rows
        inv_freq = np.power(np.float32(ROPE_THETA), -(np.arange(dim // 2, dtype=np.float32) * 2.0 / dim)).astype(np.float32)
        freq = jnp.asarray(np.concatenate([inv_freq, inv_freq])[None, :])
        pack = (n, rows, slots * kv_heads, dim)
        att, k_all, v_all, wo = step(
            prompt_lens, freq, x_tok, norm_gain.reshape(-1, dim), b_q.reshape(-1, dim), b_k.reshape(-1, dim), b_v.reshape(-1, dim),
            w_q, w_k, w_v, w_o, k_cache.reshape(pack), v_cache.reshape(pack))
        y_out, k_out, v_out = finish(x_tok, att, wo, k_all, v_all)
        shape = (rows, n * slots, kv_heads, dim)
        return y_out, k_out.reshape(shape), v_out.reshape(shape)

    return jax.shard_map(per_device, mesh=mesh, in_specs=(batch_spec, P('dp'), seq_spec, seq_spec, whole, whole, whole, whole, whole, whole, whole, whole), out_specs=(batch_spec, batch_spec, batch_spec), check_vma=False)
```

```python
import functools
import numpy as np
import jax
import jax.numpy as jnp
from jax import lax
from jax.experimental import pallas as pl
from jax.experimental.pallas import tpu as pltpu
from jax.sharding import PartitionSpec as P

RMS_EPS = 1e-6
ROPE_THETA = 1000000.0
MESH = pl.DeviceIdType.MESH
F32 = jnp.float32
BF16 = jnp.bfloat16


def flip(me, d):
    out = 0
    for k in range(4):
        bit = 1 << k
        out = out + bit * lax.rem(lax.div(me, bit) + lax.div(d, bit), 2)
    return out


def step_kernel(n, lens_hbm, freq_hbm, x_ref, gain_ref, bq_ref, bk_ref, bv_ref, wq_ref, wk_ref, wv_ref, wo_ref, k_ref, v_ref,
                att_ref, ko_ref, vo_ref, wo,
                lens_ref, freq_ref, k_land, v_land, wq, wk, wv, xs, gain, bq, bk, bv,
                q_s, kn_s, vn_s, s_s, e_s, l_s, acc, send_sem, recv_sem, load_sem, turn):
    me = lax.axis_index("cp")
    rows, heads, dim = q_s.shape
    m = k_land.shape[2]
    width = heads * dim
    loads = {}
    for idx, (name, src, dst) in enumerate([
            ("lens", lens_hbm, lens_ref), ("freq", freq_hbm, freq_ref), ("x", x_ref, xs), ("gain", gain_ref, gain), ("bq", bq_ref, bq), ("bk", bk_ref, bk), ("bv", bv_ref, bv),
            ("wk", wk_ref, wk), ("wv", wv_ref, wv), ("wq", wq_ref, wq),
            ("k", k_ref.at[me], k_land.at[:, me]), ("v", v_ref.at[me], v_land.at[:, me]), ("wo", wo_ref, wo)]):
        loads[name] = pltpu.make_async_copy(src, dst, load_sem.at[idx])

    barrier = pltpu.get_barrier_semaphore()
    for d in range(1, n):
        pl.semaphore_signal(barrier, inc=1, device_id={"cp": lax.rem(me + d, n)}, device_id_type=MESH)
    for copy in loads.values():
        copy.start()
    pl.semaphore_wait(barrier, n - 1)

    pairs = ((k_ref, k_land), (v_ref, v_land))

    def send(a, to):
        return pltpu.make_async_remote_copy(
            src_ref=pairs[a][0].at[to], dst_ref=pairs[a][1].at[:, me], send_sem=send_sem.at[a, to], recv_sem=recv_sem.at[a, me],
            device_id={"cp": to}, device_id_type=MESH)

    def arrive(a, d):
        src = lax.rem(me + n - d, n)
        pltpu.make_async_remote_copy(
            src_ref=pairs[a][0].at[0], dst_ref=pairs[a][1].at[:, src], send_sem=send_sem.at[a, src], recv_sem=recv_sem.at[a, src],
            device_id={"cp": src}, device_id_type=MESH).wait_recv()
        return src

    half, layer = n // 2, n // 4
    z = lax.div(me, layer)
    high = lax.div(me, half)
    end = lax.rem(z + high, 2) == 0
    middle = lax.rem(z + high, 2) == 1
    second = lax.rem(me, 2) == 1
    beside = [z * layer + lax.rem(me + t, layer) for t in range(1, layer)]
    near = [(4 * high + 1 - z) * layer + lax.rem(me + t, layer) for t in range(layer)]
    far = [(2 - high) * layer + lax.rem(me + t, layer) for t in range(layer)]
    far += [3 * (1 - high) * layer + lax.rem(me + t, layer) for t in range(layer)]

    def each(targets, act):
        for to in targets:
            for a in range(2):
                act(send(a, to))

    def start(copy):
        copy.start()

    def sent(copy):
        copy.wait_send()

    first = lax.rem(me, 2) == 0

    @pl.when(middle & first)
    def _():
        each(far, start)

    @pl.when(end | second)
    def _():
        each(near + beside, start)

    loads["lens"].wait()
    pos = [lens_ref[me * rows + b] for b in range(rows)]

    for name in ("freq", "x", "gain", "bq", "bk", "bv", "wk", "wv", "wq"):
        loads[name].wait()
    wide = xs[...].astype(F32)
    inv = lax.rsqrt(jnp.mean(wide * wide, axis=-1, keepdims=True) + RMS_EPS)
    gains = jnp.concatenate([gain[h:h + 1, :].astype(F32) for h in range(heads)], axis=1)
    normed = (wide * inv * gains).astype(BF16)
    which = lax.broadcasted_iota(jnp.int32, (rows, dim), 0)
    lane = lax.broadcasted_iota(jnp.int32, (rows, dim), 1)
    posf = jnp.zeros((rows, dim), F32)
    for b in range(rows):
        posf = jnp.where(which == b, pos[b].astype(F32), posf)
    angle = posf * freq_ref[...]
    cos_t = jnp.cos(angle)
    sin_t = jnp.sin(angle)
    sin_t = jnp.where(lane < dim // 2, -sin_t, sin_t)

    def rotate(t):
        return (t * cos_t + pltpu.roll(t, dim // 2, 1) * sin_t).astype(BF16).astype(F32)

    for h in range(2):
        cols = pl.ds(h * dim, dim)
        kn_s[:, h, :] = rotate(jnp.dot(normed, wk[:, cols], preferred_element_type=F32) + bk[h:h + 1, :].astype(F32))
        vn_s[:, h, :] = (jnp.dot(normed, wv[:, cols], preferred_element_type=F32) + bv[h:h + 1, :].astype(F32)).astype(BF16).astype(F32)
    for h in range(heads):
        q_s[:, h, :] = rotate(jnp.dot(normed, wq[:, h * dim:(h + 1) * dim], preferred_element_type=F32) + bq[h:h + 1, :].astype(F32))

    def hand_over(to):
        each(far[:-1], sent)
        pl.semaphore_signal(turn, inc=1, device_id={"cp": to}, device_id_type=MESH)

    @pl.when(middle & first)
    def _():
        hand_over(me + 1)
        each(near + beside, start)

    @pl.when(end | second)
    def _():
        pl.semaphore_wait(turn, 1)
        each(far, start)

    @pl.when(middle & second)
    def _():
        hand_over(3 * layer * high + lax.rem(me, layer) - 1)

    @pl.when(end & first)
    def _():
        hand_over(me + 1)

    row = lax.broadcasted_iota(jnp.int32, (m, dim), 0)
    even = lax.rem(row, 2) == 0

    def merge(land, new, out, b, i):
        at = 2 * pos[b] - i * m
        fresh = jnp.where(even, new[b, 0:1, :], new[b, 1:2, :])
        merged = jnp.where(row < at, land[b, i].astype(F32), jnp.where(row < at + 2, fresh, 0.0)).astype(BF16)
        out[b, i] = merged
        return merged

    def k_block(i):
        cols = pl.ds(pl.multiple_of(i * m, m), m)
        for b in range(rows):
            keys = merge(k_land, kn_s, ko_ref, b, i)
            s_s[b, :, cols] = lax.dot_general(q_s[b].astype(BF16), keys, (((1,), (1,)), ((), ())), preferred_element_type=F32) * (dim ** -0.5)

    def v_block(i):
        cols = pl.ds(pl.multiple_of(i * m, m), m)
        for b in range(rows):
            vals = merge(v_land, vn_s, vo_ref, b, i)
            acc[b] += jnp.dot(e_s[b, :, cols], vals, preferred_element_type=F32)

    def k_step(d, c):
        k_block(arrive(0, d))
        return c

    def v_step(d, c):
        v_block(arrive(1, d))
        return c

    loads["k"].wait()
    k_block(me)
    lax.fori_loop(1, n, k_step, 0)

    col = lax.broadcasted_iota(jnp.int32, (heads, n * m), 1)
    head = lax.broadcasted_iota(jnp.int32, (heads, n * m), 0)
    mine = lax.rem(col, 2) == lax.div(head, heads // 2)
    for b in range(rows):
        valid = mine & (col < 2 * pos[b] + 2)
        s = jnp.where(valid, s_s[b], -1e30)
        e = jnp.where(valid, jnp.exp(s - jnp.max(s, axis=-1, keepdims=True)), 0.0)
        l_s[b] = jnp.broadcast_to(jnp.sum(e, axis=-1, keepdims=True), (heads, dim))
        e_s[b] = e.astype(BF16)
    acc[...] = jnp.zeros_like(acc)

    loads["v"].wait()
    v_block(me)
    loads["wo"].wait()
    lax.fori_loop(1, n, v_step, 0)

    acc[...] = acc[...] / l_s[...]
    att_ref[...] = jnp.concatenate([acc[:, h, :] for h in range(heads)], axis=1).astype(BF16)

    each(beside + near + far[-1:], sent)

    @pl.when(end & second)
    def _():
        each(far[:-1], sent)


def step(lens, freq, x, gain, b_q, b_k, b_v, w_q, w_k, w_v, w_o, k, v):
    n, rows, m, dim = k.shape
    heads = w_q.shape[1] // dim
    kv = w_k.shape[1] // dim
    cache = pltpu.VMEM((rows, n, m, dim), BF16)
    hbm = pl.BlockSpec(memory_space=pltpu.HBM)
    vmem = pl.BlockSpec(memory_space=pltpu.VMEM)
    return pl.pallas_call(
        functools.partial(step_kernel, n),
        out_shape=[pltpu.VMEM(x.shape, BF16), cache, cache, pltpu.VMEM(w_o.shape, BF16)],
        in_specs=[hbm] * 13,
        out_specs=[vmem] * 4,
        scratch_shapes=[
            pltpu.SMEM(lens.shape, jnp.int32), pltpu.VMEM(freq.shape, F32),
            pltpu.VMEM((rows, n, m, dim), BF16), pltpu.VMEM((rows, n, m, dim), BF16),
            pltpu.VMEM(w_q.shape, BF16), pltpu.VMEM(w_k.shape, BF16), pltpu.VMEM(w_v.shape, BF16),
            pltpu.VMEM(x.shape, BF16), pltpu.VMEM(gain.shape, BF16), pltpu.VMEM(b_q.shape, BF16), pltpu.VMEM(b_k.shape, BF16), pltpu.VMEM(b_v.shape, BF16),
            pltpu.VMEM((rows, heads, dim), F32), pltpu.VMEM((rows, kv, dim), F32), pltpu.VMEM((rows, kv, dim), F32),
            pltpu.VMEM((rows, heads, n * m), F32), pltpu.VMEM((rows, heads, n * m), BF16), pltpu.VMEM((rows, heads, dim), F32),
            pltpu.VMEM((rows, heads, dim), F32),
            pltpu.SemaphoreType.DMA((2, n)), pltpu.SemaphoreType.DMA((2, n)), pltpu.SemaphoreType.DMA((13,)), pltpu.SemaphoreType.REGULAR],
        compiler_params=pltpu.CompilerParams(collective_id=0, has_side_effects=True, vmem_limit_bytes=47 * 1024 * 1024),
    )(lens, freq, x, gain, b_q, b_k, b_v, w_q, w_k, w_v, w_o, k, v)


def finish_kernel(x_ref, att_ref, wo_ref, k_ref, v_ref, y_ref, ko_ref, vo_ref, sem):
    copies = [pltpu.make_async_copy(k_ref, ko_ref, sem.at[0]), pltpu.make_async_copy(v_ref, vo_ref, sem.at[1])]
    for copy in copies:
        copy.start()
    tile = 256
    for t in range(wo_ref.shape[1] // tile):
        cols = slice(t * tile, (t + 1) * tile)
        y_ref[:, cols] = (x_ref[:, cols].astype(F32) + jnp.dot(att_ref[...], wo_ref[:, cols], preferred_element_type=F32)).astype(BF16)
    for copy in copies:
        copy.wait()


def finish(x, att, w_o, k, v):
    vmem = pl.BlockSpec(memory_space=pltpu.VMEM)
    hbm = pl.BlockSpec(memory_space=pltpu.HBM)
    cache = jax.ShapeDtypeStruct(k.shape, BF16)
    return pl.pallas_call(
        finish_kernel,
        out_shape=[jax.ShapeDtypeStruct(x.shape, BF16), cache, cache],
        in_specs=[vmem] * 5,
        out_specs=[vmem, hbm, hbm],
        scratch_shapes=[pltpu.SemaphoreType.DMA((2,))],
        compiler_params=pltpu.CompilerParams(vmem_limit_bytes=4 * 1024 * 1024),
    )(x, att, w_o, k, v)


def solution(mesh):
    batch_spec = P(('dp', 'cp'))
    seq_spec = P('dp', 'cp')
    whole = P()

    def per_device(x_tok, prompt_lens, k_cache, v_cache, norm_gain, w_q, b_q, w_k, b_k, w_v, b_v, w_o):
        rows = x_tok.shape[0]
        batch, slots, kv_heads, dim = k_cache.shape
        n = batch // rows
        inv_freq = np.power(np.float32(ROPE_THETA), -(np.arange(dim // 2, dtype=np.float32) * 2.0 / dim)).astype(np.float32)
        freq = jnp.asarray(np.concatenate([inv_freq, inv_freq])[None, :])
        pack = (n, rows, slots * kv_heads, dim)
        att, k_all, v_all, wo = step(
            prompt_lens, freq, x_tok, norm_gain.reshape(-1, dim), b_q.reshape(-1, dim), b_k.reshape(-1, dim), b_v.reshape(-1, dim),
            w_q, w_k, w_v, w_o, k_cache.reshape(pack), v_cache.reshape(pack))
        y_out, k_out, v_out = finish(x_tok, att, wo, k_all, v_all)
        shape = (rows, n * slots, kv_heads, dim)
        return y_out, k_out.reshape(shape), v_out.reshape(shape)

    return jax.shard_map(per_device, mesh=mesh, in_specs=(batch_spec, P('dp'), seq_spec, seq_spec, whole, whole, whole, whole, whole, whole, whole, whole), out_specs=(batch_spec, batch_spec, batch_spec), check_vma=False)
```

```python
import functools
import numpy as np
import jax
import jax.numpy as jnp
from jax import lax
from jax.experimental import pallas as pl
from jax.experimental.pallas import tpu as pltpu
from jax.sharding import PartitionSpec as P

RMS_EPS = 1e-6
ROPE_THETA = 1000000.0
MESH = pl.DeviceIdType.MESH
F32 = jnp.float32
BF16 = jnp.bfloat16


def flip(me, d):
    out = 0
    for k in range(4):
        bit = 1 << k
        out = out + bit * lax.rem(lax.div(me, bit) + lax.div(d, bit), 2)
    return out


def step_kernel(n, lens_hbm, freq_hbm, x_ref, gain_ref, bq_ref, bk_ref, bv_ref, wq_ref, wk_ref, wv_ref, wo_ref, k_ref, v_ref,
                att_ref, ko_ref, vo_ref, wo,
                lens_ref, freq_ref, k_land, v_land, wq, wk, wv, xs, gain, bq, bk, bv,
                q_s, kn_s, vn_s, s_s, e_s, l_s, acc, send_sem, recv_sem, load_sem, turn):
    me = lax.axis_index("cp")
    rows, heads, dim = q_s.shape
    m = k_land.shape[2]
    width = heads * dim
    loads = {}
    for idx, (name, src, dst) in enumerate([
            ("lens", lens_hbm, lens_ref), ("freq", freq_hbm, freq_ref), ("x", x_ref, xs), ("gain", gain_ref, gain), ("bq", bq_ref, bq), ("bk", bk_ref, bk), ("bv", bv_ref, bv),
            ("wk", wk_ref, wk), ("wv", wv_ref, wv), ("wq", wq_ref, wq),
            ("k", k_ref.at[me], k_land.at[:, me]), ("v", v_ref.at[me], v_land.at[:, me]), ("wo", wo_ref, wo)]):
        loads[name] = pltpu.make_async_copy(src, dst, load_sem.at[idx])

    barrier = pltpu.get_barrier_semaphore()
    for d in range(1, n):
        pl.semaphore_signal(barrier, inc=1, device_id={"cp": lax.rem(me + d, n)}, device_id_type=MESH)
    for copy in loads.values():
        copy.start()
    pl.semaphore_wait(barrier, n - 1)

    pairs = ((k_ref, k_land), (v_ref, v_land))

    def send(a, to):
        return pltpu.make_async_remote_copy(
            src_ref=pairs[a][0].at[to], dst_ref=pairs[a][1].at[:, me], send_sem=send_sem.at[a, to], recv_sem=recv_sem.at[a, me],
            device_id={"cp": to}, device_id_type=MESH)

    def arrive(a, d):
        src = lax.rem(me + n - d, n)
        pltpu.make_async_remote_copy(
            src_ref=pairs[a][0].at[0], dst_ref=pairs[a][1].at[:, src], send_sem=send_sem.at[a, src], recv_sem=recv_sem.at[a, src],
            device_id={"cp": src}, device_id_type=MESH).wait_recv()
        return src

    half, layer = n // 2, n // 4
    z = lax.div(me, layer)
    high = lax.div(me, half)
    end = lax.rem(z + high, 2) == 0
    middle = lax.rem(z + high, 2) == 1
    second = lax.rem(me, 2) == 1
    y, core = lax.rem(lax.div(me, 2), 2), lax.rem(me, 2)

    def chip(z_to, y_to):
        return [z_to * layer + 2 * y_to + core, z_to * layer + 2 * y_to + 1 - core]

    far_z = (2 - high, 3 * (1 - high))
    far = [to for y_to in (y, 1 - y) for z_to in far_z for to in chip(z_to, y_to)]
    near = chip(4 * high + 1 - z, 1 - y) + chip(4 * high + 1 - z, y)
    beside = chip(z, 1 - y) + chip(z, y)[1:]

    def each(targets, act):
        for to in targets:
            for a in range(2):
                act(send(a, to))

    def start(copy):
        copy.start()

    def sent(copy):
        copy.wait_send()

    @pl.when(middle)
    def _():
        each(far, start)

    each(beside + near, start)

    loads["lens"].wait()
    pos = [lens_ref[me * rows + b] for b in range(rows)]

    for name in ("freq", "x", "gain", "bq", "bk", "bv", "wk", "wv", "wq"):
        loads[name].wait()
    wide = xs[...].astype(F32)
    inv = lax.rsqrt(jnp.mean(wide * wide, axis=-1, keepdims=True) + RMS_EPS)
    gains = jnp.concatenate([gain[h:h + 1, :].astype(F32) for h in range(heads)], axis=1)
    normed = (wide * inv * gains).astype(BF16)
    which = lax.broadcasted_iota(jnp.int32, (rows, dim), 0)
    lane = lax.broadcasted_iota(jnp.int32, (rows, dim), 1)
    posf = jnp.zeros((rows, dim), F32)
    for b in range(rows):
        posf = jnp.where(which == b, pos[b].astype(F32), posf)
    angle = posf * freq_ref[...]
    cos_t = jnp.cos(angle)
    sin_t = jnp.sin(angle)
    sin_t = jnp.where(lane < dim // 2, -sin_t, sin_t)

    def rotate(t):
        return (t * cos_t + pltpu.roll(t, dim // 2, 1) * sin_t).astype(BF16).astype(F32)

    for h in range(2):
        cols = pl.ds(h * dim, dim)
        kn_s[:, h, :] = rotate(jnp.dot(normed, wk[:, cols], preferred_element_type=F32) + bk[h:h + 1, :].astype(F32))
        vn_s[:, h, :] = (jnp.dot(normed, wv[:, cols], preferred_element_type=F32) + bv[h:h + 1, :].astype(F32)).astype(BF16).astype(F32)
    for h in range(heads):
        q_s[:, h, :] = rotate(jnp.dot(normed, wq[:, h * dim:(h + 1) * dim], preferred_element_type=F32) + bq[h:h + 1, :].astype(F32))

    @pl.when(middle)
    def _():
        each(far[:-1], sent)
        pl.semaphore_signal(turn, inc=1, device_id={"cp": 3 * layer * high + lax.rem(me, layer) - lax.rem(me, 2)}, device_id_type=MESH)

    @pl.when(end & (lax.rem(me, 2) == 0))
    def _():
        pl.semaphore_wait(turn, 2)
        each(far, start)
        each(far[:-1], sent)
        pl.semaphore_signal(turn, inc=1, device_id={"cp": me + 1}, device_id_type=MESH)

    @pl.when(end & second)
    def _():
        pl.semaphore_wait(turn, 1)
        each(far, start)

    row = lax.broadcasted_iota(jnp.int32, (m, dim), 0)
    even = lax.rem(row, 2) == 0

    def merge(land, new, out, b, i):
        at = 2 * pos[b] - i * m
        fresh = jnp.where(even, new[b, 0:1, :], new[b, 1:2, :])
        merged = jnp.where(row < at, land[b, i].astype(F32), jnp.where(row < at + 2, fresh, 0.0)).astype(BF16)
        out[b, i] = merged
        return merged

    def k_block(i):
        cols = pl.ds(pl.multiple_of(i * m, m), m)
        for b in range(rows):
            keys = merge(k_land, kn_s, ko_ref, b, i)
            s_s[b, :, cols] = lax.dot_general(q_s[b].astype(BF16), keys, (((1,), (1,)), ((), ())), preferred_element_type=F32) * (dim ** -0.5)

    def v_block(i):
        cols = pl.ds(pl.multiple_of(i * m, m), m)
        for b in range(rows):
            vals = merge(v_land, vn_s, vo_ref, b, i)
            acc[b] += jnp.dot(e_s[b, :, cols], vals, preferred_element_type=F32)

    def k_step(d, c):
        k_block(arrive(0, d))
        return c

    def v_step(d, c):
        v_block(arrive(1, d))
        return c

    loads["k"].wait()
    k_block(me)
    lax.fori_loop(1, n, k_step, 0)

    col = lax.broadcasted_iota(jnp.int32, (heads, n * m), 1)
    head = lax.broadcasted_iota(jnp.int32, (heads, n * m), 0)
    mine = lax.rem(col, 2) == lax.div(head, heads // 2)
    for b in range(rows):
        valid = mine & (col < 2 * pos[b] + 2)
        s = jnp.where(valid, s_s[b], -1e30)
        e = jnp.where(valid, jnp.exp(s - jnp.max(s, axis=-1, keepdims=True)), 0.0)
        l_s[b] = jnp.broadcast_to(jnp.sum(e, axis=-1, keepdims=True), (heads, dim))
        e_s[b] = e.astype(BF16)
    acc[...] = jnp.zeros_like(acc)

    loads["v"].wait()
    v_block(me)
    loads["wo"].wait()
    lax.fori_loop(1, n, v_step, 0)

    acc[...] = acc[...] / l_s[...]
    att_ref[...] = jnp.concatenate([acc[:, h, :] for h in range(heads)], axis=1).astype(BF16)

    each(beside + near + far[-1:], sent)

    @pl.when(end & second)
    def _():
        each(far[:-1], sent)


def step(lens, freq, x, gain, b_q, b_k, b_v, w_q, w_k, w_v, w_o, k, v):
    n, rows, m, dim = k.shape
    heads = w_q.shape[1] // dim
    kv = w_k.shape[1] // dim
    cache = pltpu.VMEM((rows, n, m, dim), BF16)
    hbm = pl.BlockSpec(memory_space=pltpu.HBM)
    vmem = pl.BlockSpec(memory_space=pltpu.VMEM)
    return pl.pallas_call(
        functools.partial(step_kernel, n),
        out_shape=[pltpu.VMEM(x.shape, BF16), cache, cache, pltpu.VMEM(w_o.shape, BF16)],
        in_specs=[hbm] * 13,
        out_specs=[vmem] * 4,
        scratch_shapes=[
            pltpu.SMEM(lens.shape, jnp.int32), pltpu.VMEM(freq.shape, F32),
            pltpu.VMEM((rows, n, m, dim), BF16), pltpu.VMEM((rows, n, m, dim), BF16),
            pltpu.VMEM(w_q.shape, BF16), pltpu.VMEM(w_k.shape, BF16), pltpu.VMEM(w_v.shape, BF16),
            pltpu.VMEM(x.shape, BF16), pltpu.VMEM(gain.shape, BF16), pltpu.VMEM(b_q.shape, BF16), pltpu.VMEM(b_k.shape, BF16), pltpu.VMEM(b_v.shape, BF16),
            pltpu.VMEM((rows, heads, dim), F32), pltpu.VMEM((rows, kv, dim), F32), pltpu.VMEM((rows, kv, dim), F32),
            pltpu.VMEM((rows, heads, n * m), F32), pltpu.VMEM((rows, heads, n * m), BF16), pltpu.VMEM((rows, heads, dim), F32),
            pltpu.VMEM((rows, heads, dim), F32),
            pltpu.SemaphoreType.DMA((2, n)), pltpu.SemaphoreType.DMA((2, n)), pltpu.SemaphoreType.DMA((13,)), pltpu.SemaphoreType.REGULAR],
        compiler_params=pltpu.CompilerParams(collective_id=0, has_side_effects=True, vmem_limit_bytes=47 * 1024 * 1024),
    )(lens, freq, x, gain, b_q, b_k, b_v, w_q, w_k, w_v, w_o, k, v)


def finish_kernel(x_ref, att_ref, wo_ref, k_ref, v_ref, y_ref, ko_ref, vo_ref, sem):
    copies = [pltpu.make_async_copy(k_ref, ko_ref, sem.at[0]), pltpu.make_async_copy(v_ref, vo_ref, sem.at[1])]
    for copy in copies:
        copy.start()
    tile = 256
    for t in range(wo_ref.shape[1] // tile):
        cols = slice(t * tile, (t + 1) * tile)
        y_ref[:, cols] = (x_ref[:, cols].astype(F32) + jnp.dot(att_ref[...], wo_ref[:, cols], preferred_element_type=F32)).astype(BF16)
    for copy in copies:
        copy.wait()


def finish(x, att, w_o, k, v):
    vmem = pl.BlockSpec(memory_space=pltpu.VMEM)
    hbm = pl.BlockSpec(memory_space=pltpu.HBM)
    cache = jax.ShapeDtypeStruct(k.shape, BF16)
    return pl.pallas_call(
        finish_kernel,
        out_shape=[jax.ShapeDtypeStruct(x.shape, BF16), cache, cache],
        in_specs=[vmem] * 5,
        out_specs=[vmem, hbm, hbm],
        scratch_shapes=[pltpu.SemaphoreType.DMA((2,))],
        compiler_params=pltpu.CompilerParams(vmem_limit_bytes=4 * 1024 * 1024),
    )(x, att, w_o, k, v)


def solution(mesh):
    batch_spec = P(('dp', 'cp'))
    seq_spec = P('dp', 'cp')
    whole = P()

    def per_device(x_tok, prompt_lens, k_cache, v_cache, norm_gain, w_q, b_q, w_k, b_k, w_v, b_v, w_o):
        rows = x_tok.shape[0]
        batch, slots, kv_heads, dim = k_cache.shape
        n = batch // rows
        inv_freq = np.power(np.float32(ROPE_THETA), -(np.arange(dim // 2, dtype=np.float32) * 2.0 / dim)).astype(np.float32)
        freq = jnp.asarray(np.concatenate([inv_freq, inv_freq])[None, :])
        pack = (n, rows, slots * kv_heads, dim)
        att, k_all, v_all, wo = step(
            prompt_lens, freq, x_tok, norm_gain.reshape(-1, dim), b_q.reshape(-1, dim), b_k.reshape(-1, dim), b_v.reshape(-1, dim),
            w_q, w_k, w_v, w_o, k_cache.reshape(pack), v_cache.reshape(pack))
        y_out, k_out, v_out = finish(x_tok, att, wo, k_all, v_all)
        shape = (rows, n * slots, kv_heads, dim)
        return y_out, k_out.reshape(shape), v_out.reshape(shape)

    return jax.shard_map(per_device, mesh=mesh, in_specs=(batch_spec, P('dp'), seq_spec, seq_spec, whole, whole, whole, whole, whole, whole, whole, whole), out_specs=(batch_spec, batch_spec, batch_spec), check_vma=False)
```

```python
import functools
import numpy as np
import jax
import jax.numpy as jnp
from jax import lax
from jax.experimental import pallas as pl
from jax.experimental.pallas import tpu as pltpu
from jax.sharding import PartitionSpec as P

RMS_EPS = 1e-6
ROPE_THETA = 1000000.0
MESH = pl.DeviceIdType.MESH
F32 = jnp.float32
BF16 = jnp.bfloat16


def flip(me, d):
    out = 0
    for k in range(4):
        bit = 1 << k
        out = out + bit * lax.rem(lax.div(me, bit) + lax.div(d, bit), 2)
    return out


def step_kernel(n, lens_hbm, freq_hbm, x_ref, gain_ref, bq_ref, bk_ref, bv_ref, wq_ref, wk_ref, wv_ref, wo_ref, k_ref, v_ref,
                att_ref, ko_ref, vo_ref, wo,
                lens_ref, freq_ref, k_land, v_land, wq, wk, wv, xs, gain, bq, bk, bv,
                q_s, kn_s, vn_s, s_s, e_s, l_s, acc, send_sem, recv_sem, load_sem, turn):
    me = lax.axis_index("cp")
    rows, heads, dim = q_s.shape
    m = k_land.shape[2]
    width = heads * dim
    loads = {}
    for idx, (name, src, dst) in enumerate([
            ("lens", lens_hbm, lens_ref), ("freq", freq_hbm, freq_ref), ("x", x_ref, xs), ("gain", gain_ref, gain), ("bq", bq_ref, bq), ("bk", bk_ref, bk), ("bv", bv_ref, bv),
            ("wk", wk_ref, wk), ("wv", wv_ref, wv), ("wq", wq_ref, wq),
            ("k", k_ref.at[me], k_land.at[:, me]), ("v", v_ref.at[me], v_land.at[:, me]), ("wo", wo_ref, wo)]):
        loads[name] = pltpu.make_async_copy(src, dst, load_sem.at[idx])

    barrier = pltpu.get_barrier_semaphore()
    for d in range(1, n):
        pl.semaphore_signal(barrier, inc=1, device_id={"cp": lax.rem(me + d, n)}, device_id_type=MESH)
    for copy in loads.values():
        copy.start()
    pl.semaphore_wait(barrier, n - 1)

    pairs = ((k_ref, k_land), (v_ref, v_land))

    def send(a, to):
        return pltpu.make_async_remote_copy(
            src_ref=pairs[a][0].at[to], dst_ref=pairs[a][1].at[:, me], send_sem=send_sem.at[a, to], recv_sem=recv_sem.at[a, me],
            device_id={"cp": to}, device_id_type=MESH)

    def arrive(a, d):
        src = lax.rem(me + n - d, n)
        pltpu.make_async_remote_copy(
            src_ref=pairs[a][0].at[0], dst_ref=pairs[a][1].at[:, src], send_sem=send_sem.at[a, src], recv_sem=recv_sem.at[a, src],
            device_id={"cp": src}, device_id_type=MESH).wait_recv()
        return src

    half, layer = n // 2, n // 4
    z = lax.div(me, layer)
    high = lax.div(me, half)
    end = lax.rem(z + high, 2) == 0
    middle = lax.rem(z + high, 2) == 1
    second = lax.rem(me, 2) == 1
    y, core = lax.rem(lax.div(me, 2), 2), lax.rem(me, 2)

    def chip(z_to, y_to):
        return [z_to * layer + 2 * y_to + core, z_to * layer + 2 * y_to + 1 - core]

    far_z = (2 - high, 3 * (1 - high))
    far = [to for y_to in (y, 1 - y) for z_to in far_z for to in chip(z_to, y_to)]
    near = chip(4 * high + 1 - z, y) + chip(4 * high + 1 - z, 1 - y)
    beside = chip(z, 1 - y) + chip(z, y)[1:]

    def each(targets, act):
        for to in targets:
            for a in range(2):
                act(send(a, to))

    def start(copy):
        copy.start()

    def sent(copy):
        copy.wait_send()

    @pl.when(middle)
    def _():
        each(far, start)

    each(beside + near[:2], start)

    @pl.when(end)
    def _():
        each(near[2:], start)

    loads["lens"].wait()
    pos = [lens_ref[me * rows + b] for b in range(rows)]

    for name in ("freq", "x", "gain", "bq", "bk", "bv", "wk", "wv", "wq"):
        loads[name].wait()
    wide = xs[...].astype(F32)
    inv = lax.rsqrt(jnp.mean(wide * wide, axis=-1, keepdims=True) + RMS_EPS)
    gains = jnp.concatenate([gain[h:h + 1, :].astype(F32) for h in range(heads)], axis=1)
    normed = (wide * inv * gains).astype(BF16)
    which = lax.broadcasted_iota(jnp.int32, (rows, dim), 0)
    lane = lax.broadcasted_iota(jnp.int32, (rows, dim), 1)
    posf = jnp.zeros((rows, dim), F32)
    for b in range(rows):
        posf = jnp.where(which == b, pos[b].astype(F32), posf)
    angle = posf * freq_ref[...]
    cos_t = jnp.cos(angle)
    sin_t = jnp.sin(angle)
    sin_t = jnp.where(lane < dim // 2, -sin_t, sin_t)

    def rotate(t):
        return (t * cos_t + pltpu.roll(t, dim // 2, 1) * sin_t).astype(BF16).astype(F32)

    for h in range(2):
        cols = pl.ds(h * dim, dim)
        kn_s[:, h, :] = rotate(jnp.dot(normed, wk[:, cols], preferred_element_type=F32) + bk[h:h + 1, :].astype(F32))
        vn_s[:, h, :] = (jnp.dot(normed, wv[:, cols], preferred_element_type=F32) + bv[h:h + 1, :].astype(F32)).astype(BF16).astype(F32)
    for h in range(heads):
        q_s[:, h, :] = rotate(jnp.dot(normed, wq[:, h * dim:(h + 1) * dim], preferred_element_type=F32) + bq[h:h + 1, :].astype(F32))

    @pl.when(middle)
    def _():
        each(far[:-1], sent)
        pl.semaphore_signal(turn, inc=1, device_id={"cp": 3 * layer * high + lax.rem(me, layer) - lax.rem(me, 2)}, device_id_type=MESH)
        each(near[2:], start)

    @pl.when(end & (lax.rem(me, 2) == 0))
    def _():
        pl.semaphore_wait(turn, 2)
        each(far, start)
        each(far[:-1], sent)
        pl.semaphore_signal(turn, inc=1, device_id={"cp": me + 1}, device_id_type=MESH)

    @pl.when(end & second)
    def _():
        pl.semaphore_wait(turn, 1)
        each(far, start)

    row = lax.broadcasted_iota(jnp.int32, (m, dim), 0)
    even = lax.rem(row, 2) == 0

    def merge(land, new, out, b, i):
        at = 2 * pos[b] - i * m
        fresh = jnp.where(even, new[b, 0:1, :], new[b, 1:2, :])
        merged = jnp.where(row < at, land[b, i].astype(F32), jnp.where(row < at + 2, fresh, 0.0)).astype(BF16)
        out[b, i] = merged
        return merged

    def k_block(i):
        cols = pl.ds(pl.multiple_of(i * m, m), m)
        for b in range(rows):
            keys = merge(k_land, kn_s, ko_ref, b, i)
            s_s[b, :, cols] = lax.dot_general(q_s[b].astype(BF16), keys, (((1,), (1,)), ((), ())), preferred_element_type=F32) * (dim ** -0.5)

    def v_block(i):
        cols = pl.ds(pl.multiple_of(i * m, m), m)
        for b in range(rows):
            vals = merge(v_land, vn_s, vo_ref, b, i)
            acc[b] += jnp.dot(e_s[b, :, cols], vals, preferred_element_type=F32)

    def k_step(d, c):
        k_block(arrive(0, d))
        return c

    def v_step(d, c):
        v_block(arrive(1, d))
        return c

    loads["k"].wait()
    k_block(me)
    lax.fori_loop(1, n, k_step, 0)

    col = lax.broadcasted_iota(jnp.int32, (heads, n * m), 1)
    head = lax.broadcasted_iota(jnp.int32, (heads, n * m), 0)
    mine = lax.rem(col, 2) == lax.div(head, heads // 2)
    for b in range(rows):
        valid = mine & (col < 2 * pos[b] + 2)
        s = jnp.where(valid, s_s[b], -1e30)
        e = jnp.where(valid, jnp.exp(s - jnp.max(s, axis=-1, keepdims=True)), 0.0)
        l_s[b] = jnp.broadcast_to(jnp.sum(e, axis=-1, keepdims=True), (heads, dim))
        e_s[b] = e.astype(BF16)
    acc[...] = jnp.zeros_like(acc)

    loads["v"].wait()
    v_block(me)
    loads["wo"].wait()
    lax.fori_loop(1, n, v_step, 0)

    acc[...] = acc[...] / l_s[...]
    att_ref[...] = jnp.concatenate([acc[:, h, :] for h in range(heads)], axis=1).astype(BF16)

    each(beside + near + far[-1:], sent)

    @pl.when(end & second)
    def _():
        each(far[:-1], sent)


def step(lens, freq, x, gain, b_q, b_k, b_v, w_q, w_k, w_v, w_o, k, v):
    n, rows, m, dim = k.shape
    heads = w_q.shape[1] // dim
    kv = w_k.shape[1] // dim
    cache = pltpu.VMEM((rows, n, m, dim), BF16)
    hbm = pl.BlockSpec(memory_space=pltpu.HBM)
    vmem = pl.BlockSpec(memory_space=pltpu.VMEM)
    return pl.pallas_call(
        functools.partial(step_kernel, n),
        out_shape=[pltpu.VMEM(x.shape, BF16), cache, cache, pltpu.VMEM(w_o.shape, BF16)],
        in_specs=[hbm] * 13,
        out_specs=[vmem] * 4,
        scratch_shapes=[
            pltpu.SMEM(lens.shape, jnp.int32), pltpu.VMEM(freq.shape, F32),
            pltpu.VMEM((rows, n, m, dim), BF16), pltpu.VMEM((rows, n, m, dim), BF16),
            pltpu.VMEM(w_q.shape, BF16), pltpu.VMEM(w_k.shape, BF16), pltpu.VMEM(w_v.shape, BF16),
            pltpu.VMEM(x.shape, BF16), pltpu.VMEM(gain.shape, BF16), pltpu.VMEM(b_q.shape, BF16), pltpu.VMEM(b_k.shape, BF16), pltpu.VMEM(b_v.shape, BF16),
            pltpu.VMEM((rows, heads, dim), F32), pltpu.VMEM((rows, kv, dim), F32), pltpu.VMEM((rows, kv, dim), F32),
            pltpu.VMEM((rows, heads, n * m), F32), pltpu.VMEM((rows, heads, n * m), BF16), pltpu.VMEM((rows, heads, dim), F32),
            pltpu.VMEM((rows, heads, dim), F32),
            pltpu.SemaphoreType.DMA((2, n)), pltpu.SemaphoreType.DMA((2, n)), pltpu.SemaphoreType.DMA((13,)), pltpu.SemaphoreType.REGULAR],
        compiler_params=pltpu.CompilerParams(collective_id=0, has_side_effects=True, vmem_limit_bytes=47 * 1024 * 1024),
    )(lens, freq, x, gain, b_q, b_k, b_v, w_q, w_k, w_v, w_o, k, v)


def finish_kernel(x_ref, att_ref, wo_ref, k_ref, v_ref, y_ref, ko_ref, vo_ref, sem):
    copies = [pltpu.make_async_copy(k_ref, ko_ref, sem.at[0]), pltpu.make_async_copy(v_ref, vo_ref, sem.at[1])]
    for copy in copies:
        copy.start()
    tile = 256
    for t in range(wo_ref.shape[1] // tile):
        cols = slice(t * tile, (t + 1) * tile)
        y_ref[:, cols] = (x_ref[:, cols].astype(F32) + jnp.dot(att_ref[...], wo_ref[:, cols], preferred_element_type=F32)).astype(BF16)
    for copy in copies:
        copy.wait()


def finish(x, att, w_o, k, v):
    vmem = pl.BlockSpec(memory_space=pltpu.VMEM)
    hbm = pl.BlockSpec(memory_space=pltpu.HBM)
    cache = jax.ShapeDtypeStruct(k.shape, BF16)
    return pl.pallas_call(
        finish_kernel,
        out_shape=[jax.ShapeDtypeStruct(x.shape, BF16), cache, cache],
        in_specs=[vmem] * 5,
        out_specs=[vmem, hbm, hbm],
        scratch_shapes=[pltpu.SemaphoreType.DMA((2,))],
        compiler_params=pltpu.CompilerParams(vmem_limit_bytes=4 * 1024 * 1024),
    )(x, att, w_o, k, v)


def solution(mesh):
    batch_spec = P(('dp', 'cp'))
    seq_spec = P('dp', 'cp')
    whole = P()

    def per_device(x_tok, prompt_lens, k_cache, v_cache, norm_gain, w_q, b_q, w_k, b_k, w_v, b_v, w_o):
        rows = x_tok.shape[0]
        batch, slots, kv_heads, dim = k_cache.shape
        n = batch // rows
        inv_freq = np.power(np.float32(ROPE_THETA), -(np.arange(dim // 2, dtype=np.float32) * 2.0 / dim)).astype(np.float32)
        freq = jnp.asarray(np.concatenate([inv_freq, inv_freq])[None, :])
        pack = (n, rows, slots * kv_heads, dim)
        att, k_all, v_all, wo = step(
            prompt_lens, freq, x_tok, norm_gain.reshape(-1, dim), b_q.reshape(-1, dim), b_k.reshape(-1, dim), b_v.reshape(-1, dim),
            w_q, w_k, w_v, w_o, k_cache.reshape(pack), v_cache.reshape(pack))
        y_out, k_out, v_out = finish(x_tok, att, wo, k_all, v_all)
        shape = (rows, n * slots, kv_heads, dim)
        return y_out, k_out.reshape(shape), v_out.reshape(shape)

    return jax.shard_map(per_device, mesh=mesh, in_specs=(batch_spec, P('dp'), seq_spec, seq_spec, whole, whole, whole, whole, whole, whole, whole, whole), out_specs=(batch_spec, batch_spec, batch_spec), check_vma=False)
```

```python
import functools
import numpy as np
import jax
import jax.numpy as jnp
from jax import lax
from jax.experimental import pallas as pl
from jax.experimental.pallas import tpu as pltpu
from jax.sharding import PartitionSpec as P

RMS_EPS = 1e-6
ROPE_THETA = 1000000.0
MESH = pl.DeviceIdType.MESH
F32 = jnp.float32
BF16 = jnp.bfloat16


def flip(me, d):
    out = 0
    for k in range(4):
        bit = 1 << k
        out = out + bit * lax.rem(lax.div(me, bit) + lax.div(d, bit), 2)
    return out


def step_kernel(n, lens_hbm, freq_hbm, x_ref, gain_ref, bq_ref, bk_ref, bv_ref, wq_ref, wk_ref, wv_ref, wo_ref, k_ref, v_ref,
                att_ref, ko_ref, vo_ref, wo,
                lens_ref, freq_ref, k_land, v_land, wq, wk, wv, xs, gain, bq, bk, bv,
                q_s, kn_s, vn_s, s_s, e_s, l_s, acc, send_sem, recv_sem, load_sem, turn):
    me = lax.axis_index("cp")
    rows, heads, dim = q_s.shape
    m = k_land.shape[2]
    width = heads * dim
    loads = {}
    for idx, (name, src, dst) in enumerate([
            ("lens", lens_hbm, lens_ref), ("freq", freq_hbm, freq_ref), ("x", x_ref, xs), ("gain", gain_ref, gain), ("bq", bq_ref, bq), ("bk", bk_ref, bk), ("bv", bv_ref, bv),
            ("wk", wk_ref, wk), ("wv", wv_ref, wv), ("wq", wq_ref, wq),
            ("k", k_ref.at[me], k_land.at[:, me]), ("v", v_ref.at[me], v_land.at[:, me]), ("wo", wo_ref, wo)]):
        loads[name] = pltpu.make_async_copy(src, dst, load_sem.at[idx])

    barrier = pltpu.get_barrier_semaphore()
    for d in range(1, n):
        pl.semaphore_signal(barrier, inc=1, device_id={"cp": lax.rem(me + d, n)}, device_id_type=MESH)
    for copy in loads.values():
        copy.start()
    pl.semaphore_wait(barrier, n - 1)

    pairs = ((k_ref, k_land), (v_ref, v_land))

    def send(a, to):
        return pltpu.make_async_remote_copy(
            src_ref=pairs[a][0].at[to], dst_ref=pairs[a][1].at[:, me], send_sem=send_sem.at[a, to], recv_sem=recv_sem.at[a, me],
            device_id={"cp": to}, device_id_type=MESH)

    def arrive(a, d):
        src = lax.rem(me + n - d, n)
        pltpu.make_async_remote_copy(
            src_ref=pairs[a][0].at[0], dst_ref=pairs[a][1].at[:, src], send_sem=send_sem.at[a, src], recv_sem=recv_sem.at[a, src],
            device_id={"cp": src}, device_id_type=MESH).wait_recv()
        return src

    half, layer = n // 2, n // 4
    z = lax.div(me, layer)
    high = lax.div(me, half)
    end = lax.rem(z + high, 2) == 0
    middle = lax.rem(z + high, 2) == 1
    second = lax.rem(me, 2) == 1
    y, core = lax.rem(lax.div(me, 2), 2), lax.rem(me, 2)

    def chip(z_to, y_to):
        return [z_to * layer + 2 * y_to + core, z_to * layer + 2 * y_to + 1 - core]

    far_z = (2 - high, 3 * (1 - high))
    far = [to for y_to in (y, 1 - y) for z_to in far_z for to in chip(z_to, y_to)]
    near = chip(4 * high + 1 - z, 1 - y) + chip(4 * high + 1 - z, y)
    beside = chip(z, 1 - y) + chip(z, y)[1:]

    def each(targets, act):
        for to in targets:
            for a in range(2):
                act(send(a, to))

    def start(copy):
        copy.start()

    def sent(copy):
        copy.wait_send()

    @pl.when(middle)
    def _():
        each(far, start)

    each(beside + near, start)

    loads["lens"].wait()
    pos = [lens_ref[me * rows + b] for b in range(rows)]

    for name in ("freq", "x", "gain", "bq", "bk", "bv", "wk", "wv", "wq"):
        loads[name].wait()
    wide = xs[...].astype(F32)
    inv = lax.rsqrt(jnp.mean(wide * wide, axis=-1, keepdims=True) + RMS_EPS)
    gains = jnp.concatenate([gain[h:h + 1, :].astype(F32) for h in range(heads)], axis=1)
    normed = (wide * inv * gains).astype(BF16)
    which = lax.broadcasted_iota(jnp.int32, (rows, dim), 0)
    lane = lax.broadcasted_iota(jnp.int32, (rows, dim), 1)
    posf = jnp.zeros((rows, dim), F32)
    for b in range(rows):
        posf = jnp.where(which == b, pos[b].astype(F32), posf)
    angle = posf * freq_ref[...]
    cos_t = jnp.cos(angle)
    sin_t = jnp.sin(angle)
    sin_t = jnp.where(lane < dim // 2, -sin_t, sin_t)

    def rotate(t):
        return (t * cos_t + pltpu.roll(t, dim // 2, 1) * sin_t).astype(BF16).astype(F32)

    for h in range(2):
        cols = pl.ds(h * dim, dim)
        kn_s[:, h, :] = rotate(jnp.dot(normed, wk[:, cols], preferred_element_type=F32) + bk[h:h + 1, :].astype(F32))
        vn_s[:, h, :] = (jnp.dot(normed, wv[:, cols], preferred_element_type=F32) + bv[h:h + 1, :].astype(F32)).astype(BF16).astype(F32)
    for h in range(heads):
        q_s[:, h, :] = rotate(jnp.dot(normed, wq[:, h * dim:(h + 1) * dim], preferred_element_type=F32) + bq[h:h + 1, :].astype(F32))

    @pl.when(middle)
    def _():
        each(far[:4], sent)
        pl.semaphore_signal(turn, inc=1, device_id={"cp": 3 * layer * high + lax.rem(me, layer) - lax.rem(me, 2)}, device_id_type=MESH)

    @pl.when(end & (lax.rem(me, 2) == 0))
    def _():
        pl.semaphore_wait(turn, 2)
        each(far, start)
        each(far[:-1], sent)
        pl.semaphore_signal(turn, inc=1, device_id={"cp": me + 1}, device_id_type=MESH)

    @pl.when(end & second)
    def _():
        pl.semaphore_wait(turn, 1)
        each(far, start)

    row = lax.broadcasted_iota(jnp.int32, (m, dim), 0)
    even = lax.rem(row, 2) == 0

    def merge(land, new, out, b, i):
        at = 2 * pos[b] - i * m
        fresh = jnp.where(even, new[b, 0:1, :], new[b, 1:2, :])
        merged = jnp.where(row < at, land[b, i].astype(F32), jnp.where(row < at + 2, fresh, 0.0)).astype(BF16)
        out[b, i] = merged
        return merged

    def k_block(i):
        cols = pl.ds(pl.multiple_of(i * m, m), m)
        for b in range(rows):
            keys = merge(k_land, kn_s, ko_ref, b, i)
            s_s[b, :, cols] = lax.dot_general(q_s[b].astype(BF16), keys, (((1,), (1,)), ((), ())), preferred_element_type=F32) * (dim ** -0.5)

    def v_block(i):
        cols = pl.ds(pl.multiple_of(i * m, m), m)
        for b in range(rows):
            vals = merge(v_land, vn_s, vo_ref, b, i)
            acc[b] += jnp.dot(e_s[b, :, cols], vals, preferred_element_type=F32)

    def k_step(d, c):
        k_block(arrive(0, d))
        return c

    def v_step(d, c):
        v_block(arrive(1, d))
        return c

    loads["k"].wait()
    k_block(me)
    lax.fori_loop(1, n, k_step, 0)

    col = lax.broadcasted_iota(jnp.int32, (heads, n * m), 1)
    head = lax.broadcasted_iota(jnp.int32, (heads, n * m), 0)
    mine = lax.rem(col, 2) == lax.div(head, heads // 2)
    for b in range(rows):
        valid = mine & (col < 2 * pos[b] + 2)
        s = jnp.where(valid, s_s[b], -1e30)
        e = jnp.where(valid, jnp.exp(s - jnp.max(s, axis=-1, keepdims=True)), 0.0)
        l_s[b] = jnp.broadcast_to(jnp.sum(e, axis=-1, keepdims=True), (heads, dim))
        e_s[b] = e.astype(BF16)
    acc[...] = jnp.zeros_like(acc)

    loads["v"].wait()
    v_block(me)
    loads["wo"].wait()
    lax.fori_loop(1, n, v_step, 0)

    acc[...] = acc[...] / l_s[...]
    att_ref[...] = jnp.concatenate([acc[:, h, :] for h in range(heads)], axis=1).astype(BF16)

    each(beside + near + far[-1:], sent)

    @pl.when(middle)
    def _():
        each(far[4:-1], sent)

    @pl.when(end & second)
    def _():
        each(far[:-1], sent)


def step(lens, freq, x, gain, b_q, b_k, b_v, w_q, w_k, w_v, w_o, k, v):
    n, rows, m, dim = k.shape
    heads = w_q.shape[1] // dim
    kv = w_k.shape[1] // dim
    cache = pltpu.VMEM((rows, n, m, dim), BF16)
    hbm = pl.BlockSpec(memory_space=pltpu.HBM)
    vmem = pl.BlockSpec(memory_space=pltpu.VMEM)
    return pl.pallas_call(
        functools.partial(step_kernel, n),
        out_shape=[pltpu.VMEM(x.shape, BF16), cache, cache, pltpu.VMEM(w_o.shape, BF16)],
        in_specs=[hbm] * 13,
        out_specs=[vmem] * 4,
        scratch_shapes=[
            pltpu.SMEM(lens.shape, jnp.int32), pltpu.VMEM(freq.shape, F32),
            pltpu.VMEM((rows, n, m, dim), BF16), pltpu.VMEM((rows, n, m, dim), BF16),
            pltpu.VMEM(w_q.shape, BF16), pltpu.VMEM(w_k.shape, BF16), pltpu.VMEM(w_v.shape, BF16),
            pltpu.VMEM(x.shape, BF16), pltpu.VMEM(gain.shape, BF16), pltpu.VMEM(b_q.shape, BF16), pltpu.VMEM(b_k.shape, BF16), pltpu.VMEM(b_v.shape, BF16),
            pltpu.VMEM((rows, heads, dim), F32), pltpu.VMEM((rows, kv, dim), F32), pltpu.VMEM((rows, kv, dim), F32),
            pltpu.VMEM((rows, heads, n * m), F32), pltpu.VMEM((rows, heads, n * m), BF16), pltpu.VMEM((rows, heads, dim), F32),
            pltpu.VMEM((rows, heads, dim), F32),
            pltpu.SemaphoreType.DMA((2, n)), pltpu.SemaphoreType.DMA((2, n)), pltpu.SemaphoreType.DMA((13,)), pltpu.SemaphoreType.REGULAR],
        compiler_params=pltpu.CompilerParams(collective_id=0, has_side_effects=True, vmem_limit_bytes=47 * 1024 * 1024),
    )(lens, freq, x, gain, b_q, b_k, b_v, w_q, w_k, w_v, w_o, k, v)


def finish_kernel(x_ref, att_ref, wo_ref, k_ref, v_ref, y_ref, ko_ref, vo_ref, sem):
    copies = [pltpu.make_async_copy(k_ref, ko_ref, sem.at[0]), pltpu.make_async_copy(v_ref, vo_ref, sem.at[1])]
    for copy in copies:
        copy.start()
    tile = 256
    for t in range(wo_ref.shape[1] // tile):
        cols = slice(t * tile, (t + 1) * tile)
        y_ref[:, cols] = (x_ref[:, cols].astype(F32) + jnp.dot(att_ref[...], wo_ref[:, cols], preferred_element_type=F32)).astype(BF16)
    for copy in copies:
        copy.wait()


def finish(x, att, w_o, k, v):
    vmem = pl.BlockSpec(memory_space=pltpu.VMEM)
    hbm = pl.BlockSpec(memory_space=pltpu.HBM)
    cache = jax.ShapeDtypeStruct(k.shape, BF16)
    return pl.pallas_call(
        finish_kernel,
        out_shape=[jax.ShapeDtypeStruct(x.shape, BF16), cache, cache],
        in_specs=[vmem] * 5,
        out_specs=[vmem, hbm, hbm],
        scratch_shapes=[pltpu.SemaphoreType.DMA((2,))],
        compiler_params=pltpu.CompilerParams(vmem_limit_bytes=4 * 1024 * 1024),
    )(x, att, w_o, k, v)


def solution(mesh):
    batch_spec = P(('dp', 'cp'))
    seq_spec = P('dp', 'cp')
    whole = P()

    def per_device(x_tok, prompt_lens, k_cache, v_cache, norm_gain, w_q, b_q, w_k, b_k, w_v, b_v, w_o):
        rows = x_tok.shape[0]
        batch, slots, kv_heads, dim = k_cache.shape
        n = batch // rows
        inv_freq = np.power(np.float32(ROPE_THETA), -(np.arange(dim // 2, dtype=np.float32) * 2.0 / dim)).astype(np.float32)
        freq = jnp.asarray(np.concatenate([inv_freq, inv_freq])[None, :])
        pack = (n, rows, slots * kv_heads, dim)
        att, k_all, v_all, wo = step(
            prompt_lens, freq, x_tok, norm_gain.reshape(-1, dim), b_q.reshape(-1, dim), b_k.reshape(-1, dim), b_v.reshape(-1, dim),
            w_q, w_k, w_v, w_o, k_cache.reshape(pack), v_cache.reshape(pack))
        y_out, k_out, v_out = finish(x_tok, att, wo, k_all, v_all)
        shape = (rows, n * slots, kv_heads, dim)
        return y_out, k_out.reshape(shape), v_out.reshape(shape)

    return jax.shard_map(per_device, mesh=mesh, in_specs=(batch_spec, P('dp'), seq_spec, seq_spec, whole, whole, whole, whole, whole, whole, whole, whole), out_specs=(batch_spec, batch_spec, batch_spec), check_vma=False)
```

```python
import functools
import numpy as np
import jax
import jax.numpy as jnp
from jax import lax
from jax.experimental import pallas as pl
from jax.experimental.pallas import tpu as pltpu
from jax.sharding import PartitionSpec as P

RMS_EPS = 1e-6
ROPE_THETA = 1000000.0
MESH = pl.DeviceIdType.MESH
F32 = jnp.float32
BF16 = jnp.bfloat16


def flip(me, d):
    out = 0
    for k in range(4):
        bit = 1 << k
        out = out + bit * lax.rem(lax.div(me, bit) + lax.div(d, bit), 2)
    return out


def step_kernel(n, lens_hbm, freq_hbm, x_ref, gain_ref, bq_ref, bk_ref, bv_ref, wq_ref, wk_ref, wv_ref, wo_ref, k_ref, v_ref,
                att_ref, ko_ref, vo_ref, wo,
                lens_ref, freq_ref, k_land, v_land, wq, wk, wv, xs, gain, bq, bk, bv,
                q_s, kn_s, vn_s, s_s, e_s, l_s, acc, send_sem, recv_sem, load_sem, turn):
    me = lax.axis_index("cp")
    rows, heads, dim = q_s.shape
    m = k_land.shape[2]
    width = heads * dim
    loads = {}
    for idx, (name, src, dst) in enumerate([
            ("lens", lens_hbm, lens_ref), ("freq", freq_hbm, freq_ref), ("x", x_ref, xs), ("gain", gain_ref, gain), ("bq", bq_ref, bq), ("bk", bk_ref, bk), ("bv", bv_ref, bv),
            ("wk", wk_ref, wk), ("wv", wv_ref, wv), ("wq", wq_ref, wq),
            ("k", k_ref.at[me], k_land.at[:, me]), ("v", v_ref.at[me], v_land.at[:, me]), ("wo", wo_ref, wo)]):
        loads[name] = pltpu.make_async_copy(src, dst, load_sem.at[idx])

    barrier = pltpu.get_barrier_semaphore()
    for d in range(1, n):
        pl.semaphore_signal(barrier, inc=1, device_id={"cp": lax.rem(me + d, n)}, device_id_type=MESH)
    for copy in loads.values():
        copy.start()
    pl.semaphore_wait(barrier, n - 1)

    pairs = ((k_ref, k_land), (v_ref, v_land))

    def send(a, to):
        return pltpu.make_async_remote_copy(
            src_ref=pairs[a][0].at[to], dst_ref=pairs[a][1].at[:, me], send_sem=send_sem.at[a, to], recv_sem=recv_sem.at[a, me],
            device_id={"cp": to}, device_id_type=MESH)

    def arrive(a, d):
        src = lax.rem(me + n - d, n)
        pltpu.make_async_remote_copy(
            src_ref=pairs[a][0].at[0], dst_ref=pairs[a][1].at[:, src], send_sem=send_sem.at[a, src], recv_sem=recv_sem.at[a, src],
            device_id={"cp": src}, device_id_type=MESH).wait_recv()
        return src

    half, layer = n // 2, n // 4
    z = lax.div(me, layer)
    high = lax.div(me, half)
    end = lax.rem(z + high, 2) == 0
    middle = lax.rem(z + high, 2) == 1
    second = lax.rem(me, 2) == 1
    y, core = lax.rem(lax.div(me, 2), 2), lax.rem(me, 2)

    def chip(z_to, y_to):
        return [z_to * layer + 2 * y_to + core, z_to * layer + 2 * y_to + 1 - core]

    far_z = (2 - high, 3 * (1 - high))
    far = [to for y_to in (y, 1 - y) for z_to in far_z for to in chip(z_to, y_to)]
    near = chip(4 * high + 1 - z, 1 - y) + chip(4 * high + 1 - z, y)
    beside = chip(z, 1 - y) + chip(z, y)[1:]

    def each(targets, act):
        for to in targets:
            for a in range(2):
                act(send(a, to))

    def start(copy):
        copy.start()

    def sent(copy):
        copy.wait_send()

    @pl.when(middle)
    def _():
        each(far, start)

    each(beside + near, start)

    loads["lens"].wait()
    pos = [lens_ref[me * rows + b] for b in range(rows)]

    for name in ("freq", "x", "gain", "bq", "bk", "bv", "wk", "wv", "wq"):
        loads[name].wait()
    wide = xs[...].astype(F32)
    inv = lax.rsqrt(jnp.mean(wide * wide, axis=-1, keepdims=True) + RMS_EPS)
    gains = jnp.concatenate([gain[h:h + 1, :].astype(F32) for h in range(heads)], axis=1)
    normed = (wide * inv * gains).astype(BF16)
    which = lax.broadcasted_iota(jnp.int32, (rows, dim), 0)
    lane = lax.broadcasted_iota(jnp.int32, (rows, dim), 1)
    posf = jnp.zeros((rows, dim), F32)
    for b in range(rows):
        posf = jnp.where(which == b, pos[b].astype(F32), posf)
    angle = posf * freq_ref[...]
    cos_t = jnp.cos(angle)
    sin_t = jnp.sin(angle)
    sin_t = jnp.where(lane < dim // 2, -sin_t, sin_t)

    def rotate(t):
        return (t * cos_t + pltpu.roll(t, dim // 2, 1) * sin_t).astype(BF16).astype(F32)

    for h in range(2):
        cols = pl.ds(h * dim, dim)
        kn_s[:, h, :] = rotate(jnp.dot(normed, wk[:, cols], preferred_element_type=F32) + bk[h:h + 1, :].astype(F32))
        vn_s[:, h, :] = (jnp.dot(normed, wv[:, cols], preferred_element_type=F32) + bv[h:h + 1, :].astype(F32)).astype(BF16).astype(F32)
    for h in range(heads):
        q_s[:, h, :] = rotate(jnp.dot(normed, wq[:, h * dim:(h + 1) * dim], preferred_element_type=F32) + bq[h:h + 1, :].astype(F32))

    @pl.when(middle)
    def _():
        each(far[:4], sent)
        pl.semaphore_signal(turn, inc=1, device_id={"cp": 3 * layer * high + lax.rem(me, layer) - lax.rem(me, 2)}, device_id_type=MESH)

    @pl.when(end & (lax.rem(me, 2) == 0))
    def _():
        pl.semaphore_wait(turn, 2)
        each(far, start)
        each(far[:4], sent)
        pl.semaphore_signal(turn, inc=1, device_id={"cp": me + 1}, device_id_type=MESH)

    @pl.when(end & second)
    def _():
        pl.semaphore_wait(turn, 1)
        each(far, start)

    row = lax.broadcasted_iota(jnp.int32, (m, dim), 0)
    even = lax.rem(row, 2) == 0

    def merge(land, new, out, b, i):
        at = 2 * pos[b] - i * m
        fresh = jnp.where(even, new[b, 0:1, :], new[b, 1:2, :])
        merged = jnp.where(row < at, land[b, i].astype(F32), jnp.where(row < at + 2, fresh, 0.0)).astype(BF16)
        out[b, i] = merged
        return merged

    def k_block(i):
        cols = pl.ds(pl.multiple_of(i * m, m), m)
        for b in range(rows):
            keys = merge(k_land, kn_s, ko_ref, b, i)
            s_s[b, :, cols] = lax.dot_general(q_s[b].astype(BF16), keys, (((1,), (1,)), ((), ())), preferred_element_type=F32) * (dim ** -0.5)

    def v_block(i):
        cols = pl.ds(pl.multiple_of(i * m, m), m)
        for b in range(rows):
            vals = merge(v_land, vn_s, vo_ref, b, i)
            acc[b] += jnp.dot(e_s[b, :, cols], vals, preferred_element_type=F32)

    def k_step(d, c):
        k_block(arrive(0, d))
        return c

    def v_step(d, c):
        v_block(arrive(1, d))
        return c

    loads["k"].wait()
    k_block(me)
    lax.fori_loop(1, n, k_step, 0)

    col = lax.broadcasted_iota(jnp.int32, (heads, n * m), 1)
    head = lax.broadcasted_iota(jnp.int32, (heads, n * m), 0)
    mine = lax.rem(col, 2) == lax.div(head, heads // 2)
    for b in range(rows):
        valid = mine & (col < 2 * pos[b] + 2)
        s = jnp.where(valid, s_s[b], -1e30)
        e = jnp.where(valid, jnp.exp(s - jnp.max(s, axis=-1, keepdims=True)), 0.0)
        l_s[b] = jnp.broadcast_to(jnp.sum(e, axis=-1, keepdims=True), (heads, dim))
        e_s[b] = e.astype(BF16)
    acc[...] = jnp.zeros_like(acc)

    loads["v"].wait()
    v_block(me)
    loads["wo"].wait()
    lax.fori_loop(1, n, v_step, 0)

    acc[...] = acc[...] / l_s[...]
    att_ref[...] = jnp.concatenate([acc[:, h, :] for h in range(heads)], axis=1).astype(BF16)

    each(beside + near + far[-1:], sent)

    @pl.when(middle | (lax.rem(me, 2) == 0))
    def _():
        each(far[4:-1], sent)

    @pl.when(end & second)
    def _():
        each(far[:-1], sent)


def step(lens, freq, x, gain, b_q, b_k, b_v, w_q, w_k, w_v, w_o, k, v):
    n, rows, m, dim = k.shape
    heads = w_q.shape[1] // dim
    kv = w_k.shape[1] // dim
    cache = pltpu.VMEM((rows, n, m, dim), BF16)
    hbm = pl.BlockSpec(memory_space=pltpu.HBM)
    vmem = pl.BlockSpec(memory_space=pltpu.VMEM)
    return pl.pallas_call(
        functools.partial(step_kernel, n),
        out_shape=[pltpu.VMEM(x.shape, BF16), cache, cache, pltpu.VMEM(w_o.shape, BF16)],
        in_specs=[hbm] * 13,
        out_specs=[vmem] * 4,
        scratch_shapes=[
            pltpu.SMEM(lens.shape, jnp.int32), pltpu.VMEM(freq.shape, F32),
            pltpu.VMEM((rows, n, m, dim), BF16), pltpu.VMEM((rows, n, m, dim), BF16),
            pltpu.VMEM(w_q.shape, BF16), pltpu.VMEM(w_k.shape, BF16), pltpu.VMEM(w_v.shape, BF16),
            pltpu.VMEM(x.shape, BF16), pltpu.VMEM(gain.shape, BF16), pltpu.VMEM(b_q.shape, BF16), pltpu.VMEM(b_k.shape, BF16), pltpu.VMEM(b_v.shape, BF16),
            pltpu.VMEM((rows, heads, dim), F32), pltpu.VMEM((rows, kv, dim), F32), pltpu.VMEM((rows, kv, dim), F32),
            pltpu.VMEM((rows, heads, n * m), F32), pltpu.VMEM((rows, heads, n * m), BF16), pltpu.VMEM((rows, heads, dim), F32),
            pltpu.VMEM((rows, heads, dim), F32),
            pltpu.SemaphoreType.DMA((2, n)), pltpu.SemaphoreType.DMA((2, n)), pltpu.SemaphoreType.DMA((13,)), pltpu.SemaphoreType.REGULAR],
        compiler_params=pltpu.CompilerParams(collective_id=0, has_side_effects=True, vmem_limit_bytes=47 * 1024 * 1024),
    )(lens, freq, x, gain, b_q, b_k, b_v, w_q, w_k, w_v, w_o, k, v)


def finish_kernel(x_ref, att_ref, wo_ref, k_ref, v_ref, y_ref, ko_ref, vo_ref, sem):
    copies = [pltpu.make_async_copy(k_ref, ko_ref, sem.at[0]), pltpu.make_async_copy(v_ref, vo_ref, sem.at[1])]
    for copy in copies:
        copy.start()
    tile = 256
    for t in range(wo_ref.shape[1] // tile):
        cols = slice(t * tile, (t + 1) * tile)
        y_ref[:, cols] = (x_ref[:, cols].astype(F32) + jnp.dot(att_ref[...], wo_ref[:, cols], preferred_element_type=F32)).astype(BF16)
    for copy in copies:
        copy.wait()


def finish(x, att, w_o, k, v):
    vmem = pl.BlockSpec(memory_space=pltpu.VMEM)
    hbm = pl.BlockSpec(memory_space=pltpu.HBM)
    cache = jax.ShapeDtypeStruct(k.shape, BF16)
    return pl.pallas_call(
        finish_kernel,
        out_shape=[jax.ShapeDtypeStruct(x.shape, BF16), cache, cache],
        in_specs=[vmem] * 5,
        out_specs=[vmem, hbm, hbm],
        scratch_shapes=[pltpu.SemaphoreType.DMA((2,))],
        compiler_params=pltpu.CompilerParams(vmem_limit_bytes=4 * 1024 * 1024),
    )(x, att, w_o, k, v)


def solution(mesh):
    batch_spec = P(('dp', 'cp'))
    seq_spec = P('dp', 'cp')
    whole = P()

    def per_device(x_tok, prompt_lens, k_cache, v_cache, norm_gain, w_q, b_q, w_k, b_k, w_v, b_v, w_o):
        rows = x_tok.shape[0]
        batch, slots, kv_heads, dim = k_cache.shape
        n = batch // rows
        inv_freq = np.power(np.float32(ROPE_THETA), -(np.arange(dim // 2, dtype=np.float32) * 2.0 / dim)).astype(np.float32)
        freq = jnp.asarray(np.concatenate([inv_freq, inv_freq])[None, :])
        pack = (n, rows, slots * kv_heads, dim)
        att, k_all, v_all, wo = step(
            prompt_lens, freq, x_tok, norm_gain.reshape(-1, dim), b_q.reshape(-1, dim), b_k.reshape(-1, dim), b_v.reshape(-1, dim),
            w_q, w_k, w_v, w_o, k_cache.reshape(pack), v_cache.reshape(pack))
        y_out, k_out, v_out = finish(x_tok, att, wo, k_all, v_all)
        shape = (rows, n * slots, kv_heads, dim)
        return y_out, k_out.reshape(shape), v_out.reshape(shape)

    return jax.shard_map(per_device, mesh=mesh, in_specs=(batch_spec, P('dp'), seq_spec, seq_spec, whole, whole, whole, whole, whole, whole, whole, whole), out_specs=(batch_spec, batch_spec, batch_spec), check_vma=False)
```

```python
import functools
import numpy as np
import jax
import jax.numpy as jnp
from jax import lax
from jax.experimental import pallas as pl
from jax.experimental.pallas import tpu as pltpu
from jax.sharding import PartitionSpec as P

RMS_EPS = 1e-6
ROPE_THETA = 1000000.0
MESH = pl.DeviceIdType.MESH
F32 = jnp.float32
BF16 = jnp.bfloat16


def flip(me, d):
    out = 0
    for k in range(4):
        bit = 1 << k
        out = out + bit * lax.rem(lax.div(me, bit) + lax.div(d, bit), 2)
    return out


def step_kernel(n, lens_hbm, freq_hbm, x_ref, gain_ref, bq_ref, bk_ref, bv_ref, wq_ref, wk_ref, wv_ref, wo_ref, k_ref, v_ref,
                att_ref, ko_ref, vo_ref, wo,
                lens_ref, freq_ref, k_land, v_land, wq, wk, wv, xs, gain, bq, bk, bv,
                q_s, kn_s, vn_s, s_s, e_s, l_s, acc, send_sem, recv_sem, load_sem):
    me = lax.axis_index("cp")
    rows, heads, dim = q_s.shape
    m = k_land.shape[2]
    width = heads * dim
    loads = {}
    for idx, (name, src, dst) in enumerate([
            ("lens", lens_hbm, lens_ref), ("freq", freq_hbm, freq_ref), ("x", x_ref, xs), ("gain", gain_ref, gain), ("bq", bq_ref, bq), ("bk", bk_ref, bk), ("bv", bv_ref, bv),
            ("wk", wk_ref, wk), ("wv", wv_ref, wv), ("wq", wq_ref, wq),
            ("k", k_ref.at[me], k_land.at[:, me]), ("v", v_ref.at[me], v_land.at[:, me]), ("wo", wo_ref, wo)]):
        loads[name] = pltpu.make_async_copy(src, dst, load_sem.at[idx])

    barrier = pltpu.get_barrier_semaphore()
    for d in range(1, n):
        pl.semaphore_signal(barrier, inc=1, device_id={"cp": lax.rem(me + d, n)}, device_id_type=MESH)
    for copy in loads.values():
        copy.start()
    pl.semaphore_wait(barrier, n - 1)

    pairs = ((k_ref, k_land), (v_ref, v_land))

    def send(a, to):
        return pltpu.make_async_remote_copy(
            src_ref=pairs[a][0].at[to], dst_ref=pairs[a][1].at[:, me], send_sem=send_sem.at[a, to], recv_sem=recv_sem.at[a, me],
            device_id={"cp": to}, device_id_type=MESH)

    def arrive(a, d):
        src = lax.rem(me + n - d, n)
        pltpu.make_async_remote_copy(
            src_ref=pairs[a][0].at[0], dst_ref=pairs[a][1].at[:, src], send_sem=send_sem.at[a, src], recv_sem=recv_sem.at[a, src],
            device_id={"cp": src}, device_id_type=MESH).wait_recv()
        return src

    half, layer = n // 2, n // 4
    z = lax.div(me, layer)
    high = lax.div(me, half)
    end = lax.rem(z + high, 2) == 0
    middle = lax.rem(z + high, 2) == 1
    y, core = lax.rem(lax.div(me, 2), 2), lax.rem(me, 2)

    def chip(z_to, y_to):
        return [z_to * layer + 2 * y_to + core, z_to * layer + 2 * y_to + 1 - core]

    far_z = (2 - high, 3 * (1 - high))
    far = [to for y_to in (y, 1 - y) for z_to in far_z for to in chip(z_to, y_to)]
    near = chip(4 * high + 1 - z, y) + chip(4 * high + 1 - z, 1 - y)
    beside = chip(z, 1 - y) + chip(z, y)[1:]

    def each(targets, act):
        for to in targets:
            for a in range(2):
                act(send(a, to))

    def start(copy):
        copy.start()

    def sent(copy):
        copy.wait_send()

    @pl.when(middle)
    def _():
        each(beside + far + near, start)

    @pl.when(end)
    def _():
        each(beside + near + far, start)

    loads["lens"].wait()
    pos = [lens_ref[me * rows + b] for b in range(rows)]

    for name in ("freq", "x", "gain", "bq", "bk", "bv", "wk", "wv", "wq"):
        loads[name].wait()
    wide = xs[...].astype(F32)
    inv = lax.rsqrt(jnp.mean(wide * wide, axis=-1, keepdims=True) + RMS_EPS)
    gains = jnp.concatenate([gain[h:h + 1, :].astype(F32) for h in range(heads)], axis=1)
    normed = (wide * inv * gains).astype(BF16)
    which = lax.broadcasted_iota(jnp.int32, (rows, dim), 0)
    lane = lax.broadcasted_iota(jnp.int32, (rows, dim), 1)
    posf = jnp.zeros((rows, dim), F32)
    for b in range(rows):
        posf = jnp.where(which == b, pos[b].astype(F32), posf)
    angle = posf * freq_ref[...]
    cos_t = jnp.cos(angle)
    sin_t = jnp.sin(angle)
    sin_t = jnp.where(lane < dim // 2, -sin_t, sin_t)

    def rotate(t):
        return (t * cos_t + pltpu.roll(t, dim // 2, 1) * sin_t).astype(BF16).astype(F32)

    for h in range(2):
        cols = pl.ds(h * dim, dim)
        kn_s[:, h, :] = rotate(jnp.dot(normed, wk[:, cols], preferred_element_type=F32) + bk[h:h + 1, :].astype(F32))
        vn_s[:, h, :] = (jnp.dot(normed, wv[:, cols], preferred_element_type=F32) + bv[h:h + 1, :].astype(F32)).astype(BF16).astype(F32)
    for h in range(heads):
        q_s[:, h, :] = rotate(jnp.dot(normed, wq[:, h * dim:(h + 1) * dim], preferred_element_type=F32) + bq[h:h + 1, :].astype(F32))

    row = lax.broadcasted_iota(jnp.int32, (m, dim), 0)
    even = lax.rem(row, 2) == 0

    def merge(land, new, out, b, i):
        at = 2 * pos[b] - i * m
        fresh = jnp.where(even, new[b, 0:1, :], new[b, 1:2, :])
        merged = jnp.where(row < at, land[b, i].astype(F32), jnp.where(row < at + 2, fresh, 0.0)).astype(BF16)
        out[b, i] = merged
        return merged

    def k_block(i):
        cols = pl.ds(pl.multiple_of(i * m, m), m)
        for b in range(rows):
            keys = merge(k_land, kn_s, ko_ref, b, i)
            s_s[b, :, cols] = lax.dot_general(q_s[b].astype(BF16), keys, (((1,), (1,)), ((), ())), preferred_element_type=F32) * (dim ** -0.5)

    def v_block(i):
        cols = pl.ds(pl.multiple_of(i * m, m), m)
        for b in range(rows):
            vals = merge(v_land, vn_s, vo_ref, b, i)
            acc[b] += jnp.dot(e_s[b, :, cols], vals, preferred_element_type=F32)

    def k_step(d, c):
        k_block(arrive(0, d))
        return c

    def v_step(d, c):
        v_block(arrive(1, d))
        return c

    loads["k"].wait()
    k_block(me)
    lax.fori_loop(1, n, k_step, 0)

    col = lax.broadcasted_iota(jnp.int32, (heads, n * m), 1)
    head = lax.broadcasted_iota(jnp.int32, (heads, n * m), 0)
    mine = lax.rem(col, 2) == lax.div(head, heads // 2)
    for b in range(rows):
        valid = mine & (col < 2 * pos[b] + 2)
        s = jnp.where(valid, s_s[b], -1e30)
        e = jnp.where(valid, jnp.exp(s - jnp.max(s, axis=-1, keepdims=True)), 0.0)
        l_s[b] = jnp.broadcast_to(jnp.sum(e, axis=-1, keepdims=True), (heads, dim))
        e_s[b] = e.astype(BF16)
    acc[...] = jnp.zeros_like(acc)

    loads["v"].wait()
    v_block(me)
    loads["wo"].wait()
    lax.fori_loop(1, n, v_step, 0)

    acc[...] = acc[...] / l_s[...]
    att_ref[...] = jnp.concatenate([acc[:, h, :] for h in range(heads)], axis=1).astype(BF16)

    each(beside + near + far, sent)


def step(lens, freq, x, gain, b_q, b_k, b_v, w_q, w_k, w_v, w_o, k, v):
    n, rows, m, dim = k.shape
    heads = w_q.shape[1] // dim
    kv = w_k.shape[1] // dim
    cache = pltpu.VMEM((rows, n, m, dim), BF16)
    hbm = pl.BlockSpec(memory_space=pltpu.HBM)
    vmem = pl.BlockSpec(memory_space=pltpu.VMEM)
    return pl.pallas_call(
        functools.partial(step_kernel, n),
        out_shape=[pltpu.VMEM(x.shape, BF16), cache, cache, pltpu.VMEM(w_o.shape, BF16)],
        in_specs=[hbm] * 13,
        out_specs=[vmem] * 4,
        scratch_shapes=[
            pltpu.SMEM(lens.shape, jnp.int32), pltpu.VMEM(freq.shape, F32),
            pltpu.VMEM((rows, n, m, dim), BF16), pltpu.VMEM((rows, n, m, dim), BF16),
            pltpu.VMEM(w_q.shape, BF16), pltpu.VMEM(w_k.shape, BF16), pltpu.VMEM(w_v.shape, BF16),
            pltpu.VMEM(x.shape, BF16), pltpu.VMEM(gain.shape, BF16), pltpu.VMEM(b_q.shape, BF16), pltpu.VMEM(b_k.shape, BF16), pltpu.VMEM(b_v.shape, BF16),
            pltpu.VMEM((rows, heads, dim), F32), pltpu.VMEM((rows, kv, dim), F32), pltpu.VMEM((rows, kv, dim), F32),
            pltpu.VMEM((rows, heads, n * m), F32), pltpu.VMEM((rows, heads, n * m), BF16), pltpu.VMEM((rows, heads, dim), F32),
            pltpu.VMEM((rows, heads, dim), F32),
            pltpu.SemaphoreType.DMA((2, n)), pltpu.SemaphoreType.DMA((2, n)), pltpu.SemaphoreType.DMA((13,))],
        compiler_params=pltpu.CompilerParams(collective_id=0, has_side_effects=True, vmem_limit_bytes=47 * 1024 * 1024),
    )(lens, freq, x, gain, b_q, b_k, b_v, w_q, w_k, w_v, w_o, k, v)


def finish_kernel(x_ref, att_ref, wo_ref, k_ref, v_ref, y_ref, ko_ref, vo_ref, sem):
    copies = [pltpu.make_async_copy(k_ref, ko_ref, sem.at[0]), pltpu.make_async_copy(v_ref, vo_ref, sem.at[1])]
    for copy in copies:
        copy.start()
    tile = 256
    for t in range(wo_ref.shape[1] // tile):
        cols = slice(t * tile, (t + 1) * tile)
        y_ref[:, cols] = (x_ref[:, cols].astype(F32) + jnp.dot(att_ref[...], wo_ref[:, cols], preferred_element_type=F32)).astype(BF16)
    for copy in copies:
        copy.wait()


def finish(x, att, w_o, k, v):
    vmem = pl.BlockSpec(memory_space=pltpu.VMEM)
    hbm = pl.BlockSpec(memory_space=pltpu.HBM)
    cache = jax.ShapeDtypeStruct(k.shape, BF16)
    return pl.pallas_call(
        finish_kernel,
        out_shape=[jax.ShapeDtypeStruct(x.shape, BF16), cache, cache],
        in_specs=[vmem] * 5,
        out_specs=[vmem, hbm, hbm],
        scratch_shapes=[pltpu.SemaphoreType.DMA((2,))],
        compiler_params=pltpu.CompilerParams(vmem_limit_bytes=4 * 1024 * 1024),
    )(x, att, w_o, k, v)


def solution(mesh):
    batch_spec = P(('dp', 'cp'))
    seq_spec = P('dp', 'cp')
    whole = P()

    def per_device(x_tok, prompt_lens, k_cache, v_cache, norm_gain, w_q, b_q, w_k, b_k, w_v, b_v, w_o):
        rows = x_tok.shape[0]
        batch, slots, kv_heads, dim = k_cache.shape
        n = batch // rows
        inv_freq = np.power(np.float32(ROPE_THETA), -(np.arange(dim // 2, dtype=np.float32) * 2.0 / dim)).astype(np.float32)
        freq = jnp.asarray(np.concatenate([inv_freq, inv_freq])[None, :])
        pack = (n, rows, slots * kv_heads, dim)
        att, k_all, v_all, wo = step(
            prompt_lens, freq, x_tok, norm_gain.reshape(-1, dim), b_q.reshape(-1, dim), b_k.reshape(-1, dim), b_v.reshape(-1, dim),
            w_q, w_k, w_v, w_o, k_cache.reshape(pack), v_cache.reshape(pack))
        y_out, k_out, v_out = finish(x_tok, att, wo, k_all, v_all)
        shape = (rows, n * slots, kv_heads, dim)
        return y_out, k_out.reshape(shape), v_out.reshape(shape)

    return jax.shard_map(per_device, mesh=mesh, in_specs=(batch_spec, P('dp'), seq_spec, seq_spec, whole, whole, whole, whole, whole, whole, whole, whole), out_specs=(batch_spec, batch_spec, batch_spec), check_vma=False)
```
